256 devices in a mesh: elem: 32 (over z_lo, y, core), band: 8 (over z_hi, x).
Axes of the slice: x: 4, y: 4, z: 8 (z_hi: 2, z_lo: 4; z = z_hi * 4 + z_lo), core: 2. Of those that a mesh axis runs over, the one named last changes fastest.
Arguments:
- y_current: bfloat16 [1024, 64, 2048], P('elem', None, 'band'), may hold values from -6 to 6
- y_previous: bfloat16 [1024, 64, 2048], P('elem', None, 'band'), may hold values from -6 to 6
- h_blocks: bfloat16 [1024, 64, 320], P('elem'), may hold values from -0.3125 to 0.3125
- basis_sizes: int32 [1024], P('elem'), may hold values from 40 to 64
- neighbours: int32 [1024, 4], P('elem'), may hold values from 0 to 1023, as said below
Outputs:
- filtered: bfloat16 [1024, 64, 2048], P('elem', None, 'band')
- margin: float32 [2048, 2048], P('elem', 'band')
The draws below stay inside these ranges and needn't reach their ends.
Inputs may be any that keep to these rules, and one draw needn't show every extreme that they name: `neighbours`: the elements lie on a periodic grid of 64 x 16; row i lists the elements that share an edge with element i, in the order previous grid row, next grid row, previous column, next column, so adjacency is symmetric. Element g belongs to index g // 32 of elem, whose elements fill 2 consecutive grid rows in some order; a neighbour therefore belongs to the same index or to one of the two beside it, periodically, and exactly 16 of an index's elements have a neighbour on the next index, and 16 on the previous one.
All inputs are finite; a program needn't handle non-finite values.
Results may differ from the reference program's by a relative error of at most 0.018.
Values may be sent and summed in bfloat16 or wider, within the bound.
A program may use at most 64 MiB of HBM per device.

```python
import jax
import jax.numpy as jnp
from jax import lax

BMAX = 64
SX = 2
GY = 16
BD = 256
DEGREES = 2
EL_DEV = 32
ELEMS = 1024
NBAND = 2048
N_ELEM = 32
N_BAND = 8


def draw_neighbours(key, part):
    keys = jax.random.split(jax.random.fold_in(key, 7), N_ELEM)

    def one_order(single):
        return jax.random.permutation(single, EL_DEV)
    orders = jax.vmap(one_order)(keys).astype(jnp.int32)
    owners = jnp.arange(N_ELEM, dtype=jnp.int32)[:, None] * EL_DEV
    grid = (owners + orders).reshape(SX * N_ELEM, GY)
    upper = jnp.roll(grid, 1, axis=0)
    lower = jnp.roll(grid, -1, axis=0)
    left_side = jnp.roll(grid, 1, axis=1)
    right_side = jnp.roll(grid, -1, axis=1)
    table = jnp.stack([upper, lower, left_side, right_side], axis=-1).reshape(-1, 4)
    return jnp.zeros((ELEMS, 4), jnp.int32).at[grid.reshape(-1)].set(table)


def with_ends(array, own_key, least, high):
    extent = array.shape
    place = [jax.random.randint(jax.random.fold_in(own_key, axis), (), 0, extent[axis]) for axis in range(len(extent))]
    array = array.at[tuple(place)].set(least)
    longest = extent.index(max(extent))
    place[longest] = (place[longest] + 1) % extent[longest]
    return array.at[tuple(place)].set(high)


def level_of(own_key, dims, cuts, smallest, top_value):
    def one(axis_at, parts):
        draws = jax.random.uniform(jax.random.fold_in(jax.random.fold_in(own_key, 6), axis_at), (parts,), jnp.float32, smallest / len(cuts), top_value / len(cuts))
        return jnp.repeat(jnp.exp(draws), dims[axis_at] // parts).reshape((-1,) + (1,) * (len(dims) - axis_at - 1))

    loudness = one(*cuts[0])
    for cut in cuts[1:]:
        loudness = loudness * one(*cut)
    return loudness


def bell_draw(key, dims, width, reach, cuts=(), held_as=jnp.bfloat16):
    drawn = width * jax.random.normal(key, dims, jnp.float32)
    if cuts:
        drawn = drawn * level_of(key, dims, cuts, -0.22, 0.18)
    return jnp.clip(drawn, -reach, reach).astype(held_as)


def setup_inputs(seed: int = 0) -> dict:
    key_list = jax.random.split(jax.random.key(seed), 6)
    y_current = bell_draw(key_list[0], (ELEMS, BMAX, NBAND), 1.0, 6.0, ((0, 32), (2, 8)))
    y_previous = bell_draw(key_list[1], (ELEMS, BMAX, NBAND), 1.0, 6.0, ((0, 32), (2, 8)))
    h_blocks = bell_draw(key_list[2], (ELEMS, BMAX, 5 * BMAX), (5 * BMAX) ** -0.5, 0.3125, ((0, 32),))
    basis_sizes = with_ends(jax.random.randint(key_list[3], (ELEMS,), BMAX * 5 // 8, BMAX + 1), jax.random.fold_in(key_list[3], 1), BMAX * 5 // 8, BMAX).astype(jnp.int32)
    neighbours = draw_neighbours(jax.random.fold_in(key_list[5], 71), 0)
    return dict(y_current=y_current, y_previous=y_previous, h_blocks=h_blocks, basis_sizes=basis_sizes, neighbours=neighbours)


center_value = 0.3
spectral_half = 1.7


def filter_block(pair, h_blocks, neighbours, row_mask):
    current, previous = pair
    current = current * row_mask
    previous = previous * row_mask
    hmatrix = h_blocks.astype(jnp.float32)
    mask_float = row_mask.astype(jnp.float32)
    for degree in range(DEGREES):
        nearby = current[neighbours]
        stacked = jnp.concatenate([current[:, None], nearby], axis=1)
        stacked = stacked.reshape(current.shape[0], 5 * BMAX, current.shape[2]).astype(jnp.float32)
        applied = jnp.einsum("irc,icb->irb", hmatrix, stacked, precision=lax.Precision.HIGHEST)
        following = mask_float * ((2.0 / spectral_half) * (applied - center_value * current.astype(jnp.float32)) - previous.astype(jnp.float32))
        previous = current
        current = following.astype(jnp.bfloat16)
    return current


def reference(y_current, y_previous, h_blocks, basis_sizes, neighbours):
    row_mask = (jnp.arange(BMAX, dtype=jnp.int32)[None, :] < basis_sizes[:, None]).astype(jnp.bfloat16)[:, :, None]

    def split_bands(values):
        return values.reshape(ELEMS, BMAX, N_BAND, BD).transpose(2, 0, 1, 3)

    def run_block(pair):
        return filter_block(pair, h_blocks, neighbours, row_mask)

    blocks = lax.map(run_block, (split_bands(y_current), split_bands(y_previous)))
    filtered = blocks.transpose(1, 2, 0, 3).reshape(ELEMS, BMAX, NBAND)
    flat = filtered.reshape(ELEMS * BMAX, NBAND).astype(jnp.float32)
    margin = jnp.dot(flat.T, flat, precision=lax.Precision.HIGHEST, preferred_element_type=jnp.float32)
    margin = margin / jnp.float32(ELEMS * BMAX)
    return filtered, margin
```

```python
import jax
import jax.numpy as jnp
from jax import lax
from jax.experimental import pallas as pl
from jax.experimental.pallas import tpu as pltpu
from jax.sharding import Mesh
from jax.sharding import PartitionSpec as P

BMAX = 64
EL = 32
GY = 16
BD = 256
NB = 2048
ROWS = GY * BMAX
CH = 4
NCH = GY // CH

CENTER = 0.3
SCALE = 2.0 / 1.7

ELEM = ("zl", "y", "c")
BAND = ("zh", "x")
BF = jnp.bfloat16
F32 = jnp.float32
MESH_ID = pl.DeviceIdType.MESH


def tables_kernel(nb, sizes, tbl, slot, mark, rank):
    me = (lax.axis_index("zl") * 4 + lax.axis_index("y")) * 2 + lax.axis_index("c")

    def clear(i, _):
        mark[i] = 0
        return 0

    lax.fori_loop(0, 2 * EL, clear, 0)

    def place(i, ones):
        row = jnp.where(nb[i, 0] >> 5 == me, 1, 0)
        at = jnp.where(row == 1, GY + ones, i - ones)
        slot[i] = at
        tbl[at, 0] = i
        tbl[at, 1] = sizes[i]
        tbl[i, 6] = at
        mark[row * EL + (nb[i, row] & (EL - 1))] = 1
        return ones + row

    lax.fori_loop(0, EL, place, 0)

    def count(i, seen):
        rank[i] = seen
        return seen + mark[i]

    lax.fori_loop(0, 2 * EL, count, 0)

    def fill(i, _):
        at = slot[i]
        row = at >> 4
        tbl[at, 2] = slot[nb[i, 1 - row] & (EL - 1)]
        tbl[at, 3] = slot[nb[i, 2] & (EL - 1)]
        tbl[at, 4] = slot[nb[i, 3] & (EL - 1)]
        tbl[at, 5] = rank[row * EL + (nb[i, row] & (EL - 1))] - row * GY
        return 0

    lax.fori_loop(0, EL, fill, 0)


def make_tables(neighbours, basis_sizes):
    smem = pl.BlockSpec(memory_space=pltpu.SMEM)
    return pl.pallas_call(
        tables_kernel,
        out_shape=jax.ShapeDtypeStruct((EL, 8), jnp.int32),
        in_specs=[smem, smem],
        out_specs=smem,
        scratch_shapes=[
            pltpu.SMEM((EL,), jnp.int32),
            pltpu.SMEM((2 * EL,), jnp.int32),
            pltpu.SMEM((2 * EL,), jnp.int32),
        ],
    )(neighbours, basis_sizes)


def main_kernel(
    tbl, yc_h, yp_h, h_h, out_f, out_m,
    yc, yp, hv, cur0, cur1, far_p0, far_n0, far_p1, far_n1, acc, fil, outv, xg, pb, rc, s1, ry, s2, rz, mv,
    lsem, hsend, hrecv, zsend, zrecv, xsend, xrecv, csend, crecv, ysend, yrecv, rsend, rrecv,
):
    zl, y, c = (lax.axis_index(a) for a in ELEM)
    zh, x = (lax.axis_index(a) for a in BAND)
    z = zh * 4 + zl
    e = (zl * 4 + y) * 2 + c

    def elem_id(other):
        return {"zl": other // 8, "y": (other // 2) % 4, "c": other % 2}

    def z_id(other):
        return {"zh": other // 4, "zl": other % 4}

    nxt, prv = elem_id((e + 1) % 32), elem_id((e + 31) % 32)
    xp, xm = {"x": (x + 1) % 4}, {"x": (x + 3) % 4}

    def remote(src, dst, ss, rs, to):
        return pltpu.make_async_remote_copy(
            src_ref=src, dst_ref=dst, send_sem=ss, recv_sem=rs, device_id=to, device_id_type=MESH_ID
        )

    load_c = pltpu.make_async_copy(yc_h, yc, lsem.at[0])
    load_p = pltpu.make_async_copy(yp_h, yp, lsem.at[1])
    load_h = pltpu.make_async_copy(h_h, hv, lsem.at[2])
    load_c.start()
    load_h.start()
    load_p.start()

    barrier = pltpu.get_barrier_semaphore()
    partners = [nxt, prv, xp, xm]
    partners += [{"y": (y + d) % 4} for d in (1, 2, 3)]
    partners += [z_id((z + d) % 8) for d in range(1, 8)]
    for to in partners:
        pl.semaphore_signal(barrier, inc=1, device_id=to, device_id_type=MESH_ID)

    rows = lax.broadcasted_iota(jnp.int32, (BMAX, BD), 0)
    zero = jnp.zeros((BMAX, BD), BF)

    load_c.wait()

    def pack(p, _):
        value = yc[tbl[p, 0]].astype(F32)
        cur0[p] = jnp.where(rows < tbl[p, 1], value, 0.0).astype(BF)
        return 0

    lax.fori_loop(GY, EL, pack, 0)
    pl.semaphore_wait(barrier, len(partners))

    halo = ((far_p0, far_n0), (far_p1, far_n1))

    def halo_copies(cur, degree):
        up = remote(cur.at[pl.ds(GY, GY)], halo[degree][0], hsend.at[degree, 0], hrecv.at[degree, 0], nxt)
        down = remote(cur.at[pl.ds(0, GY)], halo[degree][1], hsend.at[degree, 1], hrecv.at[degree, 1], prv)
        return up, down

    up0, down0 = halo_copies(cur0, 0)
    up0.start()
    lax.fori_loop(0, GY, pack, 0)
    down0.start()
    load_h.wait()
    load_p.wait()

    def local_part(cur, prev_of, row):
        def one(p, _):
            i = tbl[p, 0]
            own, n2, n3, n4 = cur[p], cur[tbl[p, 2]], cur[tbl[p, 3]], cur[tbl[p, 4]]
            pair = [zero, n2] if row == 0 else [n2, zero]
            stack = jnp.concatenate([own] + pair + [n3, n4], axis=0)
            applied = jnp.dot(hv[i], stack, preferred_element_type=F32)
            acc[p] = SCALE * (applied - CENTER * own.astype(F32)) - prev_of(p, i).astype(F32)
            return 0

        lax.fori_loop(row * GY, row * GY + GY, one, 0)

    def full_value(p, row, degree):
        i = tbl[p, 0]
        far = halo[degree][row][tbl[p, 5]]
        if row == 0:
            applied = jnp.dot(hv[i, :, 0:128], jnp.concatenate([zero, far], axis=0), preferred_element_type=F32)
        else:
            applied = jnp.dot(hv[i, :, 128:256], jnp.concatenate([far, zero], axis=0), preferred_element_type=F32)
        return jnp.where(rows < tbl[p, 1], acc[p] + SCALE * applied, 0.0).astype(BF)

    for row in (1, 0):
        local_part(cur0, lambda p, i: yp[i], row)

    up1, down1 = halo_copies(cur1, 1)

    def first(row):
        def one(p, _):
            cur1[p] = full_value(p, row, 0)
            return 0

        lax.fori_loop(row * GY, row * GY + GY, one, 0)

    down0.wait_recv()
    first(1)
    up1.start()
    up0.wait_recv()
    first(0)
    down1.start()

    for row in (1, 0):
        local_part(cur1, lambda p, i: cur0[p], row)
    down1.wait_recv()
    up1.wait_recv()

    def z_copy(half, j, src_zh):
        part = pl.ds(j * CH, CH)
        return remote(
            fil.at[pl.ds(half * GY + j * CH, CH)], xg.at[0, src_zh, part], zsend.at[half, j], zrecv.at[src_zh, j],
            z_id((zl + 2 + 4 * half) % 8),
        )

    def second(j, _):
        for row in (1, 0):
            for k in range(CH):
                p = row * GY + j * CH + k
                fil[p] = full_value(p, row, 1)
            z_copy(row, j, zh).start()
        return 0

    lax.fori_loop(0, NCH, second, 0)

    def put(i, _):
        s = tbl[i, 6]
        outv[i] = fil[s]
        return 0

    lax.fori_loop(0, EL, put, 0)
    store_f = pltpu.make_async_copy(outv, out_f, lsem.at[3])
    store_f.start()

    def x_copy(stage, j, h):
        part = pl.ds(j * CH, CH)
        src = 0 if stage < 2 else stage - 1
        dst = (1, 2, 3, 3)[stage]
        to = (xp, xm, xp, xm)[stage]
        sem = stage if stage < 2 else 2
        return remote(xg.at[src, h, part], xg.at[dst, h, part], xsend.at[sem, j, h], xrecv.at[sem, j, h], to)

    def forward(j):
        for h in (0, 1):
            x_copy(0, j, h).wait_recv()
            x_copy(1, j, h).wait_recv()
            x_copy(2 if j < NCH // 2 else 3, j, h).start()

    for j in range(NCH):
        for h in (0, 1):
            z_copy(0, j, h).wait_recv()
            x_copy(0, j, h).start()
            x_copy(1, j, h).start()
        if j > 0:
            forward(j - 1)
    forward(NCH - 1)

    def c_copy(b_a):
        at_zl, at_y = b_a // 2, pl.ds((b_a % 2) * 2, 2)
        return remote(
            pb.at[1 - c, at_zl, at_y], rc.at[at_zl, at_y], csend.at[b_a], crecv.at[b_a], {"c": 1 - c}
        )

    def product(slot, x_a):
        for zh_a in (0, 1):
            b_a = zh_a * 4 + x_a
            at_zl, at_y = b_a // 2, (b_a % 2) * 2
            for zh_b in (0, 1):
                tile = lax.dot_general(
                    xg[slot, zh_a].reshape(ROWS, BD), xg[0, zh_b].reshape(ROWS, BD), (((0,), (0,)), ((), ())), preferred_element_type=F32
                ).astype(BF)
                for s in range(4):
                    pb[s % 2, at_zl, at_y + s // 2, zh_b] = tile[s * 64 : s * 64 + 64]
            c_copy(b_a).start()

    x_of = [x, (x + 3) % 4, (x + 1) % 4, (x + 2) % 4]
    for slot in range(4):
        if slot == 3:
            for j in range(NCH):
                for h in (0, 1):
                    x_copy(2 if j < NCH // 2 else 3, j, h).wait_recv()
        product(slot, x_of[slot])

    for slot in range(4):
        for zh_a in (0, 1):
            b_a = zh_a * 4 + x_of[slot]
            at_zl, at_y = b_a // 2, pl.ds((b_a % 2) * 2, 2)
            c_copy(b_a).wait_recv()
            s1[at_zl, at_y] = (
                pb[c, at_zl, at_y].astype(F32) + rc[at_zl, at_y].astype(F32)
            ).astype(BF)

    def y_copy(d):
        to = (y + d) % 4
        return remote(s1.at[:, to], ry.at[d - 1], ysend.at[d - 1], yrecv.at[d - 1], {"y": to})

    for d in (2, 1, 3):
        y_copy(d).start()
    for d in (1, 3, 2):
        y_copy(d).wait_recv()
    for k in range(4):
        total = s1[k, y].astype(F32)
        for d in range(3):
            total = total + ry[d, k].astype(F32)
        s2[k] = total.astype(BF)

    def r_copy(d):
        to = (z + d) % 8
        return remote(s2.at[to % 4, to // 4], rz.at[d - 1], rsend.at[d - 1], rrecv.at[d - 1], z_id(to))

    for d in (4, 3, 5, 2, 6, 1, 7):
        r_copy(d).start()
    total = s2[zl, zh].astype(F32)
    for d in (1, 7, 2, 6, 3, 5, 4):
        r_copy(d).wait_recv()
        total = total + rz[d - 1].astype(F32)
    mv[...] = total * (1.0 / 65536.0)
    store_m = pltpu.make_async_copy(mv, out_m, lsem.at[4])
    store_m.start()

    for copy in (up0, down0, up1, down1):
        copy.wait_send()
    for j in range(NCH):
        for half in (0, 1):
            z_copy(half, j, zh).wait_send()
        for h in (0, 1):
            x_copy(0, j, h).wait_send()
            x_copy(1, j, h).wait_send()
            x_copy(2 if j < NCH // 2 else 3, j, h).wait_send()
    for b_a in range(8):
        c_copy(b_a).wait_send()
    for d in (1, 2, 3):
        y_copy(d).wait_send()
    for d in range(1, 8):
        r_copy(d).wait_send()
    store_f.wait()
    store_m.wait()


def on_device(y_current, y_previous, h_blocks, basis_sizes, neighbours):
    tbl = make_tables(neighbours, basis_sizes)
    any_space = pl.BlockSpec(memory_space=pl.ANY)
    dma = pltpu.SemaphoreType.DMA
    return pl.pallas_call(
        main_kernel,
        out_shape=(
            jax.ShapeDtypeStruct((EL, BMAX, BD), BF),
            jax.ShapeDtypeStruct((64, BD), F32),
        ),
        in_specs=[pl.BlockSpec(memory_space=pltpu.SMEM)] + [any_space] * 3,
        out_specs=(any_space, any_space),
        scratch_shapes=[
            pltpu.VMEM((EL, BMAX, BD), BF),
            pltpu.VMEM((EL, BMAX, BD), BF),
            pltpu.VMEM((EL, BMAX, 5 * BMAX), BF),
            pltpu.VMEM((EL, BMAX, BD), BF),
            pltpu.VMEM((EL, BMAX, BD), BF),
            *[pltpu.VMEM((GY, BMAX, BD), BF)] * 4,
            pltpu.VMEM((EL, BMAX, BD), F32),
            pltpu.VMEM((EL, BMAX, BD), BF),
            pltpu.VMEM((EL, BMAX, BD), BF),
            pltpu.VMEM((4, 2, GY, BMAX, BD), BF),
            pltpu.VMEM((2, 4, 4, 2, 64, BD), BF),
            pltpu.VMEM((4, 4, 2, 64, BD), BF),
            pltpu.VMEM((4, 4, 2, 64, BD), BF),
            pltpu.VMEM((3, 4, 2, 64, BD), BF),
            pltpu.VMEM((4, 2, 64, BD), BF),
            pltpu.VMEM((7, 64, BD), BF),
            pltpu.VMEM((64, BD), F32),
            dma((5,)),
            dma((2, 2)), dma((2, 2)),
            dma((2, NCH)), dma((2, NCH)),
            dma((3, NCH, 2)), dma((3, NCH, 2)),
            dma((8,)), dma((8,)),
            dma((3,)), dma((3,)),
            dma((7,)), dma((7,)),
        ],
        compiler_params=pltpu.CompilerParams(collective_id=0, has_side_effects=True),
    )(tbl, y_current, y_previous, h_blocks)


def solution(mesh):
    split = Mesh(mesh.devices.reshape(4, 4, 2, 2, 4), ELEM + BAND)
    return jax.shard_map(
        on_device,
        mesh=split,
        in_specs=(
            P(ELEM, None, BAND),
            P(ELEM, None, BAND),
            P(ELEM, None, None),
            P(ELEM),
            P(ELEM, None),
        ),
        out_specs=(P(ELEM, None, BAND), P(ELEM, BAND)),
        check_vma=False,
    )
```

```python
import jax
import jax.numpy as jnp
from jax import lax
from jax.experimental import pallas as pl
from jax.experimental.pallas import tpu as pltpu
from jax.sharding import Mesh
from jax.sharding import PartitionSpec as P

BMAX = 64
EL = 32
GY = 16
BD = 256
NB = 2048
ROWS = GY * BMAX
CH = 2
NCH = GY // CH
HALF = NCH // 2

CENTER = 0.3
SCALE = 2.0 / 1.7

ELEM = ("zl", "y", "c")
BAND = ("zh", "x")
BF = jnp.bfloat16
F32 = jnp.float32
MESH_ID = pl.DeviceIdType.MESH


def tables_kernel(nb, sizes, tbl, slot, mark, rank):
    me = (lax.axis_index("zl") * 4 + lax.axis_index("y")) * 2 + lax.axis_index("c")
    for i in range(2 * EL):
        mark[i] = 0
    ones = jnp.int32(0)
    rows = []
    for i in range(EL):
        row = jnp.where(nb[0, i] >> 5 == me, 1, 0)
        at = jnp.where(row == 1, GY + ones, i - ones)
        slot[i] = at
        tbl[at, 0] = i
        tbl[at, 1] = sizes[i]
        tbl[i, 6] = at
        mark[row * EL + (nb[row, i] & (EL - 1))] = 1
        ones = ones + row
        rows.append(row)
    seen = jnp.int32(0)
    for i in range(2 * EL):
        rank[i] = seen
        seen = seen + mark[i]
    for i in range(EL):
        at, row = slot[i], rows[i]
        tbl[at, 2] = slot[nb[1 - row, i] & (EL - 1)]
        tbl[at, 3] = slot[nb[2, i] & (EL - 1)]
        tbl[at, 4] = slot[nb[3, i] & (EL - 1)]
        tbl[at, 5] = rank[row * EL + (nb[row, i] & (EL - 1))] - row * GY


def make_tables(neighbours, basis_sizes):
    smem = pl.BlockSpec(memory_space=pltpu.SMEM)
    return pl.pallas_call(
        tables_kernel,
        out_shape=jax.ShapeDtypeStruct((EL, 8), jnp.int32),
        in_specs=[smem, smem],
        out_specs=smem,
        scratch_shapes=[
            pltpu.SMEM((EL,), jnp.int32),
            pltpu.SMEM((2 * EL,), jnp.int32),
            pltpu.SMEM((2 * EL,), jnp.int32),
        ],
        name="tables",
    )(neighbours.T, basis_sizes)


def main_kernel(
    tbl_h, yc_h, yp_h, h_h, out_f, out_m, tbl,
    yc, yp, hv, cur0, cur1, far_p0, far_n0, far_p1, far_n1, acc, fil, outv, xg, x1, x2, x3, pb, rc, s1, ry, s2, rz, mv, ft, fr,
    lsem, hsend, hrecv, zsend, zrecv, xsend, xrecv, gsend, grecv, csend, crecv, ysend, yrecv, rsend, rrecv, fsend, frecv,
):
    zl, y, c = (lax.axis_index(a) for a in ELEM)
    zh, x = (lax.axis_index(a) for a in BAND)
    z = zh * 4 + zl
    e = (zl * 4 + y) * 2 + c

    def elem_id(other):
        return {"zl": other // 8, "y": (other // 2) % 4, "c": other % 2}

    def z_id(other):
        return {"zh": other // 4, "zl": other % 4}

    nxt, prv = elem_id((e + 1) % 32), elem_id((e + 31) % 32)
    xp, xm = {"x": (x + 1) % 4}, {"x": (x + 3) % 4}

    def remote(src, dst, ss, rs, to):
        return pltpu.make_async_remote_copy(
            src_ref=src, dst_ref=dst, send_sem=ss, recv_sem=rs, device_id=to, device_id_type=MESH_ID
        )

    load_t = pltpu.make_async_copy(tbl_h, tbl, lsem.at[5])
    load_c = pltpu.make_async_copy(yc_h, yc, lsem.at[0])
    load_p = pltpu.make_async_copy(yp_h, yp, lsem.at[1])
    load_h = pltpu.make_async_copy(h_h, hv, lsem.at[2])
    load_t.start()
    load_c.start()
    load_h.start()
    load_p.start()

    barrier = pltpu.get_barrier_semaphore()
    partners = [nxt, prv, xp, xm]
    partners += [{"y": (y + d) % 4} for d in (1, 2, 3)]
    partners += [z_id((z + d) % 8) for d in range(1, 8)]
    for to in partners:
        pl.semaphore_signal(barrier, inc=1, device_id=to, device_id_type=MESH_ID)

    b_own, b_rows, s_rows = zh * 4 + x, e // 4, e % 4
    mirrored = b_rows % 4 != x

    def mirror_id(s):
        return {**elem_id(4 * b_own + s), "zh": b_rows // 4, "x": b_rows % 4}

    @pl.when(mirrored)
    def _():
        for s in range(4):
            pl.semaphore_signal(barrier, inc=1, device_id=mirror_id(s), device_id_type=MESH_ID)


    rows = lax.broadcasted_iota(jnp.int32, (BMAX, BD), 0)
    zero = jnp.zeros((BMAX, BD), BF)

    with jax.named_scope('w_load'):
        load_t.wait()
        load_c.wait()

    def pack(p, _):
        value = yc[tbl[p, 0]].astype(F32)
        cur0[p] = jnp.where(rows < tbl[p, 1], value, 0.0).astype(BF)
        return 0

    with jax.named_scope('pack1'):
        lax.fori_loop(GY, EL, pack, 0, unroll=4)
    with jax.named_scope('barrier'):
        pl.semaphore_wait(barrier, len(partners) + 4 * mirrored.astype(jnp.int32))

    halo = ((far_p0, far_n0), (far_p1, far_n1))

    def halo_copies(cur, degree):
        up = remote(cur.at[pl.ds(GY, GY)], halo[degree][0], hsend.at[degree, 0], hrecv.at[degree, 0], nxt)
        down = remote(cur.at[pl.ds(0, GY)], halo[degree][1], hsend.at[degree, 1], hrecv.at[degree, 1], prv)
        return up, down

    up0, down0 = halo_copies(cur0, 0)
    up0.start()
    with jax.named_scope('pack0'):
        lax.fori_loop(0, GY, pack, 0, unroll=4)
    down0.start()
    load_h.wait()
    load_p.wait()

    def local_part(cur, prev_of, row):
        def one(p, _):
            i = tbl[p, 0]
            own, n2, n3, n4 = cur[p], cur[tbl[p, 2]], cur[tbl[p, 3]], cur[tbl[p, 4]]
            pair = [zero, n2] if row == 0 else [n2, zero]
            stack = jnp.concatenate([own] + pair + [n3, n4], axis=0)
            applied = jnp.dot(hv[i], stack, preferred_element_type=F32)
            acc[p] = SCALE * (applied - CENTER * own.astype(F32)) - prev_of(p, i).astype(F32)
            return 0

        lax.fori_loop(row * GY, row * GY + GY, one, 0, unroll=8)

    def full_value(p, row, degree):
        i = tbl[p, 0]
        far = halo[degree][row][tbl[p, 5]]
        if row == 0:
            applied = jnp.dot(hv[i, :, 0:128], jnp.concatenate([zero, far], axis=0), preferred_element_type=F32)
        else:
            applied = jnp.dot(hv[i, :, 128:256], jnp.concatenate([far, zero], axis=0), preferred_element_type=F32)
        return jnp.where(rows < tbl[p, 1], acc[p] + SCALE * applied, 0.0).astype(BF)

    with jax.named_scope('local0'):
      for row in (1, 0):
        local_part(cur0, lambda p, i: yp[i], row)

    up1, down1 = halo_copies(cur1, 1)

    def first(row):
        def one(p, _):
            cur1[p] = full_value(p, row, 0)
            return 0

        lax.fori_loop(row * GY, row * GY + GY, one, 0, unroll=8)

    with jax.named_scope('w_halo0'):
        down0.wait_recv()
    with jax.named_scope('first1'):
        first(1)
    up1.start()
    with jax.named_scope('w_halo0b'):
        up0.wait_recv()
    with jax.named_scope('first0'):
        first(0)
    down1.start()

    with jax.named_scope('local1'):
      for row in (1, 0):
        local_part(cur1, lambda p, i: cur0[p], row)
    with jax.named_scope('w_halo1'):
        down1.wait_recv()
        up1.wait_recv()

    def swap(front, k):
        return 2 * (front + (k // 2) * (1 - 2 * front)) + k % 2

    def piece(k, front):
        return (k % 2) * HALF + swap(front, k // 2)

    to_pass = ((x + 2) % 4) // 2

    def z_copy(half, k, src_zh):
        j = piece(k, to_pass)
        return remote(
            fil.at[pl.ds(half * GY + j * CH, CH)], xg.at[src_zh, pl.ds(j * CH, CH)],
            zsend.at[half, k], zrecv.at[src_zh, k], z_id((zl + 2 + 4 * half) % 8),
        )

    def second(kk, _):
        for k in (2 * kk, 2 * kk + 1):
            for row in (1, 0):
                for m in range(CH):
                    p = row * GY + piece(k, to_pass) * CH + m
                    fil[p] = full_value(p, row, 1)
        for k in (2 * kk, 2 * kk + 1):
            for row in (1, 0):
                z_copy(row, k, zh).start()
        return 0

    with jax.named_scope('second'):
        lax.fori_loop(0, HALF, second, 0)

    def put(i, _):
        s = tbl[i, 6]
        outv[i] = fil[s]
        return 0

    with jax.named_scope('put'):
        lax.fori_loop(0, EL, put, 0, unroll=4)
    store_f = pltpu.make_async_copy(outv, out_f, lsem.at[3])
    store_f.start()

    def x_copy(way, q, h, front):
        at = swap(front, q) * CH
        return remote(
            xg.at[h, pl.ds(way * HALF * CH + at, CH)], (x1, x2)[way].at[h, pl.ds(at, CH)],
            xsend.at[way, q, h], xrecv.at[way, q, h], (xp, xm)[way],
        )

    came = (((x + 1) % 4) // 2, ((x + 3) % 4) // 2)

    def pass_on(way, q, h):
        at = swap(came[way], q) * CH
        return remote(
            (x1, x2)[way].at[h, pl.ds(at, CH)], x3.at[h, way, pl.ds(q * CH, CH)],
            gsend.at[way, q, h], grecv.at[way, q, h], (xp, xm)[way],
        )

    for k in range(NCH):
        way, q = k % 2, k // 2
        for h in (0, 1):
            with jax.named_scope(f'wz{k}{h}'):
                z_copy(0, k, h).wait_recv()
            x_copy(way, q, h, to_pass).start()
        if 2 <= k < 6:
            way, q = k % 2, k // 2 - 1
            for h in (0, 1):
                with jax.named_scope(f'wx{k}{h}'):
                    x_copy(way, q, h, came[way]).wait_recv()
                pass_on(way, q, h).start()

    def c_copy(b_a):
        at_zl, at_y = b_a // 2, pl.ds((b_a % 2) * 2, 2)
        return remote(
            pb.at[1 - c, at_zl, at_y], rc.at[at_zl, at_y], csend.at[b_a], crecv.at[b_a], {"c": 1 - c}
        )

    def product(x_a, left, right):
        for zh_a in (0, 1):
            b_a = zh_a * 4 + x_a
            at_zl, at_y = b_a // 2, (b_a % 2) * 2
            for zh_b in (0, 1):
                tile = lax.dot_general(
                    left(zh_a).reshape(-1, BD), right(zh_b).reshape(-1, BD), (((0,), (0,)), ((), ())),
                    preferred_element_type=F32,
                ).astype(BF)
                for s in range(4):
                    pb[s % 2, at_zl, at_y + s // 2, zh_b] = tile[s * 64 : s * 64 + 64]
            c_copy(b_a).start()

    def settle(x_a):
        for zh_a in (0, 1):
            b_a = zh_a * 4 + x_a
            at_zl, at_y = b_a // 2, pl.ds((b_a % 2) * 2, 2)
            with jax.named_scope(f'wc{zh_a}'):
                c_copy(b_a).wait_recv()
            s1[at_zl, at_y] = (
                pb[c, at_zl, at_y].astype(F32) + rc[at_zl, at_y].astype(F32)
            ).astype(BF)

    def y_copy(to, d):
        return remote(s1.at[:, to], ry.at[d - 1], ysend.at[d - 1], yrecv.at[d - 1], {"y": to})

    def y_start(parity):
        for k in (0, 1):
            to = parity * 2 + k

            @pl.when(to != y)
            def _():
                y_copy(to, (to + 4 - y) % 4).start()

    quarter = (x // 2) * GY // 4
    x_far, x_prev, x_next = (x + 2) % 4, (x + 3) % 4, (x + 1) % 4

    with jax.named_scope('prod_own'):
        product(x, lambda h: xg[h], lambda h: xg[h])
    with jax.named_scope('w_pass'):
        for way in (0, 1):
            for q in (0, 1):
                for h in (0, 1):
                    pass_on(way, q, h).wait_recv()
    with jax.named_scope('prod_far'):
        product(
            x_far, lambda h: x3[h],
            lambda h: jnp.concatenate([xg[h, pl.ds(quarter, 4)], xg[h, pl.ds(GY // 2 + quarter, 4)]], axis=0),
        )
    settle(x)
    settle(x_far)
    y_start(x % 2)
    for way in (0, 1):
        with jax.named_scope(f'w_x{way}'):
            for q in (2, 3):
                for h in (0, 1):
                    x_copy(way, q, h, came[way]).wait_recv()
        part = pl.ds(way * GY // 2, GY // 2)
        with jax.named_scope(f'prod_x{way}'):
            product((x_prev, x_next)[way], lambda h: (x1, x2)[way][h], lambda h: xg[h, part])
    settle(x_prev)
    settle(x_next)
    y_start(1 - x % 2)

    for d in (1, 3, 2):
        with jax.named_scope(f'wy{d}'):
            y_copy((y + d) % 4, d).wait_recv()
    for k in range(4):
        total = s1[k, y].astype(F32)
        for d in range(3):
            total = total + ry[d, k].astype(F32)
        s2[k] = total.astype(BF)

    def r_copy(d):
        to = (z + d) % 8
        return remote(s2.at[to % 4, to // 4], rz.at[d - 1], rsend.at[d - 1], rrecv.at[d - 1], z_id(to))

    for d in (4, 3, 5, 2, 6, 1, 7):
        r_copy(d).start()
    total = s2[zl, zh].astype(F32)
    for d in (1, 7, 2, 6, 3, 5, 4):
        with jax.named_scope(f'wr{d}'):
            r_copy(d).wait_recv()
        total = total + rz[d - 1].astype(F32)
    total = total * (1.0 / 65536.0)
    mv[...] = total

    def f_copy(s, recv):
        return remote(ft.at[s], fr.at[recv], fsend.at[s], frecv.at[recv], mirror_id(s))

    @pl.when(mirrored)
    def _():
        turned = total.T.astype(BF)
        for s in range(4):
            ft[s] = turned[s * 64 : s * 64 + 64]
            f_copy(s, s_rows).start()
        with jax.named_scope('w_mirror'):
            for s in range(4):
                f_copy(s, s).wait_recv()
        mv[...] = mv[...] + jnp.concatenate([fr[s].astype(F32) for s in range(4)], axis=1)
        for s in range(4):
            f_copy(s, s_rows).wait_send()

    store_m = pltpu.make_async_copy(mv, out_m, lsem.at[4])
    store_m.start()

    with jax.named_scope('tail'):
      for copy in (up0, down0, up1, down1):
        copy.wait_send()
    for k in range(NCH):
        for h in (0, 1):
            z_copy(h, k, zh).wait_send()
            x_copy(k % 2, k // 2, h, to_pass).wait_send()
    for way in (0, 1):
        for q in (0, 1):
            for h in (0, 1):
                pass_on(way, q, h).wait_send()
    for b_a in range(8):
        c_copy(b_a).wait_send()
    for d in (1, 2, 3):
        y_copy((y + d) % 4, d).wait_send()
    for d in range(1, 8):
        r_copy(d).wait_send()
    store_f.wait()
    store_m.wait()


def on_device(y_current, y_previous, h_blocks, basis_sizes, neighbours):
    tbl = make_tables(neighbours, basis_sizes)
    any_space = pl.BlockSpec(memory_space=pl.ANY)
    dma = pltpu.SemaphoreType.DMA
    return pl.pallas_call(
        main_kernel,
        out_shape=(
            jax.ShapeDtypeStruct((EL, BMAX, BD), BF),
            jax.ShapeDtypeStruct((64, BD), F32),
        ),
        in_specs=[any_space] * 4,
        out_specs=(any_space, any_space),
        scratch_shapes=[
            pltpu.SMEM((EL, 8), jnp.int32),
            pltpu.VMEM((EL, BMAX, BD), BF),
            pltpu.VMEM((EL, BMAX, BD), BF),
            pltpu.VMEM((EL, BMAX, 5 * BMAX), BF),
            pltpu.VMEM((EL, BMAX, BD), BF),
            pltpu.VMEM((EL, BMAX, BD), BF),
            *[pltpu.VMEM((GY, BMAX, BD), BF)] * 4,
            pltpu.VMEM((EL, BMAX, BD), F32),
            pltpu.VMEM((EL, BMAX, BD), BF),
            pltpu.VMEM((EL, BMAX, BD), BF),
            pltpu.VMEM((2, GY, BMAX, BD), BF),
            pltpu.VMEM((2, GY // 2, BMAX, BD), BF),
            pltpu.VMEM((2, GY // 2, BMAX, BD), BF),
            pltpu.VMEM((2, 2, GY // 4, BMAX, BD), BF),
            pltpu.VMEM((2, 4, 4, 2, 64, BD), BF),
            pltpu.VMEM((4, 4, 2, 64, BD), BF),
            pltpu.VMEM((4, 4, 2, 64, BD), BF),
            pltpu.VMEM((3, 4, 2, 64, BD), BF),
            pltpu.VMEM((4, 2, 64, BD), BF),
            pltpu.VMEM((7, 64, BD), BF),
            pltpu.VMEM((64, BD), F32),
            pltpu.VMEM((4, 64, 64), BF),
            pltpu.VMEM((4, 64, 64), BF),
            dma((6,)),
            dma((2, 2)), dma((2, 2)),
            dma((2, NCH)), dma((2, NCH)),
            dma((2, HALF, 2)), dma((2, HALF, 2)),
            dma((2, 2, 2)), dma((2, 2, 2)),
            dma((8,)), dma((8,)),
            dma((3,)), dma((3,)),
            dma((7,)), dma((7,)),
            dma((4,)), dma((4,)),
        ],
        compiler_params=pltpu.CompilerParams(collective_id=0, has_side_effects=True),
        name="chain",
    )(tbl, y_current, y_previous, h_blocks)


def solution(mesh):
    split = Mesh(mesh.devices.reshape(4, 4, 2, 2, 4), ELEM + BAND)
    return jax.shard_map(
        on_device,
        mesh=split,
        in_specs=(
            P(ELEM, None, BAND),
            P(ELEM, None, BAND),
            P(ELEM, None, None),
            P(ELEM),
            P(ELEM, None),
        ),
        out_specs=(P(ELEM, None, BAND), P(ELEM, BAND)),
        check_vma=False,
    )
```

```python
import jax
import jax.numpy as jnp
from jax import lax
from jax.experimental import pallas as pl
from jax.experimental.pallas import tpu as pltpu
from jax.sharding import Mesh
from jax.sharding import PartitionSpec as P

BMAX = 64
EL = 32
GY = 16
BD = 256
NB = 2048
ROWS = GY * BMAX
HB = 128
CH = 4
NCH = GY // CH
ORDER = (0, 2, 1, 3)

CENTER = 0.3
SCALE = 2.0 / 1.7

ELEM = ("zl", "y", "c")
BAND = ("zh", "x")
BF = jnp.bfloat16
F32 = jnp.float32
MESH_ID = pl.DeviceIdType.MESH


def tables_kernel(nb, sizes, tbl, slot, mark, rank):
    me = (lax.axis_index("zl") * 4 + lax.axis_index("y")) * 2 + lax.axis_index("c")
    for i in range(2 * EL):
        mark[i] = 0
    ones = jnp.int32(0)
    rows = []
    for i in range(EL):
        row = jnp.where(nb[0, i] >> 5 == me, 1, 0)
        at = jnp.where(row == 1, GY + ones, i - ones)
        slot[i] = at
        tbl[at, 0] = i
        tbl[at, 1] = sizes[i]
        tbl[i, 6] = at
        mark[row * EL + (nb[row, i] & (EL - 1))] = 1
        ones = ones + row
        rows.append(row)
    seen = jnp.int32(0)
    for i in range(2 * EL):
        rank[i] = seen
        seen = seen + mark[i]
    for i in range(EL):
        at, row = slot[i], rows[i]
        tbl[at, 2] = slot[nb[1 - row, i] & (EL - 1)]
        tbl[at, 3] = slot[nb[2, i] & (EL - 1)]
        tbl[at, 4] = slot[nb[3, i] & (EL - 1)]
        tbl[at, 5] = rank[row * EL + (nb[row, i] & (EL - 1))] - row * GY


def make_tables(neighbours, basis_sizes):
    smem = pl.BlockSpec(memory_space=pltpu.SMEM)
    return pl.pallas_call(
        tables_kernel,
        out_shape=jax.ShapeDtypeStruct((EL, 8), jnp.int32),
        in_specs=[smem, smem],
        out_specs=smem,
        scratch_shapes=[
            pltpu.SMEM((EL,), jnp.int32),
            pltpu.SMEM((2 * EL,), jnp.int32),
            pltpu.SMEM((2 * EL,), jnp.int32),
        ],
        name="tables",
    )(neighbours.T, basis_sizes)


def main_kernel(
    tbl_h, yc_h, yp_h, h_h, out_f, out_m, tbl,
    yc, yp, hv, cur0, cur1, f000, f001, f010, f011, f100, f101, f110, f111,
    acc, fil, outv, xg, x1, x2, x3, pb, rc, s1, ry, s2, rz, mv,
    lsem, hsend, hrecv, zsend, zrecv, xsend, xrecv, gsend, grecv, csend, crecv, ysend, yrecv, rsend, rrecv,
):
    zl, y, c = (lax.axis_index(a) for a in ELEM)
    zh, x = (lax.axis_index(a) for a in BAND)
    z = zh * 4 + zl
    e = (zl * 4 + y) * 2 + c

    def elem_id(other):
        return {"zl": other // 8, "y": (other // 2) % 4, "c": other % 2}

    def z_id(other):
        return {"zh": other // 4, "zl": other % 4}

    nxt, prv = elem_id((e + 1) % 32), elem_id((e + 31) % 32)
    x_prev, x_next, x_far = (x + 3) % 4, (x + 1) % 4, (x + 2) % 4
    xp, xm = {"x": x_next}, {"x": x_prev}

    def remote(src, dst, ss, rs, to):
        return pltpu.make_async_remote_copy(
            src_ref=src, dst_ref=dst, send_sem=ss, recv_sem=rs, device_id=to, device_id_type=MESH_ID
        )

    loads = [
        pltpu.make_async_copy(src, dst, lsem.at[k])
        for k, (src, dst) in enumerate(
            [(tbl_h, tbl)]
            + [(yc_h.at[:, :, pl.ds(b * HB, HB)], yc.at[b]) for b in (0, 1)]
            + [(h_h, hv)]
            + [(yp_h.at[:, :, pl.ds(b * HB, HB)], yp.at[b]) for b in (0, 1)]
        )
    ]
    for load in loads:
        load.start()

    barrier = pltpu.get_barrier_semaphore()
    partners = [nxt, prv, xp, xm]
    partners += [{"y": (y + d) % 4} for d in (1, 2, 3)]
    partners += [z_id((z + d) % 8) for d in range(1, 8)]
    for to in partners:
        pl.semaphore_signal(barrier, inc=1, device_id=to, device_id_type=MESH_ID)

    rows = lax.broadcasted_iota(jnp.int32, (BMAX, HB), 0)
    zero = jnp.zeros((BMAX, HB), BF)

    with jax.named_scope('w_load'):
        for load in loads[:3]:
            load.wait()

    def pack(row, b):
        def one(p, _):
            value = yc[b, tbl[p, 0]].astype(F32)
            cur0[b, p] = jnp.where(rows < tbl[p, 1], value, 0.0).astype(BF)
            return 0

        lax.fori_loop(row * GY, row * GY + GY, one, 0, unroll=4)

    halo = (((f000, f001), (f010, f011)), ((f100, f101), (f110, f111)))

    def halo_copy(degree, row, b):
        return remote(
            (cur0, cur1)[degree].at[b, pl.ds((1 - row) * GY, GY)], halo[degree][row][b],
            hsend.at[degree, row, b], hrecv.at[degree, row, b], (nxt, prv)[row],
        )

    with jax.named_scope('pack'):
        pack(1, 0)
    with jax.named_scope('barrier'):
        pl.semaphore_wait(barrier, len(partners))
    halo_copy(0, 0, 0).start()
    pack(0, 0)
    halo_copy(0, 1, 0).start()
    pack(1, 1)
    halo_copy(0, 0, 1).start()
    pack(0, 1)
    halo_copy(0, 1, 1).start()
    for load in loads[3:]:
        load.wait()

    def local_part(degree, row, b):
        cur = (cur0, cur1)[degree]

        def one(p, _):
            i = tbl[p, 0]
            own, n2, n3, n4 = cur[b, p], cur[b, tbl[p, 2]], cur[b, tbl[p, 3]], cur[b, tbl[p, 4]]
            pair = [zero, n2] if row == 0 else [n2, zero]
            stack = jnp.concatenate([own] + pair + [n3, n4], axis=0)
            applied = jnp.dot(hv[i], stack, preferred_element_type=F32)
            before = yp[b, i] if degree == 0 else cur0[b, p]
            acc[b, p] = SCALE * (applied - CENTER * own.astype(F32)) - before.astype(F32)
            return 0

        lax.fori_loop(row * GY, row * GY + GY, one, 0, unroll=8)

    def full_value(degree, row, b, p):
        i = tbl[p, 0]
        far = halo[degree][row][b][tbl[p, 5]]
        if row == 0:
            applied = jnp.dot(hv[i, :, 0:128], jnp.concatenate([zero, far], axis=0), preferred_element_type=F32)
        else:
            applied = jnp.dot(hv[i, :, 128:256], jnp.concatenate([far, zero], axis=0), preferred_element_type=F32)
        return jnp.where(rows < tbl[p, 1], acc[b, p] + SCALE * applied, 0.0).astype(BF)

    def first(row, b):
        def one(p, _):
            cur1[b, p] = full_value(0, row, b, p)
            return 0

        lax.fori_loop(row * GY, row * GY + GY, one, 0, unroll=8)

    def z_copy(half, b, j, src_zh):
        return remote(
            fil.at[b, pl.ds(half * GY + j * CH, CH)], xg.at[b, src_zh, pl.ds(j * CH, CH)],
            zsend.at[half, b, j], zrecv.at[src_zh, b, j], z_id((zl + 2 + 4 * half) % 8),
        )

    def second(b):
        def one(k, _):
            j = (k % 2) * 2 + k // 2
            for row in (1, 0):
                for m in range(CH):
                    p = row * GY + j * CH + m
                    fil[b, p] = full_value(1, row, b, p)
            for row in (1, 0):
                z_copy(row, b, j, zh).start()
            return 0

        lax.fori_loop(0, NCH, one, 0)

    for b in (0, 1):
        with jax.named_scope(f'local0{b}'):
            local_part(0, 1, b)
            local_part(0, 0, b)
    for b in (0, 1):
        with jax.named_scope(f'w_h0{b}1'):
            halo_copy(0, 1, b).wait_recv()
        first(1, b)
        halo_copy(1, 0, b).start()
        with jax.named_scope(f'w_h0{b}0'):
            halo_copy(0, 0, b).wait_recv()
        first(0, b)
        halo_copy(1, 1, b).start()
        with jax.named_scope(f'local1{b}'):
            local_part(1, 1, b)
            local_part(1, 0, b)
    for b in (0, 1):
        with jax.named_scope(f'w_h1{b}'):
            halo_copy(1, 1, b).wait_recv()
            halo_copy(1, 0, b).wait_recv()
        with jax.named_scope(f'second{b}'):
            second(b)

    def put(i, _):
        s = tbl[i, 6]
        outv[i] = jnp.concatenate([fil[0, s], fil[1, s]], axis=1)
        return 0

    with jax.named_scope('put'):
        lax.fori_loop(0, EL, put, 0, unroll=4)
    store_f = pltpu.make_async_copy(outv, out_f, lsem.at[6])
    store_f.start()

    def x_copy(way, b, j, h):
        part = pl.ds(j * CH, CH)
        return remote(
            xg.at[b, h, part], (x1, x2)[way].at[b, h, part],
            xsend.at[way, b, j, h], xrecv.at[way, b, j, h], (xp, xm)[way],
        )

    def pass_on(b, j, h):
        part, way = pl.ds(j * CH, CH), j // 2
        return remote(
            (x1, x2)[way].at[b, h, part], x3.at[b, h, part], gsend.at[b, j, h], grecv.at[b, j, h], (xp, xm)[way]
        )

    for b in (0, 1):
        for j in ORDER:
            for h in (0, 1):
                with jax.named_scope(f'wz{b}{j}{h}'):
                    z_copy(0, b, j, h).wait_recv()
                x_copy(0, b, j, h).start()
                x_copy(1, b, j, h).start()

    def pass_half(b):
        for j in ORDER:
            for h in (0, 1):
                with jax.named_scope(f'wx{b}{j}{h}'):
                    x_copy(j // 2, b, j, h).wait_recv()
                pass_on(b, j, h).start()

    def c_copy(x_a, zh_a):
        at = (zh_a, x_a // 2, pl.ds((x_a % 2) * 2, 2))
        return remote(pb.at[(1 - c, *at)], rc.at[at], csend.at[x_a, zh_a], crecv.at[x_a, zh_a], {"c": 1 - c})

    def whole(ref, h):
        return jnp.concatenate([ref[b, h].reshape(GY * BMAX, HB) for b in (0, 1)], axis=1)

    def product(x_a, ref):
        for zh_a in (0, 1):
            for zh_b in (0, 1):
                tile = lax.dot_general(
                    whole(ref, zh_a), whole(xg, zh_b), (((0,), (0,)), ((), ())), preferred_element_type=F32
                ).astype(BF)
                for s in range(4):
                    pb[s % 2, zh_a, x_a // 2, (x_a % 2) * 2 + s // 2, zh_b] = tile[s * 64 : s * 64 + 64]
            c_copy(x_a, zh_a).start()

    def y_copy(to, d, xh):
        return remote(
            s1.at[:, xh, to], ry.at[d - 1, xh], ysend.at[d - 1, xh], yrecv.at[d - 1, xh], {"y": to}
        )

    def settle(x_a):
        xh, pair = x_a // 2, pl.ds((x_a % 2) * 2, 2)
        for zh_a in (0, 1):
            with jax.named_scope(f'wc{zh_a}'):
                c_copy(x_a, zh_a).wait_recv()
            s1[zh_a, xh, pair] = (
                pb[c, zh_a, xh, pair].astype(F32) + rc[zh_a, xh, pair].astype(F32)
            ).astype(BF)
        for k in (0, 1):
            to = (x_a % 2) * 2 + k

            @pl.when(to != y)
            def _():
                y_copy(to, (to + 4 - y) % 4, xh).start()

    def r_copy(to, src_xh):
        d = (to + 8 - z) % 8
        return remote(
            s2.at[src_xh, (to % 4) // 2, to // 4], rz.at[d - 1], rsend.at[d - 1], rrecv.at[d - 1], z_id(to)
        )

    def gather_y(xh):
        for d in (1, 3, 2):
            y_copy((y + d) % 4, d, xh).wait_recv()
        for zh_a in (0, 1):
            total = s1[zh_a, xh, y].astype(F32)
            for d in range(3):
                total = total + ry[d, xh, zh_a].astype(F32)
            s2[xh, zh_a] = total.astype(BF)
        for zh_a in (0, 1):
            for zh_b in (0, 1):
                to = zh_b * 4 + zh_a * 2 + xh

                @pl.when(to != z)
                def _():
                    r_copy(to, xh).start()

    same = y // 2 == x % 2
    pass_half(0)
    with jax.named_scope('prod_own'):
        product(x, xg)
    pass_half(1)
    settle(x)
    for way in (0, 1):
        with jax.named_scope(f'w_x{way}'):
            for b in (0, 1):
                for j in ((2, 3), (0, 1))[way]:
                    for h in (0, 1):
                        x_copy(way, b, j, h).wait_recv()
        with jax.named_scope(f'prod_x{way}'):
            product((x_prev, x_next)[way], (x1, x2)[way])
    settle(x_prev)
    settle(x_next)

    with jax.named_scope('gather_y1'):
        @pl.when(same)
        def _():
            gather_y(x // 2)

        @pl.when(jnp.logical_not(same))
        def _():
            gather_y(0)
            gather_y(1)

    with jax.named_scope('w_far'):
        for b in (0, 1):
            for j in ORDER:
                for h in (0, 1):
                    pass_on(b, j, h).wait_recv()
    with jax.named_scope('prod_far'):
        product(x_far, x3)
    settle(x_far)

    with jax.named_scope('gather_y2'):
        @pl.when(same)
        def _():
            gather_y(1 - x // 2)

    total = s2[zl % 2, zl // 2, zh].astype(F32)
    for d in (1, 7, 2, 6, 3, 5, 4):
        with jax.named_scope(f'wr{d}'):
            r_copy((z + d) % 8, 0).wait_recv()
        total = total + rz[d - 1].astype(F32)
    mv[...] = total * (1.0 / 65536.0)
    store_m = pltpu.make_async_copy(mv, out_m, lsem.at[7])
    store_m.start()

    with jax.named_scope('tail'):
        for degree in (0, 1):
            for row in (0, 1):
                for b in (0, 1):
                    halo_copy(degree, row, b).wait_send()
        for b in (0, 1):
            for j in range(NCH):
                for h in (0, 1):
                    z_copy(h, b, j, zh).wait_send()
                    x_copy(0, b, j, h).wait_send()
                    x_copy(1, b, j, h).wait_send()
                    pass_on(b, j, h).wait_send()
        for x_a in range(4):
            for zh_a in (0, 1):
                c_copy(x_a, zh_a).wait_send()
        for d in (1, 2, 3):
            for xh in (0, 1):
                y_copy((y + d) % 4, d, xh).wait_send()
        for d in range(1, 8):
            r_copy((z + d) % 8, 0).wait_send()
        store_f.wait()
        store_m.wait()


def on_device(y_current, y_previous, h_blocks, basis_sizes, neighbours):
    tbl = make_tables(neighbours, basis_sizes)
    any_space = pl.BlockSpec(memory_space=pl.ANY)
    dma = pltpu.SemaphoreType.DMA
    halves = pltpu.VMEM((2, EL, BMAX, HB), BF)
    met = pltpu.VMEM((2, 2, GY, BMAX, HB), BF)
    return pl.pallas_call(
        main_kernel,
        out_shape=(
            jax.ShapeDtypeStruct((EL, BMAX, BD), BF),
            jax.ShapeDtypeStruct((64, BD), F32),
        ),
        in_specs=[any_space] * 4,
        out_specs=(any_space, any_space),
        scratch_shapes=[
            pltpu.SMEM((EL, 8), jnp.int32),
            halves,
            halves,
            pltpu.VMEM((EL, BMAX, 5 * BMAX), BF),
            halves,
            halves,
            *[pltpu.VMEM((GY, BMAX, HB), BF)] * 8,
            pltpu.VMEM((2, EL, BMAX, HB), F32),
            halves,
            pltpu.VMEM((EL, BMAX, BD), BF),
            met,
            met,
            met,
            met,
            pltpu.VMEM((2, 2, 2, 4, 2, 64, BD), BF),
            pltpu.VMEM((2, 2, 4, 2, 64, BD), BF),
            pltpu.VMEM((2, 2, 4, 2, 64, BD), BF),
            pltpu.VMEM((3, 2, 2, 2, 64, BD), BF),
            pltpu.VMEM((2, 2, 2, 64, BD), BF),
            pltpu.VMEM((7, 64, BD), BF),
            pltpu.VMEM((64, BD), F32),
            dma((8,)),
            dma((2, 2, 2)), dma((2, 2, 2)),
            dma((2, 2, NCH)), dma((2, 2, NCH)),
            dma((2, 2, NCH, 2)), dma((2, 2, NCH, 2)),
            dma((2, NCH, 2)), dma((2, NCH, 2)),
            dma((4, 2)), dma((4, 2)),
            dma((3, 2)), dma((3, 2)),
            dma((7,)), dma((7,)),
        ],
        compiler_params=pltpu.CompilerParams(collective_id=0, has_side_effects=True),
        name="chain",
    )(tbl, y_current, y_previous, h_blocks)


def solution(mesh):
    split = Mesh(mesh.devices.reshape(4, 4, 2, 2, 4), ELEM + BAND)
    return jax.shard_map(
        on_device,
        mesh=split,
        in_specs=(
            P(ELEM, None, BAND),
            P(ELEM, None, BAND),
            P(ELEM, None, None),
            P(ELEM),
            P(ELEM, None),
        ),
        out_specs=(P(ELEM, None, BAND), P(ELEM, BAND)),
        check_vma=False,
    )
```

```python
import jax
import jax.numpy as jnp
from jax import lax
from jax.experimental import pallas as pl
from jax.experimental.pallas import tpu as pltpu
from jax.sharding import Mesh
from jax.sharding import PartitionSpec as P

BMAX = 64
EL = 32
GY = 16
BD = 256
NB = 2048
ROWS = GY * BMAX
HB = 128
CH = 4
NCH = GY // CH
ORDER = (0, 2, 1, 3)

CENTER = 0.3
SCALE = 2.0 / 1.7

ELEM = ("zl", "y", "c")
BAND = ("zh", "x")
BF = jnp.bfloat16
F32 = jnp.float32
MESH_ID = pl.DeviceIdType.MESH


def tables_kernel(nb, sizes, tbl, slot, mark, rank):
    me = (lax.axis_index("zl") * 4 + lax.axis_index("y")) * 2 + lax.axis_index("c")
    for i in range(2 * EL):
        mark[i] = 0
    ones = jnp.int32(0)
    rows = []
    for i in range(EL):
        row = jnp.where(nb[0, i] >> 5 == me, 1, 0)
        at = jnp.where(row == 1, GY + ones, i - ones)
        slot[i] = at
        tbl[at, 0] = i
        tbl[at, 1] = sizes[i]
        tbl[i, 6] = at
        mark[row * EL + (nb[row, i] & (EL - 1))] = 1
        ones = ones + row
        rows.append(row)
    seen = jnp.int32(0)
    for i in range(2 * EL):
        rank[i] = seen
        seen = seen + mark[i]
    for i in range(EL):
        at, row = slot[i], rows[i]
        tbl[at, 2] = slot[nb[1 - row, i] & (EL - 1)]
        tbl[at, 3] = slot[nb[2, i] & (EL - 1)]
        tbl[at, 4] = slot[nb[3, i] & (EL - 1)]
        tbl[at, 5] = rank[row * EL + (nb[row, i] & (EL - 1))] - row * GY


def make_tables(neighbours, basis_sizes):
    smem = pl.BlockSpec(memory_space=pltpu.SMEM)
    return pl.pallas_call(
        tables_kernel,
        out_shape=jax.ShapeDtypeStruct((EL, 8), jnp.int32),
        in_specs=[smem, smem],
        out_specs=smem,
        scratch_shapes=[
            pltpu.SMEM((EL,), jnp.int32),
            pltpu.SMEM((2 * EL,), jnp.int32),
            pltpu.SMEM((2 * EL,), jnp.int32),
        ],
        name="tables",
    )(neighbours.T, basis_sizes)


def main_kernel(
    tbl_h, yc_h, yp_h, h_h, out_f, out_m, tbl,
    yc, yp, hv, cur0, cur1, f000, f001, f010, f011, f100, f101, f110, f111,
    acc, fil, outv, xg, x1, x2, x3, pb, rc, s1, ry, s2, rz, mv,
    lsem, hsend, hrecv, zsend, zrecv, xsend, xrecv, gsend, grecv, csend, crecv, ysend, yrecv, rsend, rrecv, gate,
):
    zl, y, c = (lax.axis_index(a) for a in ELEM)
    zh, x = (lax.axis_index(a) for a in BAND)
    z = zh * 4 + zl
    e = (zl * 4 + y) * 2 + c
    outer = jnp.logical_or(y == 0, y == 3)
    crossing = jnp.logical_or(jnp.logical_and(y == 0, c == 0), jnp.logical_and(y == 3, c == 1))

    def elem_id(other):
        return {"zl": other // 8, "y": (other // 2) % 4, "c": other % 2}

    def z_id(other):
        return {"zh": other // 4, "zl": other % 4}

    nxt, prv = elem_id((e + 1) % 32), elem_id((e + 31) % 32)
    x_prev, x_next, x_far = (x + 3) % 4, (x + 1) % 4, (x + 2) % 4
    xp, xm = {"x": x_next}, {"x": x_prev}

    def remote(src, dst, ss, rs, to):
        return pltpu.make_async_remote_copy(
            src_ref=src, dst_ref=dst, send_sem=ss, recv_sem=rs, device_id=to, device_id_type=MESH_ID
        )

    loads = [
        pltpu.make_async_copy(src, dst, lsem.at[k])
        for k, (src, dst) in enumerate(
            [(tbl_h, tbl)]
            + [(yc_h.at[:, :, pl.ds(b * HB, HB)], yc.at[b]) for b in (0, 1)]
            + [(h_h, hv)]
            + [(yp_h.at[:, :, pl.ds(b * HB, HB)], yp.at[b]) for b in (0, 1)]
        )
    ]
    for load in loads:
        load.start()

    barrier = pltpu.get_barrier_semaphore()
    partners = [nxt, prv, xp, xm]
    partners += [{"y": (y + d) % 4} for d in (1, 2, 3)]
    partners += [z_id((z + d) % 8) for d in range(1, 8)]
    for to in partners:
        pl.semaphore_signal(barrier, inc=1, device_id=to, device_id_type=MESH_ID)

    rows = lax.broadcasted_iota(jnp.int32, (BMAX, HB), 0)
    zero = jnp.zeros((BMAX, HB), BF)

    with jax.named_scope('w_load'):
        for load in loads[:3]:
            load.wait()

    def pack(row, b):
        def one(p, _):
            value = yc[b, tbl[p, 0]].astype(F32)
            cur0[b, p] = jnp.where(rows < tbl[p, 1], value, 0.0).astype(BF)
            return 0

        lax.fori_loop(row * GY, row * GY + GY, one, 0, unroll=4)

    halo = (((f000, f001), (f010, f011)), ((f100, f101), (f110, f111)))

    def halo_copy(degree, row, b):
        return remote(
            (cur0, cur1)[degree].at[b, pl.ds((1 - row) * GY, GY)], halo[degree][row][b],
            hsend.at[degree, row, b], hrecv.at[degree, row, b], (nxt, prv)[row],
        )

    with jax.named_scope('pack'):
        pack(1, 0)
    with jax.named_scope('barrier'):
        pl.semaphore_wait(barrier, len(partners))
    halo_copy(0, 0, 0).start()
    pack(0, 0)
    halo_copy(0, 1, 0).start()
    pack(1, 1)
    halo_copy(0, 0, 1).start()
    pack(0, 1)
    halo_copy(0, 1, 1).start()
    for load in loads[3:]:
        load.wait()

    def local_part(degree, row, b):
        cur = (cur0, cur1)[degree]

        def one(p, _):
            i = tbl[p, 0]
            own, n2, n3, n4 = cur[b, p], cur[b, tbl[p, 2]], cur[b, tbl[p, 3]], cur[b, tbl[p, 4]]
            pair = [zero, n2] if row == 0 else [n2, zero]
            stack = jnp.concatenate([own] + pair + [n3, n4], axis=0)
            applied = jnp.dot(hv[i], stack, preferred_element_type=F32)
            before = yp[b, i] if degree == 0 else cur0[b, p]
            acc[b, p] = SCALE * (applied - CENTER * own.astype(F32)) - before.astype(F32)
            return 0

        lax.fori_loop(row * GY, row * GY + GY, one, 0, unroll=8)

    def full_value(degree, row, b, p):
        i = tbl[p, 0]
        far = halo[degree][row][b][tbl[p, 5]]
        if row == 0:
            applied = jnp.dot(hv[i, :, 0:128], jnp.concatenate([zero, far], axis=0), preferred_element_type=F32)
        else:
            applied = jnp.dot(hv[i, :, 128:256], jnp.concatenate([far, zero], axis=0), preferred_element_type=F32)
        return jnp.where(rows < tbl[p, 1], acc[b, p] + SCALE * applied, 0.0).astype(BF)

    def first(row, b):
        def one(p, _):
            cur1[b, p] = full_value(0, row, b, p)
            return 0

        lax.fori_loop(row * GY, row * GY + GY, one, 0, unroll=8)

    def z_copy(half, b, j, src_zh):
        return remote(
            fil.at[b, pl.ds(half * GY + j * CH, CH)], xg.at[b, src_zh, pl.ds(j * CH, CH)],
            zsend.at[half, b, j], zrecv.at[src_zh, b, j], z_id((zl + 2 + 4 * half) % 8),
        )

    def second(b):
        def one(k, _):
            j = (k % 2) * 2 + k // 2
            for row in (1, 0):
                for m in range(CH):
                    p = row * GY + j * CH + m
                    fil[b, p] = full_value(1, row, b, p)
            if b == 0:
                @pl.when(jnp.logical_not(outer))
                def _():
                    for row in (1, 0):
                        z_copy(row, b, j, zh).start()
            else:
                for row in (1, 0):
                    z_copy(row, b, j, zh).start()
            return 0

        lax.fori_loop(0, NCH, one, 0)

    for b in (0, 1):
        with jax.named_scope(f'local0{b}'):
            local_part(0, 1, b)
            local_part(0, 0, b)
    for b in (0, 1):
        with jax.named_scope(f'w_h0{b}1'):
            halo_copy(0, 1, b).wait_recv()
        first(1, b)
        halo_copy(1, 0, b).start()
        with jax.named_scope(f'w_h0{b}0'):
            halo_copy(0, 0, b).wait_recv()
        first(0, b)
        halo_copy(1, 1, b).start()
        with jax.named_scope(f'local1{b}'):
            local_part(1, 1, b)
            local_part(1, 0, b)
    for b in (0, 1):
        with jax.named_scope(f'w_h1{b}'):
            halo_copy(1, 1, b).wait_recv()
            halo_copy(1, 0, b).wait_recv()
        if b == 1:
            @pl.when(crossing)
            def _():
                pl.semaphore_signal(gate, inc=1, device_id={"c": 1 - c}, device_id_type=MESH_ID)

            @pl.when(jnp.logical_and(outer, jnp.logical_not(crossing)))
            def _():
                with jax.named_scope('w_gate'):
                    pl.semaphore_wait(gate, 1)

            @pl.when(outer)
            def _():
                for j in ORDER:
                    for row in (1, 0):
                        z_copy(row, 0, j, zh).start()
        with jax.named_scope(f'second{b}'):
            second(b)

    def put(i, _):
        s = tbl[i, 6]
        outv[i] = jnp.concatenate([fil[0, s], fil[1, s]], axis=1)
        return 0

    with jax.named_scope('put'):
        lax.fori_loop(0, EL, put, 0, unroll=4)
    store_f = pltpu.make_async_copy(outv, out_f, lsem.at[6])
    store_f.start()

    def x_copy(way, b, j, h):
        part = pl.ds(j * CH, CH)
        return remote(
            xg.at[b, h, part], (x1, x2)[way].at[b, h, part],
            xsend.at[way, b, j, h], xrecv.at[way, b, j, h], (xp, xm)[way],
        )

    def pass_on(b, j, h):
        part, way = pl.ds(j * CH, CH), j // 2
        return remote(
            (x1, x2)[way].at[b, h, part], x3.at[b, h, part], gsend.at[b, j, h], grecv.at[b, j, h], (xp, xm)[way]
        )

    for b in (0, 1):
        for j in ORDER:
            for h in (0, 1):
                with jax.named_scope(f'wz{b}{j}{h}'):
                    z_copy(0, b, j, h).wait_recv()
                x_copy(0, b, j, h).start()
                x_copy(1, b, j, h).start()

    def pass_half(b):
        for j in ORDER:
            for h in (0, 1):
                with jax.named_scope(f'wx{b}{j}{h}'):
                    x_copy(j // 2, b, j, h).wait_recv()
                pass_on(b, j, h).start()

    def bound_for(x_a, b):
        return (x_a % 2) * 2 + b

    def c_copy(x_a, b):
        at = (pl.ds(0, 2), x_a // 2, bound_for(x_a, b))
        return remote(pb.at[(1 - c, *at)], rc.at[at], csend.at[x_a, b], crecv.at[x_a, b], {"c": 1 - c})

    def product(x_a, b, ref):
        left = jnp.concatenate([ref[b, h].reshape(GY * BMAX, HB) for h in (0, 1)], axis=1)
        for zh_b in (0, 1):
            right = jnp.concatenate([xg[k, zh_b].reshape(GY * BMAX, HB) for k in (0, 1)], axis=1)
            tile = lax.dot_general(left, right, (((0,), (0,)), ((), ())), preferred_element_type=F32).astype(BF)
            for zh_a in (0, 1):
                for core in (0, 1):
                    at = zh_a * HB + core * 64
                    pb[core, zh_a, x_a // 2, bound_for(x_a, b), zh_b] = tile[at : at + 64]
        c_copy(x_a, b).start()

    def y_copy(to, d, xh):
        return remote(
            s1.at[:, xh, to], ry.at[d - 1, xh], ysend.at[d - 1, xh], yrecv.at[d - 1, xh], {"y": to}
        )

    def settle(x_a, b):
        xh, to = x_a // 2, bound_for(x_a, b)
        with jax.named_scope(f'wc{b}'):
            c_copy(x_a, b).wait_recv()
        for zh_a in (0, 1):
            s1[zh_a, xh, to] = (pb[c, zh_a, xh, to].astype(F32) + rc[zh_a, xh, to].astype(F32)).astype(BF)

        @pl.when(to != y)
        def _():
            y_copy(to, (to + 4 - y) % 4, xh).start()

    def r_copy(to, src_xh):
        d = (to + 8 - z) % 8
        return remote(
            s2.at[src_xh, (to % 4) // 2, to // 4], rz.at[d - 1], rsend.at[d - 1], rrecv.at[d - 1], z_id(to)
        )

    def gather_y(xh):
        for d in (1, 3, 2):
            y_copy((y + d) % 4, d, xh).wait_recv()
        for zh_a in (0, 1):
            total = s1[zh_a, xh, y].astype(F32)
            for d in range(3):
                total = total + ry[d, xh, zh_a].astype(F32)
            s2[xh, zh_a] = total.astype(BF)
        for zh_a in (0, 1):
            for zh_b in (0, 1):
                to = zh_b * 4 + zh_a * 2 + xh

                @pl.when(to != z)
                def _():
                    r_copy(to, xh).start()

    def beside(b):
        for way in (0, 1):
            with jax.named_scope(f'w_x{way}'):
                for j in ((2, 3), (0, 1))[way]:
                    for h in (0, 1):
                        x_copy(way, b, j, h).wait_recv()
            product((x_prev, x_next)[way], b, (x1, x2)[way])

    def far_unit(b):
        with jax.named_scope(f'w_far{b}'):
            for j in ORDER:
                for h in (0, 1):
                    pass_on(b, j, h).wait_recv()
        product(x_far, b, x3)
        settle(x_far, b)

    same = y // 2 == x % 2
    pass_half(0)
    with jax.named_scope('prod_e'):
        product(x, 0, xg)
        product(x, 1, xg)
        beside(0)
    with jax.named_scope('settle_e'):
        settle(x, 0)
        settle(x, 1)
        settle(x_prev, 0)
        settle(x_next, 0)
    pass_half(1)
    with jax.named_scope('prod_l'):
        beside(1)
    with jax.named_scope('settle_l'):
        settle(x_prev, 1)
        settle(x_next, 1)
    far_unit(0)

    with jax.named_scope('gather_y1'):
        @pl.when(same)
        def _():
            gather_y(x // 2)

        @pl.when(jnp.logical_not(same))
        def _():
            gather_y(0)
            gather_y(1)

    far_unit(1)

    with jax.named_scope('gather_y2'):
        @pl.when(same)
        def _():
            gather_y(1 - x // 2)

    total = s2[zl % 2, zl // 2, zh].astype(F32)
    for d in (1, 7, 2, 6, 3, 5, 4):
        with jax.named_scope(f'wr{d}'):
            r_copy((z + d) % 8, 0).wait_recv()
        total = total + rz[d - 1].astype(F32)
    mv[...] = total * (1.0 / 65536.0)
    store_m = pltpu.make_async_copy(mv, out_m, lsem.at[7])
    store_m.start()

    with jax.named_scope('tail'):
        for degree in (0, 1):
            for row in (0, 1):
                for b in (0, 1):
                    halo_copy(degree, row, b).wait_send()
        for b in (0, 1):
            for j in range(NCH):
                for h in (0, 1):
                    z_copy(h, b, j, zh).wait_send()
                    x_copy(0, b, j, h).wait_send()
                    x_copy(1, b, j, h).wait_send()
                    pass_on(b, j, h).wait_send()
        for x_a in range(4):
            for b in (0, 1):
                c_copy(x_a, b).wait_send()
        for d in (1, 2, 3):
            for xh in (0, 1):
                y_copy((y + d) % 4, d, xh).wait_send()
        for d in range(1, 8):
            r_copy((z + d) % 8, 0).wait_send()
        store_f.wait()
        store_m.wait()


def on_device(y_current, y_previous, h_blocks, basis_sizes, neighbours):
    tbl = make_tables(neighbours, basis_sizes)
    any_space = pl.BlockSpec(memory_space=pl.ANY)
    dma = pltpu.SemaphoreType.DMA
    halves = pltpu.VMEM((2, EL, BMAX, HB), BF)
    met = pltpu.VMEM((2, 2, GY, BMAX, HB), BF)
    return pl.pallas_call(
        main_kernel,
        out_shape=(
            jax.ShapeDtypeStruct((EL, BMAX, BD), BF),
            jax.ShapeDtypeStruct((64, BD), F32),
        ),
        in_specs=[any_space] * 4,
        out_specs=(any_space, any_space),
        scratch_shapes=[
            pltpu.SMEM((EL, 8), jnp.int32),
            halves,
            halves,
            pltpu.VMEM((EL, BMAX, 5 * BMAX), BF),
            halves,
            halves,
            *[pltpu.VMEM((GY, BMAX, HB), BF)] * 8,
            pltpu.VMEM((2, EL, BMAX, HB), F32),
            halves,
            pltpu.VMEM((EL, BMAX, BD), BF),
            met,
            met,
            met,
            met,
            pltpu.VMEM((2, 2, 2, 4, 2, 64, BD), BF),
            pltpu.VMEM((2, 2, 4, 2, 64, BD), BF),
            pltpu.VMEM((2, 2, 4, 2, 64, BD), BF),
            pltpu.VMEM((3, 2, 2, 2, 64, BD), BF),
            pltpu.VMEM((2, 2, 2, 64, BD), BF),
            pltpu.VMEM((7, 64, BD), BF),
            pltpu.VMEM((64, BD), F32),
            dma((8,)),
            dma((2, 2, 2)), dma((2, 2, 2)),
            dma((2, 2, NCH)), dma((2, 2, NCH)),
            dma((2, 2, NCH, 2)), dma((2, 2, NCH, 2)),
            dma((2, NCH, 2)), dma((2, NCH, 2)),
            dma((4, 2)), dma((4, 2)),
            dma((3, 2)), dma((3, 2)),
            dma((7,)), dma((7,)),
            pltpu.SemaphoreType.REGULAR,
        ],
        compiler_params=pltpu.CompilerParams(collective_id=0, has_side_effects=True),
        name="chain",
    )(tbl, y_current, y_previous, h_blocks)


def solution(mesh):
    split = Mesh(mesh.devices.reshape(4, 4, 2, 2, 4), ELEM + BAND)
    return jax.shard_map(
        on_device,
        mesh=split,
        in_specs=(
            P(ELEM, None, BAND),
            P(ELEM, None, BAND),
            P(ELEM, None, None),
            P(ELEM),
            P(ELEM, None),
        ),
        out_specs=(P(ELEM, None, BAND), P(ELEM, BAND)),
        check_vma=False,
    )
```

```python
import jax
import jax.numpy as jnp
from jax import lax
from jax.experimental import pallas as pl
from jax.experimental.pallas import tpu as pltpu
from jax.sharding import Mesh
from jax.sharding import PartitionSpec as P

BMAX = 64
EL = 32
GY = 16
BD = 256
NB = 2048
ROWS = GY * BMAX
HB = 128
CH = 4
NCH = GY // CH
ORDER = (0, 2, 1, 3)

CENTER = 0.3
SCALE = 2.0 / 1.7

ELEM = ("zl", "y", "c")
BAND = ("zh", "x")
BF = jnp.bfloat16
F32 = jnp.float32
MESH_ID = pl.DeviceIdType.MESH


def ones_of(word):
    word = word - (lax.shift_right_logical(word, 1) & 0x55555555)
    word = (word & 0x33333333) + (lax.shift_right_logical(word, 2) & 0x33333333)
    word = (word + lax.shift_right_logical(word, 4)) & 0x0F0F0F0F
    return lax.shift_right_logical(word * 0x01010101, 24)


def make_tables(me, nb, sizes, tbl, slot, link, power):
    for i in range(EL):
        power[i] = jnp.int32(1 << i if i < 31 else -(1 << 31))
    ones, rows = jnp.int32(0), []
    wanted = [jnp.int32(0), jnp.int32(0)]
    for i in range(EL):
        row = jnp.where(nb[0, i] >> 5 == me, 1, 0)
        rows.append(row)
        slot[i] = jnp.where(row == 1, GY + ones, i - ones) & (EL - 1)
        ones = ones + row
        for k in (0, 1):
            wanted[k] = wanted[k] + jnp.where(row == k, power[nb[k, i] & (EL - 1)], 0)
    first = [jnp.int32(0), jnp.int32(0)]
    for i in reversed(range(EL)):
        link[i] = jnp.where(rows[i] == 1, first[1], first[0])
        first = [jnp.where(rows[i] == k, i, first[k]) for k in (0, 1)]
    for row in (0, 1):
        i = first[row]
        for p in range(row * GY, row * GY + GY):
            tbl[p, 0] = i
            tbl[p, 1] = sizes[i]
            tbl[p, 2] = slot[nb[1 - row, i] & (EL - 1)]
            tbl[p, 3] = slot[nb[2, i] & (EL - 1)]
            tbl[p, 4] = slot[nb[3, i] & (EL - 1)]
            tbl[p, 5] = ones_of(wanted[row] & (power[nb[row, i] & (EL - 1)] - 1)) & (GY - 1)
            i = link[i]


def main_kernel(
    nb_h, size_h, yc_h, yp_h, h_h, out_f, out_m, nb, sizes, tbl, slot, link, power,
    yc, yp, hv, cur0, cur1, f000, f001, f010, f011, f100, f101, f110, f111,
    acc, fil, outv, xg, x1, x2, x3, pb, rc, s1, ry, s2, rz, mv,
    lsem, hsend, hrecv, zsend, zrecv, xsend, xrecv, gsend, grecv, csend, crecv, ysend, yrecv, rsend, rrecv,
):
    zl, y, c = (lax.axis_index(a) for a in ELEM)
    zh, x = (lax.axis_index(a) for a in BAND)
    z = zh * 4 + zl
    e = (zl * 4 + y) * 2 + c
    outer = jnp.logical_or(y == 0, y == 3)

    def elem_id(other):
        return {"zl": other // 8, "y": (other // 2) % 4, "c": other % 2}

    def z_id(other):
        return {"zh": other // 4, "zl": other % 4}

    nxt, prv = elem_id((e + 1) % 32), elem_id((e + 31) % 32)
    x_prev, x_next, x_far = (x + 3) % 4, (x + 1) % 4, (x + 2) % 4
    xp, xm = {"x": x_next}, {"x": x_prev}

    def remote(src, dst, ss, rs, to):
        return pltpu.make_async_remote_copy(
            src_ref=src, dst_ref=dst, send_sem=ss, recv_sem=rs, device_id=to, device_id_type=MESH_ID
        )

    loads = [
        pltpu.make_async_copy(src, dst, lsem.at[k])
        for k, (src, dst) in enumerate(
            [(nb_h, nb), (size_h, sizes)]
            + [(yc_h.at[:, :, pl.ds(b * HB, HB)], yc.at[b]) for b in (0, 1)]
            + [(h_h, hv)]
            + [(yp_h.at[:, :, pl.ds(b * HB, HB)], yp.at[b]) for b in (0, 1)]
        )
    ]
    for load in loads:
        load.start()

    barrier = pltpu.get_barrier_semaphore()
    partners = [nxt, prv, xp, xm]
    partners += [{"y": (y + d) % 4} for d in (1, 2, 3)]
    partners += [z_id((z + d) % 8) for d in range(1, 8)]
    for to in partners:
        pl.semaphore_signal(barrier, inc=1, device_id=to, device_id_type=MESH_ID)

    rows = lax.broadcasted_iota(jnp.int32, (BMAX, HB), 0)
    zero = jnp.zeros((BMAX, HB), BF)

    with jax.named_scope('w_load'):
        for load in loads[:2]:
            load.wait()
    with jax.named_scope('tables'):
        make_tables(e, nb, sizes, tbl, slot, link, power)
    for load in loads[2:4]:
        load.wait()

    def pack(row, b):
        def one(p, _):
            value = yc[b, tbl[p, 0]].astype(F32)
            cur0[b, p] = jnp.where(rows < tbl[p, 1], value, 0.0).astype(BF)
            return 0

        lax.fori_loop(row * GY, row * GY + GY, one, 0, unroll=4)

    halo = (((f000, f001), (f010, f011)), ((f100, f101), (f110, f111)))

    def halo_copy(degree, row, b):
        return remote(
            (cur0, cur1)[degree].at[b, pl.ds((1 - row) * GY, GY)], halo[degree][row][b],
            hsend.at[degree, row, b], hrecv.at[degree, row, b], (nxt, prv)[row],
        )

    with jax.named_scope('pack'):
        pack(1, 0)
    with jax.named_scope('barrier'):
        pl.semaphore_wait(barrier, len(partners))
    halo_copy(0, 0, 0).start()
    pack(0, 0)
    halo_copy(0, 1, 0).start()
    pack(1, 1)
    halo_copy(0, 0, 1).start()
    pack(0, 1)
    halo_copy(0, 1, 1).start()
    for load in loads[4:]:
        load.wait()

    def local_part(degree, row, b):
        cur = (cur0, cur1)[degree]

        def one(p, _):
            i = tbl[p, 0]
            own, n2, n3, n4 = cur[b, p], cur[b, tbl[p, 2]], cur[b, tbl[p, 3]], cur[b, tbl[p, 4]]
            pair = [zero, n2] if row == 0 else [n2, zero]
            stack = jnp.concatenate([own] + pair + [n3, n4], axis=0)
            applied = jnp.dot(hv[i], stack, preferred_element_type=F32)
            before = yp[b, i] if degree == 0 else cur0[b, p]
            acc[b, p] = SCALE * (applied - CENTER * own.astype(F32)) - before.astype(F32)
            return 0

        lax.fori_loop(row * GY, row * GY + GY, one, 0, unroll=8)

    def full_value(degree, row, b, p):
        i = tbl[p, 0]
        far = halo[degree][row][b][tbl[p, 5]]
        if row == 0:
            applied = jnp.dot(hv[i, :, 0:128], jnp.concatenate([zero, far], axis=0), preferred_element_type=F32)
        else:
            applied = jnp.dot(hv[i, :, 128:256], jnp.concatenate([far, zero], axis=0), preferred_element_type=F32)
        return jnp.where(rows < tbl[p, 1], acc[b, p] + SCALE * applied, 0.0).astype(BF)

    def first(row, b):
        def one(p, _):
            cur1[b, p] = full_value(0, row, b, p)
            return 0

        lax.fori_loop(row * GY, row * GY + GY, one, 0, unroll=8)

    def z_copy(half, b, j):
        return remote(
            fil.at[b, pl.ds(half * GY + j * CH, CH)], xg.at[b, zh, pl.ds(j * CH, CH)],
            zsend.at[half, b], zrecv.at[b, j], z_id((zl + 2 + 4 * half) % 8),
        )

    def x_copy(way, b, j):
        part = pl.ds(j * CH, CH)
        return remote(
            xg.at[b, :, part], (x1, x2)[way].at[b, :, part], xsend.at[way, b], xrecv.at[way, b, j], (xp, xm)[way]
        )

    def pass_on(b, j):
        part, way = pl.ds(j * CH, CH), j // 2
        return remote((x1, x2)[way].at[b, :, part], x3.at[b, :, part], gsend.at[b], grecv.at[b, j], (xp, xm)[way])

    def bytes_of(ref, sem):
        return pltpu.make_async_copy(ref, ref, sem)

    def z_to_x(b):
        for j in ORDER:
            with jax.named_scope(f'wz{b}{j}'):
                bytes_of(xg.at[b, :, pl.ds(j * CH, CH)], zrecv.at[b, j]).wait()
            x_copy(0, b, j).start()
            x_copy(1, b, j).start()

    def second(b):
        def one(k, _):
            j = (k % 2) * 2 + k // 2
            for row in (1, 0):
                for m in range(CH):
                    p = row * GY + j * CH + m
                    fil[b, p] = full_value(1, row, b, p)
            for row in (1, 0):
                z_copy(row, b, j).start()
            return 0

        lax.fori_loop(0, NCH, one, 0)

    for b in (0, 1):
        with jax.named_scope(f'local0{b}'):
            local_part(0, 1, b)
            local_part(0, 0, b)
    for b in (0, 1):
        with jax.named_scope(f'w_h0{b}1'):
            halo_copy(0, 1, b).wait_recv()
        first(1, b)
        halo_copy(1, 0, b).start()
        with jax.named_scope(f'w_h0{b}0'):
            halo_copy(0, 0, b).wait_recv()
        first(0, b)
        halo_copy(1, 1, b).start()
        with jax.named_scope(f'local1{b}'):
            local_part(1, 1, b)
            local_part(1, 0, b)
    def finish(b):
        with jax.named_scope(f'w_h1{b}'):
            halo_copy(1, 1, b).wait_recv()
            halo_copy(1, 0, b).wait_recv()
        with jax.named_scope(f'second{b}'):
            second(b)

    finish(0)

    @pl.when(outer)
    def _():
        z_to_x(0)

    finish(1)

    @pl.when(jnp.logical_not(outer))
    def _():
        z_to_x(0)

    z_to_x(1)

    def put(i, _):
        s = slot[i]
        outv[i] = jnp.concatenate([fil[0, s], fil[1, s]], axis=1)
        return 0

    with jax.named_scope('put'):
        lax.fori_loop(0, EL, put, 0, unroll=4)
    store_f = pltpu.make_async_copy(outv, out_f, lsem.at[7])
    store_f.start()

    def pass_half(b):
        for j in ORDER:
            with jax.named_scope(f'wx{b}{j}'):
                x_copy(j // 2, b, j).wait_recv()
            pass_on(b, j).start()

    def bound_for(x_a, b):
        return (x_a % 2) * 2 + b

    def c_copy(x_a, b):
        at = (pl.ds(0, 2), x_a // 2, bound_for(x_a, b))
        return remote(pb.at[(1 - c, *at)], rc.at[at], csend, crecv.at[x_a, b], {"c": 1 - c})

    def product(x_a, b, ref):
        left = jnp.concatenate([ref[b, h].reshape(GY * BMAX, HB) for h in (0, 1)], axis=1)
        for zh_b in (0, 1):
            right = jnp.concatenate([xg[k, zh_b].reshape(GY * BMAX, HB) for k in (0, 1)], axis=1)
            tile = lax.dot_general(left, right, (((0,), (0,)), ((), ())), preferred_element_type=F32).astype(BF)
            for zh_a in (0, 1):
                for core in (0, 1):
                    at = zh_a * HB + core * 64
                    pb[core, zh_a, x_a // 2, bound_for(x_a, b), zh_b] = tile[at : at + 64]
        c_copy(x_a, b).start()

    def y_copy(to, d, xh):
        return remote(
            s1.at[:, xh, to], ry.at[d - 1, xh], ysend, yrecv.at[d - 1, xh], {"y": to}
        )

    def settle(x_a, b):
        xh, to = x_a // 2, bound_for(x_a, b)
        with jax.named_scope(f'wc{b}'):
            c_copy(x_a, b).wait_recv()
        for zh_a in (0, 1):
            s1[zh_a, xh, to] = (pb[c, zh_a, xh, to].astype(F32) + rc[zh_a, xh, to].astype(F32)).astype(BF)

        @pl.when(to != y)
        def _():
            y_copy(to, (to + 4 - y) % 4, xh).start()

    def r_copy(to, src_xh):
        d = (to + 8 - z) % 8
        return remote(
            s2.at[src_xh, (to % 4) // 2, to // 4], rz.at[d - 1], rsend, rrecv, z_id(to)
        )

    def gather_y(xh):
        for d in (1, 3, 2):
            y_copy((y + d) % 4, d, xh).wait_recv()
        for zh_a in (0, 1):
            total = s1[zh_a, xh, y].astype(F32)
            for d in range(3):
                total = total + ry[d, xh, zh_a].astype(F32)
            s2[xh, zh_a] = total.astype(BF)
        for zh_a in (0, 1):
            for zh_b in (0, 1):
                to = zh_b * 4 + zh_a * 2 + xh

                @pl.when(to != z)
                def _():
                    r_copy(to, xh).start()

    def beside(b):
        for way in (0, 1):
            with jax.named_scope(f'w_x{way}'):
                for j in ((2, 3), (0, 1))[way]:
                    x_copy(way, b, j).wait_recv()
            product((x_prev, x_next)[way], b, (x1, x2)[way])

    def far_unit(b):
        with jax.named_scope(f'w_far{b}'):
            for j in ORDER:
                pass_on(b, j).wait_recv()
        product(x_far, b, x3)
        settle(x_far, b)

    same = y // 2 == x % 2
    pass_half(0)
    with jax.named_scope('prod_e'):
        product(x, 0, xg)
        product(x, 1, xg)
        beside(0)
    with jax.named_scope('settle_e'):
        settle(x, 0)
        settle(x, 1)
        settle(x_prev, 0)
        settle(x_next, 0)
    pass_half(1)
    with jax.named_scope('prod_l'):
        beside(1)
    with jax.named_scope('settle_l'):
        settle(x_prev, 1)
        settle(x_next, 1)
    far_unit(0)
    far_unit(1)

    with jax.named_scope('gather_y1'):
        @pl.when(same)
        def _():
            gather_y(x // 2)

        @pl.when(jnp.logical_not(same))
        def _():
            gather_y(0)
            gather_y(1)

    with jax.named_scope('gather_y2'):
        @pl.when(same)
        def _():
            gather_y(1 - x // 2)

    total = s2[zl % 2, zl // 2, zh].astype(F32)
    with jax.named_scope('wr'):
        bytes_of(rz, rrecv).wait()
    for d in range(7):
        total = total + rz[d].astype(F32)
    mv[...] = total * (1.0 / 65536.0)
    store_m = pltpu.make_async_copy(mv, out_m, lsem.at[8])
    store_m.start()

    with jax.named_scope('tail'):
        for degree in (0, 1):
            for row in (0, 1):
                for b in (0, 1):
                    halo_copy(degree, row, b).wait_send()
        for b in (0, 1):
            for k in (0, 1):
                bytes_of(fil.at[b, pl.ds(k * GY, GY)], zsend.at[k, b]).wait()
                bytes_of(xg.at[b], xsend.at[k, b]).wait()
            bytes_of(x3.at[b], gsend.at[b]).wait()
        bytes_of(rc, csend).wait()
        bytes_of(ry, ysend).wait()
        bytes_of(rz, rsend).wait()
        store_f.wait()
        store_m.wait()


def on_device(y_current, y_previous, h_blocks, basis_sizes, neighbours):
    any_space = pl.BlockSpec(memory_space=pl.ANY)
    dma = pltpu.SemaphoreType.DMA
    halves = pltpu.VMEM((2, EL, BMAX, HB), BF)
    met = pltpu.VMEM((2, 2, GY, BMAX, HB), BF)
    return pl.pallas_call(
        main_kernel,
        out_shape=(
            jax.ShapeDtypeStruct((EL, BMAX, BD), BF),
            jax.ShapeDtypeStruct((64, BD), F32),
        ),
        in_specs=[any_space] * 5,
        out_specs=(any_space, any_space),
        scratch_shapes=[
            pltpu.SMEM((4, EL), jnp.int32),
            pltpu.SMEM((EL,), jnp.int32),
            pltpu.SMEM((EL, 8), jnp.int32),
            pltpu.SMEM((EL,), jnp.int32),
            pltpu.SMEM((EL,), jnp.int32),
            pltpu.SMEM((EL,), jnp.int32),
            halves,
            halves,
            pltpu.VMEM((EL, BMAX, 5 * BMAX), BF),
            halves,
            halves,
            *[pltpu.VMEM((GY, BMAX, HB), BF)] * 8,
            pltpu.VMEM((2, EL, BMAX, HB), F32),
            halves,
            pltpu.VMEM((EL, BMAX, BD), BF),
            met,
            met,
            met,
            met,
            pltpu.VMEM((2, 2, 2, 4, 2, 64, BD), BF),
            pltpu.VMEM((2, 2, 4, 2, 64, BD), BF),
            pltpu.VMEM((2, 2, 4, 2, 64, BD), BF),
            pltpu.VMEM((3, 2, 2, 2, 64, BD), BF),
            pltpu.VMEM((2, 2, 2, 64, BD), BF),
            pltpu.VMEM((7, 64, BD), BF),
            pltpu.VMEM((64, BD), F32),
            dma((9,)),
            dma((2, 2, 2)), dma((2, 2, 2)),
            dma((2, 2)), dma((2, NCH)),
            dma((2, 2)), dma((2, 2, NCH)),
            dma((2,)), dma((2, NCH)),
            dma, dma((4, 2)),
            dma, dma((3, 2)),
            dma, dma,
        ],
        compiler_params=pltpu.CompilerParams(collective_id=0, has_side_effects=True),
        name="chain",
    )(neighbours.T, basis_sizes, y_current, y_previous, h_blocks)


def solution(mesh):
    split = Mesh(mesh.devices.reshape(4, 4, 2, 2, 4), ELEM + BAND)
    return jax.shard_map(
        on_device,
        mesh=split,
        in_specs=(
            P(ELEM, None, BAND),
            P(ELEM, None, BAND),
            P(ELEM, None, None),
            P(ELEM),
            P(ELEM, None),
        ),
        out_specs=(P(ELEM, None, BAND), P(ELEM, BAND)),
        check_vma=False,
    )
```

```python
import jax
import jax.numpy as jnp
from jax import lax
from jax.experimental import pallas as pl
from jax.experimental.pallas import tpu as pltpu
from jax.sharding import Mesh
from jax.sharding import PartitionSpec as P

BMAX = 64
EL = 32
GY = 16
BD = 256
NB = 2048
ROWS = GY * BMAX
HB = 128
CH = 4
NCH = GY // CH
ORDER = (0, 2, 1, 3)

CENTER = 0.3
SCALE = 2.0 / 1.7

ELEM = ("zl", "y", "c")
BAND = ("zh", "x")
BF = jnp.bfloat16
F32 = jnp.float32
MESH_ID = pl.DeviceIdType.MESH


def ones_of(word):
    word = word - (lax.shift_right_logical(word, 1) & 0x55555555)
    word = (word & 0x33333333) + (lax.shift_right_logical(word, 2) & 0x33333333)
    word = (word + lax.shift_right_logical(word, 4)) & 0x0F0F0F0F
    return lax.shift_right_logical(word * 0x01010101, 24)


def make_tables(me, nb, sizes, tbl, slot, link, power):
    for i in range(EL):
        power[i] = jnp.int32(1 << i if i < 31 else -(1 << 31))
    ones, rows = jnp.int32(0), []
    wanted = [jnp.int32(0), jnp.int32(0)]
    for i in range(EL):
        row = jnp.where(nb[0, i] >> 5 == me, 1, 0)
        rows.append(row)
        slot[i] = jnp.where(row == 1, GY + ones, i - ones) & (EL - 1)
        ones = ones + row
        for k in (0, 1):
            wanted[k] = wanted[k] + jnp.where(row == k, power[nb[k, i] & (EL - 1)], 0)
    first = [jnp.int32(0), jnp.int32(0)]
    for i in reversed(range(EL)):
        link[i] = jnp.where(rows[i] == 1, first[1], first[0])
        first = [jnp.where(rows[i] == k, i, first[k]) for k in (0, 1)]
    for row in (0, 1):
        i = first[row]
        for p in range(row * GY, row * GY + GY):
            tbl[p, 0] = i
            tbl[p, 1] = sizes[i]
            tbl[p, 2] = slot[nb[1 - row, i] & (EL - 1)]
            tbl[p, 3] = slot[nb[2, i] & (EL - 1)]
            tbl[p, 4] = slot[nb[3, i] & (EL - 1)]
            tbl[p, 5] = ones_of(wanted[row] & (power[nb[row, i] & (EL - 1)] - 1)) & (GY - 1)
            i = link[i]


def main_kernel(
    nb_h, size_h, yc_h, yp_h, h_h, out_f, out_m, nb, sizes, tbl, slot, link, power,
    yc, yp, hv, cur0, cur1, f000, f001, f010, f011, f100, f101, f110, f111,
    acc, fil, outv, xg, x1, x2, x3, pb, rc, s1, ry, s2, rz, mv, ft, fr,
    lsem, hsend, hrecv, zsend, zrecv, xsend, xrecv, gsend, grecv, csend, crecv, ysend, yrecv, rsend, rrecv, fsend, frecv,
):
    zl, y, c = (lax.axis_index(a) for a in ELEM)
    zh, x = (lax.axis_index(a) for a in BAND)
    z = zh * 4 + zl
    e = (zl * 4 + y) * 2 + c
    outer = jnp.logical_or(y == 0, y == 3)

    def elem_id(other):
        return {"zl": other // 8, "y": (other // 2) % 4, "c": other % 2}

    def z_id(other):
        return {"zh": other // 4, "zl": other % 4}

    nxt, prv = elem_id((e + 1) % 32), elem_id((e + 31) % 32)
    x_prev, x_next, x_far = (x + 3) % 4, (x + 1) % 4, (x + 2) % 4
    xp, xm = {"x": x_next}, {"x": x_prev}

    def remote(src, dst, ss, rs, to):
        return pltpu.make_async_remote_copy(
            src_ref=src, dst_ref=dst, send_sem=ss, recv_sem=rs, device_id=to, device_id_type=MESH_ID
        )

    loads = [
        pltpu.make_async_copy(src, dst, lsem.at[k])
        for k, (src, dst) in enumerate(
            [(nb_h, nb), (size_h, sizes)]
            + [(yc_h.at[:, :, pl.ds(b * HB, HB)], yc.at[b]) for b in (0, 1)]
            + [(h_h, hv)]
            + [(yp_h.at[:, :, pl.ds(b * HB, HB)], yp.at[b]) for b in (0, 1)]
        )
    ]
    for load in loads:
        load.start()

    barrier = pltpu.get_barrier_semaphore()
    partners = [nxt, prv, xp, xm]
    partners += [{"y": (y + d) % 4} for d in (1, 2, 3)]
    partners += [z_id((z + d) % 8) for d in range(1, 8)]
    for to in partners:
        pl.semaphore_signal(barrier, inc=1, device_id=to, device_id_type=MESH_ID)

    same = y // 2 == x % 2
    mirrored = jnp.logical_not(same)
    b_own, b_rows = zh * 4 + x, e // 4

    def mirror_id(s):
        return {**elem_id(4 * b_own + s), "zh": b_rows // 4, "x": b_rows % 4}

    @pl.when(mirrored)
    def _():
        for s in range(4):
            pl.semaphore_signal(barrier, inc=1, device_id=mirror_id(s), device_id_type=MESH_ID)

    rows = lax.broadcasted_iota(jnp.int32, (BMAX, HB), 0)
    zero = jnp.zeros((BMAX, HB), BF)

    with jax.named_scope('w_load'):
        for load in loads[:2]:
            load.wait()
    with jax.named_scope('tables'):
        make_tables(e, nb, sizes, tbl, slot, link, power)
    for load in loads[2:4]:
        load.wait()

    def pack(row, b):
        def one(p, _):
            value = yc[b, tbl[p, 0]].astype(F32)
            cur0[b, p] = jnp.where(rows < tbl[p, 1], value, 0.0).astype(BF)
            return 0

        lax.fori_loop(row * GY, row * GY + GY, one, 0, unroll=4)

    halo = (((f000, f001), (f010, f011)), ((f100, f101), (f110, f111)))

    def halo_copy(degree, row, b):
        return remote(
            (cur0, cur1)[degree].at[b, pl.ds((1 - row) * GY, GY)], halo[degree][row][b],
            hsend.at[degree, row, b], hrecv.at[degree, row, b], (nxt, prv)[row],
        )

    with jax.named_scope('pack'):
        pack(1, 0)
    with jax.named_scope('barrier'):
        pl.semaphore_wait(barrier, len(partners) + 4 * mirrored.astype(jnp.int32))
    halo_copy(0, 0, 0).start()
    pack(0, 0)
    halo_copy(0, 1, 0).start()
    pack(1, 1)
    halo_copy(0, 0, 1).start()
    pack(0, 1)
    halo_copy(0, 1, 1).start()
    for load in loads[4:]:
        load.wait()

    def local_part(degree, row, b):
        cur = (cur0, cur1)[degree]

        def one(p, _):
            i = tbl[p, 0]
            own, n2, n3, n4 = cur[b, p], cur[b, tbl[p, 2]], cur[b, tbl[p, 3]], cur[b, tbl[p, 4]]
            pair = [zero, n2] if row == 0 else [n2, zero]
            stack = jnp.concatenate([own] + pair + [n3, n4], axis=0)
            applied = jnp.dot(hv[i], stack, preferred_element_type=F32)
            before = yp[b, i] if degree == 0 else cur0[b, p]
            acc[b, p] = SCALE * (applied - CENTER * own.astype(F32)) - before.astype(F32)
            return 0

        lax.fori_loop(row * GY, row * GY + GY, one, 0, unroll=8)

    def full_value(degree, row, b, p):
        i = tbl[p, 0]
        far = halo[degree][row][b][tbl[p, 5]]
        if row == 0:
            applied = jnp.dot(hv[i, :, 0:128], jnp.concatenate([zero, far], axis=0), preferred_element_type=F32)
        else:
            applied = jnp.dot(hv[i, :, 128:256], jnp.concatenate([far, zero], axis=0), preferred_element_type=F32)
        return jnp.where(rows < tbl[p, 1], acc[b, p] + SCALE * applied, 0.0).astype(BF)

    def first(row, b):
        def one(p, _):
            cur1[b, p] = full_value(0, row, b, p)
            return 0

        lax.fori_loop(row * GY, row * GY + GY, one, 0, unroll=8)

    def z_copy(half, b, j):
        return remote(
            fil.at[b, pl.ds(half * GY + j * CH, CH)], xg.at[b, zh, pl.ds(j * CH, CH)],
            zsend.at[half, b], zrecv.at[b, j], z_id((zl + 2 + 4 * half) % 8),
        )

    def x_copy(b, j):
        way, at = j // 2, pl.ds(j % 2 * CH, CH)
        return remote(
            xg.at[b, :, pl.ds(j * CH, CH)], (x1, x2)[way].at[b, :, at], xsend.at[b], xrecv.at[b, j], (xp, xm)[way]
        )

    def pass_on(b, j):
        way, at = j // 2, pl.ds(j % 2 * CH, CH)
        return remote(
            (x1, x2)[way].at[b, :, at], x3.at[b, :, pl.ds(j * CH, CH)], gsend.at[b], grecv.at[b, j], (xp, xm)[way]
        )

    def bytes_of(ref, sem):
        return pltpu.make_async_copy(ref, ref, sem)

    def z_to_x(b, j):
        with jax.named_scope(f'wz{b}{j}'):
            bytes_of(xg.at[b, :, pl.ds(j * CH, CH)], zrecv.at[b, j]).wait()
        x_copy(b, j).start()

    def x_to_far(b, j):
        with jax.named_scope(f'wx{b}{j}'):
            x_copy(b, j).wait_recv()
        pass_on(b, j).start()

    def second(b):
        def one(k, _):
            j = (k % 2) * 2 + k // 2
            for row in (1, 0):
                for m in range(CH):
                    p = row * GY + j * CH + m
                    fil[b, p] = full_value(1, row, b, p)
            for row in (1, 0):
                z_copy(row, b, j).start()
            return 0

        lax.fori_loop(0, NCH, one, 0)

    for b in (0, 1):
        with jax.named_scope(f'local0{b}'):
            local_part(0, 1, b)
            local_part(0, 0, b)
    for b in (0, 1):
        with jax.named_scope(f'w_h0{b}1'):
            halo_copy(0, 1, b).wait_recv()
        first(1, b)
        halo_copy(1, 0, b).start()
        with jax.named_scope(f'w_h0{b}0'):
            halo_copy(0, 0, b).wait_recv()
        first(0, b)
        halo_copy(1, 1, b).start()
        with jax.named_scope(f'local1{b}'):
            local_part(1, 1, b)
            local_part(1, 0, b)
    def finish(b):
        with jax.named_scope(f'w_h1{b}'):
            halo_copy(1, 1, b).wait_recv()
            halo_copy(1, 0, b).wait_recv()
        with jax.named_scope(f'second{b}'):
            second(b)

    finish(0)

    @pl.when(outer)
    def _():
        for j in ORDER:
            z_to_x(0, j)

    finish(1)

    @pl.when(jnp.logical_not(outer))
    def _():
        for j in ORDER:
            z_to_x(0, j)

    for j in ORDER[:3]:
        x_to_far(0, j)
    z_to_x(1, ORDER[0])
    x_to_far(0, ORDER[3])
    z_to_x(1, ORDER[1])
    z_to_x(1, ORDER[2])
    x_to_far(1, ORDER[0])
    z_to_x(1, ORDER[3])
    x_to_far(1, ORDER[1])

    def put(i, _):
        s = slot[i]
        outv[i] = jnp.concatenate([fil[0, s], fil[1, s]], axis=1)
        return 0

    with jax.named_scope('put'):
        lax.fori_loop(0, EL, put, 0, unroll=4)
    store_f = pltpu.make_async_copy(outv, out_f, lsem.at[7])
    store_f.start()

    def bound_for(x_a, b):
        return (x_a % 2) * 2 + b

    def c_copy(x_a, b):
        at = (pl.ds(0, 2), x_a // 2, bound_for(x_a, b))
        return remote(pb.at[(1 - c, *at)], rc.at[at], csend, crecv.at[x_a, b], {"c": 1 - c})

    def product(x_a, b, ref, first_row=0):
        count = ref.shape[2]
        part = pl.ds(first_row, count)
        left = jnp.concatenate([ref[b, h].reshape(count * BMAX, HB) for h in (0, 1)], axis=1)
        for zh_b in (0, 1):
            right = jnp.concatenate([xg[k, zh_b, part].reshape(count * BMAX, HB) for k in (0, 1)], axis=1)
            tile = lax.dot_general(left, right, (((0,), (0,)), ((), ())), preferred_element_type=F32).astype(BF)
            for zh_a in (0, 1):
                for core in (0, 1):
                    at = zh_a * HB + core * 64
                    pb[core, zh_a, x_a // 2, bound_for(x_a, b), zh_b] = tile[at : at + 64]
        c_copy(x_a, b).start()

    def y_copy(to, d, xh):
        return remote(
            s1.at[:, xh, to], ry.at[d - 1, xh], ysend, yrecv.at[d - 1, xh], {"y": to}
        )

    def settle(x_a, b):
        xh, to = x_a // 2, bound_for(x_a, b)
        with jax.named_scope(f'wc{b}'):
            c_copy(x_a, b).wait_recv()
        for zh_a in (0, 1):
            s1[zh_a, xh, to] = (pb[c, zh_a, xh, to].astype(F32) + rc[zh_a, xh, to].astype(F32)).astype(BF)

        @pl.when(to != y)
        def _():
            y_copy(to, (to + 4 - y) % 4, xh).start()

    def r_copy(to, src_xh):
        d = (to + 8 - z) % 8
        return remote(
            s2.at[src_xh, (to % 4) // 2, to // 4], rz.at[d - 1], rsend, rrecv, z_id(to)
        )

    def gather_y(xh):
        for d in (1, 3, 2):
            y_copy((y + d) % 4, d, xh).wait_recv()
        for zh_a in (0, 1):
            total = s1[zh_a, xh, y].astype(F32)
            for d in range(3):
                total = total + ry[d, xh, zh_a].astype(F32)
            s2[xh, zh_a] = total.astype(BF)
        for zh_a in (0, 1):
            for zh_b in (0, 1):
                to = zh_b * 4 + zh_a * 2 + xh

                @pl.when(to != z)
                def _():
                    r_copy(to, xh).start()

    def beside(b):
        product(x_prev, b, x1)
        product(x_next, b, x2, GY // 2)

    def far_unit(b):
        with jax.named_scope(f'w_far{b}'):
            for j in ORDER:
                pass_on(b, j).wait_recv()
        product(x_far, b, x3)

    with jax.named_scope('prod_e'):
        beside(0)
        product(x, 0, xg)
        product(x, 1, xg)
    x_to_far(1, ORDER[2])
    x_to_far(1, ORDER[3])
    with jax.named_scope('prod_l'):
        beside(1)
    with jax.named_scope('settle'):
        for x_a, b in ((x_prev, 0), (x_next, 0), (x_prev, 1), (x_next, 1), (x, 0), (x, 1)):
            settle(x_a, b)
    far_unit(0)
    far_unit(1)
    with jax.named_scope('settle_far'):
        settle(x_far, 0)
        settle(x_far, 1)

    with jax.named_scope('gather_y'):
        @pl.when(same)
        def _():
            gather_y(x // 2)
            gather_y(1 - x // 2)

        @pl.when(mirrored)
        def _():
            gather_y(0)
            gather_y(1)

    total = s2[zl % 2, zl // 2, zh].astype(F32)
    with jax.named_scope('wr'):
        bytes_of(rz, rrecv).wait()
    for d in range(7):
        total = total + rz[d].astype(F32)
    total = total * (1.0 / 65536.0)
    mv[...] = total

    def f_copy(s, to):
        return remote(ft.at[s], fr.at[to], fsend.at[s], frecv.at[to], mirror_id(s))

    @pl.when(mirrored)
    def _():
        turned = total.T.astype(BF)
        for s in range(4):
            ft[s] = turned[s * 64 : s * 64 + 64]
            f_copy(s, e % 4).start()
        with jax.named_scope('w_mirror'):
            for s in range(4):
                f_copy(s, s).wait_recv()
        mv[...] = mv[...] + jnp.concatenate([fr[s].astype(F32) for s in range(4)], axis=1)
        for s in range(4):
            f_copy(s, e % 4).wait_send()

    store_m = pltpu.make_async_copy(mv, out_m, lsem.at[8])
    store_m.start()

    with jax.named_scope('tail'):
        for degree in (0, 1):
            for row in (0, 1):
                for b in (0, 1):
                    halo_copy(degree, row, b).wait_send()
        for b in (0, 1):
            for k in (0, 1):
                bytes_of(fil.at[b, pl.ds(k * GY, GY)], zsend.at[k, b]).wait()
            bytes_of(xg.at[b], xsend.at[b]).wait()
            bytes_of(x3.at[b], gsend.at[b]).wait()
        bytes_of(rc, csend).wait()
        bytes_of(ry, ysend).wait()
        bytes_of(rz, rsend).wait()
        store_f.wait()
        store_m.wait()


def on_device(y_current, y_previous, h_blocks, basis_sizes, neighbours):
    any_space = pl.BlockSpec(memory_space=pl.ANY)
    dma = pltpu.SemaphoreType.DMA
    halves = pltpu.VMEM((2, EL, BMAX, HB), BF)
    met = pltpu.VMEM((2, 2, GY, BMAX, HB), BF)
    return pl.pallas_call(
        main_kernel,
        out_shape=(
            jax.ShapeDtypeStruct((EL, BMAX, BD), BF),
            jax.ShapeDtypeStruct((64, BD), F32),
        ),
        in_specs=[any_space] * 5,
        out_specs=(any_space, any_space),
        scratch_shapes=[
            pltpu.SMEM((4, EL), jnp.int32),
            pltpu.SMEM((EL,), jnp.int32),
            pltpu.SMEM((EL, 8), jnp.int32),
            pltpu.SMEM((EL,), jnp.int32),
            pltpu.SMEM((EL,), jnp.int32),
            pltpu.SMEM((EL,), jnp.int32),
            halves,
            halves,
            pltpu.VMEM((EL, BMAX, 5 * BMAX), BF),
            halves,
            halves,
            *[pltpu.VMEM((GY, BMAX, HB), BF)] * 8,
            pltpu.VMEM((2, EL, BMAX, HB), F32),
            halves,
            pltpu.VMEM((EL, BMAX, BD), BF),
            met,
            pltpu.VMEM((2, 2, GY // 2, BMAX, HB), BF),
            pltpu.VMEM((2, 2, GY // 2, BMAX, HB), BF),
            met,
            pltpu.VMEM((2, 2, 2, 4, 2, 64, BD), BF),
            pltpu.VMEM((2, 2, 4, 2, 64, BD), BF),
            pltpu.VMEM((2, 2, 4, 2, 64, BD), BF),
            pltpu.VMEM((3, 2, 2, 2, 64, BD), BF),
            pltpu.VMEM((2, 2, 2, 64, BD), BF),
            pltpu.VMEM((7, 64, BD), BF),
            pltpu.VMEM((64, BD), F32),
            pltpu.VMEM((4, 64, 64), BF),
            pltpu.VMEM((4, 64, 64), BF),
            dma((9,)),
            dma((2, 2, 2)), dma((2, 2, 2)),
            dma((2, 2)), dma((2, NCH)),
            dma((2,)), dma((2, NCH)),
            dma((2,)), dma((2, NCH)),
            dma, dma((4, 2)),
            dma, dma((3, 2)),
            dma, dma,
            dma((4,)), dma((4,)),
        ],
        compiler_params=pltpu.CompilerParams(collective_id=0, has_side_effects=True),
        name="chain",
    )(neighbours.T, basis_sizes, y_current, y_previous, h_blocks)


def solution(mesh):
    split = Mesh(mesh.devices.reshape(4, 4, 2, 2, 4), ELEM + BAND)
    return jax.shard_map(
        on_device,
        mesh=split,
        in_specs=(
            P(ELEM, None, BAND),
            P(ELEM, None, BAND),
            P(ELEM, None, None),
            P(ELEM),
            P(ELEM, None),
        ),
        out_specs=(P(ELEM, None, BAND), P(ELEM, BAND)),
        check_vma=False,
    )
```

```python
import jax
import jax.numpy as jnp
from jax import lax
from jax.experimental import pallas as pl
from jax.experimental.pallas import tpu as pltpu
from jax.sharding import Mesh
from jax.sharding import PartitionSpec as P

BMAX = 64
EL = 32
GY = 16
BD = 256
NB = 2048
ROWS = GY * BMAX
HB = 128
CH = 4
NCH = GY // CH
ORDER = (0, 2, 1, 3)

CENTER = 0.3
SCALE = 2.0 / 1.7

ELEM = ("zl", "y", "c")
BAND = ("zh", "x")
BF = jnp.bfloat16
F32 = jnp.float32
MESH_ID = pl.DeviceIdType.MESH


def ones_of(word):
    word = word - (lax.shift_right_logical(word, 1) & 0x55555555)
    word = (word & 0x33333333) + (lax.shift_right_logical(word, 2) & 0x33333333)
    word = (word + lax.shift_right_logical(word, 4)) & 0x0F0F0F0F
    return lax.shift_right_logical(word * 0x01010101, 24)


def make_tables(me, nb, sizes, tbl, slot, link, power):
    for i in range(EL):
        power[i] = jnp.int32(1 << i if i < 31 else -(1 << 31))
    ones, rows = jnp.int32(0), []
    wanted = [jnp.int32(0), jnp.int32(0)]
    for i in range(EL):
        row = jnp.where(nb[0, i] >> 5 == me, 1, 0)
        rows.append(row)
        slot[i] = jnp.where(row == 1, GY + ones, i - ones) & (EL - 1)
        ones = ones + row
        for k in (0, 1):
            wanted[k] = wanted[k] + jnp.where(row == k, power[nb[k, i] & (EL - 1)], 0)
    first = [jnp.int32(0), jnp.int32(0)]
    for i in reversed(range(EL)):
        link[i] = jnp.where(rows[i] == 1, first[1], first[0])
        first = [jnp.where(rows[i] == k, i, first[k]) for k in (0, 1)]
    for row in (0, 1):
        i = first[row]
        for p in range(row * GY, row * GY + GY):
            tbl[p, 0] = i
            tbl[p, 1] = sizes[i]
            tbl[p, 2] = slot[nb[1 - row, i] & (EL - 1)]
            tbl[p, 3] = slot[nb[2, i] & (EL - 1)]
            tbl[p, 4] = slot[nb[3, i] & (EL - 1)]
            tbl[p, 5] = ones_of(wanted[row] & (power[nb[row, i] & (EL - 1)] - 1)) & (GY - 1)
            i = link[i]


def main_kernel(
    nb_h, size_h, yc_h, yp_h, h_h, out_f, out_m, nb, sizes, tbl, slot, link, power,
    yc, yp, hv, cur0, cur1, f000, f001, f010, f011, f100, f101, f110, f111,
    acc, fil, outv, xg, x1, x2, x3, pb, rc, s1, ry, s2, rz, mv, ft, fr,
    lsem, hsend, hrecv, zsend, zrecv, xsend, xrecv, gsend, grecv, csend, crecv, ysend, yrecv, rsend, rrecv, fsend, frecv,
):
    zl, y, c = (lax.axis_index(a) for a in ELEM)
    zh, x = (lax.axis_index(a) for a in BAND)
    z = zh * 4 + zl
    e = (zl * 4 + y) * 2 + c
    outer = jnp.logical_or(y == 0, y == 3)

    def elem_id(other):
        return {"zl": other // 8, "y": (other // 2) % 4, "c": other % 2}

    def z_id(other):
        return {"zh": other // 4, "zl": other % 4}

    nxt, prv = elem_id((e + 1) % 32), elem_id((e + 31) % 32)
    x_prev, x_next, x_far = (x + 3) % 4, (x + 1) % 4, (x + 2) % 4
    xp, xm = {"x": x_next}, {"x": x_prev}

    def remote(src, dst, ss, rs, to):
        return pltpu.make_async_remote_copy(
            src_ref=src, dst_ref=dst, send_sem=ss, recv_sem=rs, device_id=to, device_id_type=MESH_ID
        )

    loads = [
        pltpu.make_async_copy(src, dst, lsem.at[k])
        for k, (src, dst) in enumerate(
            [(nb_h, nb), (size_h, sizes)]
            + [(yc_h.at[:, :, pl.ds(b * HB, HB)], yc.at[b]) for b in (0, 1)]
            + [(h_h, hv)]
            + [(yp_h.at[:, :, pl.ds(b * HB, HB)], yp.at[b]) for b in (0, 1)]
        )
    ]
    for load in loads:
        load.start()

    barrier = pltpu.get_barrier_semaphore()
    partners = [nxt, prv, xp, xm]
    partners += [{"y": (y + d) % 4} for d in (1, 2, 3)]
    partners += [z_id((z + d) % 8) for d in range(1, 8)]
    for to in partners:
        pl.semaphore_signal(barrier, inc=1, device_id=to, device_id_type=MESH_ID)

    same = y // 2 == x % 2
    mirrored = jnp.logical_not(same)
    b_rows = e // 4

    @pl.when(mirrored)
    def _():
        for other in range(8):
            for s in range(4):
                source = {**z_id(other), "y": x % 2 * 2 + s // 2, "c": s % 2, "x": b_rows % 4}
                pl.semaphore_signal(barrier, inc=1, device_id=source, device_id_type=MESH_ID)

    rows = lax.broadcasted_iota(jnp.int32, (BMAX, HB), 0)
    zero = jnp.zeros((BMAX, HB), BF)

    with jax.named_scope('w_load'):
        for load in loads[:2]:
            load.wait()
    with jax.named_scope('tables'):
        make_tables(e, nb, sizes, tbl, slot, link, power)
    for load in loads[2:4]:
        load.wait()

    def pack(row, b):
        def one(p, _):
            value = yc[b, tbl[p, 0]].astype(F32)
            cur0[b, p] = jnp.where(rows < tbl[p, 1], value, 0.0).astype(BF)
            return 0

        lax.fori_loop(row * GY, row * GY + GY, one, 0, unroll=4)

    halo = (((f000, f001), (f010, f011)), ((f100, f101), (f110, f111)))

    def halo_copy(degree, row, b):
        return remote(
            (cur0, cur1)[degree].at[b, pl.ds((1 - row) * GY, GY)], halo[degree][row][b],
            hsend.at[degree, row, b], hrecv.at[degree, row, b], (nxt, prv)[row],
        )

    with jax.named_scope('pack'):
        pack(1, 0)
    with jax.named_scope('barrier'):
        pl.semaphore_wait(barrier, len(partners) + 32 * mirrored.astype(jnp.int32))
    halo_copy(0, 0, 0).start()
    pack(0, 0)
    halo_copy(0, 1, 0).start()
    pack(1, 1)
    halo_copy(0, 0, 1).start()
    pack(0, 1)
    halo_copy(0, 1, 1).start()
    for load in loads[4:]:
        load.wait()

    def local_part(degree, row, b):
        cur = (cur0, cur1)[degree]

        def one(p, _):
            i = tbl[p, 0]
            own, n2, n3, n4 = cur[b, p], cur[b, tbl[p, 2]], cur[b, tbl[p, 3]], cur[b, tbl[p, 4]]
            pair = [zero, n2] if row == 0 else [n2, zero]
            stack = jnp.concatenate([own] + pair + [n3, n4], axis=0)
            applied = jnp.dot(hv[i], stack, preferred_element_type=F32)
            before = yp[b, i] if degree == 0 else cur0[b, p]
            acc[b, p] = SCALE * (applied - CENTER * own.astype(F32)) - before.astype(F32)
            return 0

        lax.fori_loop(row * GY, row * GY + GY, one, 0, unroll=8)

    def full_value(degree, row, b, p):
        i = tbl[p, 0]
        far = halo[degree][row][b][tbl[p, 5]]
        if row == 0:
            applied = jnp.dot(hv[i, :, 0:128], jnp.concatenate([zero, far], axis=0), preferred_element_type=F32)
        else:
            applied = jnp.dot(hv[i, :, 128:256], jnp.concatenate([far, zero], axis=0), preferred_element_type=F32)
        return jnp.where(rows < tbl[p, 1], acc[b, p] + SCALE * applied, 0.0).astype(BF)

    def first(row, b):
        def one(p, _):
            cur1[b, p] = full_value(0, row, b, p)
            return 0

        lax.fori_loop(row * GY, row * GY + GY, one, 0, unroll=8)

    def z_copy(half, b, j):
        return remote(
            fil.at[b, pl.ds(half * GY + j * CH, CH)], xg.at[b, zh, pl.ds(j * CH, CH)],
            zsend.at[half, b], zrecv.at[b, j], z_id((zl + 2 + 4 * half) % 8),
        )

    def x_copy(b, j):
        way, at = j // 2, pl.ds(j % 2 * CH, CH)
        return remote(
            xg.at[b, :, pl.ds(j * CH, CH)], (x1, x2)[way].at[b, :, at], xsend.at[b], xrecv.at[b, j], (xp, xm)[way]
        )

    def pass_on(b, j):
        way, at = j // 2, pl.ds(j % 2 * CH, CH)
        return remote(
            (x1, x2)[way].at[b, :, at], x3.at[b, :, pl.ds(j * CH, CH)], gsend.at[b], grecv.at[b, j], (xp, xm)[way]
        )

    def bytes_of(ref, sem):
        return pltpu.make_async_copy(ref, ref, sem)

    def z_to_x(b, j):
        with jax.named_scope(f'wz{b}{j}'):
            bytes_of(xg.at[b, :, pl.ds(j * CH, CH)], zrecv.at[b, j]).wait()
        x_copy(b, j).start()

    def x_to_far(b, j):
        with jax.named_scope(f'wx{b}{j}'):
            x_copy(b, j).wait_recv()
        pass_on(b, j).start()

    def second(b):
        def one(k, _):
            j = (k % 2) * 2 + k // 2
            for row in (1, 0):
                for m in range(CH):
                    p = row * GY + j * CH + m
                    fil[b, p] = full_value(1, row, b, p)
            for row in (1, 0):
                z_copy(row, b, j).start()
            return 0

        lax.fori_loop(0, NCH, one, 0)

    for b in (0, 1):
        with jax.named_scope(f'local0{b}'):
            local_part(0, 1, b)
            local_part(0, 0, b)
    for b in (0, 1):
        with jax.named_scope(f'w_h0{b}1'):
            halo_copy(0, 1, b).wait_recv()
        first(1, b)
        halo_copy(1, 0, b).start()
        with jax.named_scope(f'w_h0{b}0'):
            halo_copy(0, 0, b).wait_recv()
        first(0, b)
        halo_copy(1, 1, b).start()
        with jax.named_scope(f'local1{b}'):
            local_part(1, 1, b)
            local_part(1, 0, b)
    def finish(b):
        with jax.named_scope(f'w_h1{b}'):
            halo_copy(1, 1, b).wait_recv()
            halo_copy(1, 0, b).wait_recv()
        with jax.named_scope(f'second{b}'):
            second(b)

    finish(0)

    @pl.when(outer)
    def _():
        for j in ORDER:
            z_to_x(0, j)

    finish(1)

    @pl.when(jnp.logical_not(outer))
    def _():
        for j in ORDER:
            z_to_x(0, j)

    for j in ORDER[:3]:
        x_to_far(0, j)
    z_to_x(1, ORDER[0])
    x_to_far(0, ORDER[3])
    for j in ORDER[1:]:
        z_to_x(1, j)

    def put(i, _):
        s = slot[i]
        outv[i] = jnp.concatenate([fil[0, s], fil[1, s]], axis=1)
        return 0

    def bound_for(x_a, b):
        return (x_a % 2) * 2 + b

    def c_copy(x_a, b):
        at = (pl.ds(0, 2), x_a // 2, bound_for(x_a, b))
        return remote(pb.at[(1 - c, *at)], rc.at[at], csend, crecv.at[x_a, b], {"c": 1 - c})

    def product(x_a, b, ref, first_row=0):
        count = ref.shape[2]
        part = pl.ds(first_row, count)
        left = jnp.concatenate([ref[b, h].reshape(count * BMAX, HB) for h in (0, 1)], axis=1)
        for zh_b in (0, 1):
            right = jnp.concatenate([xg[k, zh_b, part].reshape(count * BMAX, HB) for k in (0, 1)], axis=1)
            tile = lax.dot_general(left, right, (((0,), (0,)), ((), ())), preferred_element_type=F32).astype(BF)
            for zh_a in (0, 1):
                for core in (0, 1):
                    at = zh_a * HB + core * 64
                    pb[core, zh_a, x_a // 2, bound_for(x_a, b), zh_b] = tile[at : at + 64]
        c_copy(x_a, b).start()

    def y_copy(to, d, xh):
        return remote(
            s1.at[:, xh, to], ry.at[d - 1, xh], ysend, yrecv.at[d - 1, xh], {"y": to}
        )

    def settle(x_a, b):
        xh, to = x_a // 2, bound_for(x_a, b)
        with jax.named_scope(f'wc{b}'):
            c_copy(x_a, b).wait_recv()
        for zh_a in (0, 1):
            s1[zh_a, xh, to] = (pb[c, zh_a, xh, to].astype(F32) + rc[zh_a, xh, to].astype(F32)).astype(BF)

        @pl.when(to != y)
        def _():
            y_copy(to, (to + 4 - y) % 4, xh).start()

    def r_copy(to, src_xh):
        d = (to + 8 - z) % 8
        return remote(
            s2.at[src_xh, (to % 4) // 2, to // 4], rz.at[d - 1], rsend, rrecv, z_id(to)
        )

    def f_copy(xh, zh_a, zh_b, s):
        tile_rows, tile_columns = (zh_a * 2 + xh) * 2 + y // 2, zh_b * 4 + x
        to = {**elem_id(4 * tile_columns + s), "zh": tile_rows // 4, "x": tile_rows % 4}
        return remote(ft.at[xh, zh_a, zh_b, s], fr.at[e % 4, z], fsend, frecv, to)

    def gather_y(xh):
        for d in (1, 3, 2):
            y_copy((y + d) % 4, d, xh).wait_recv()
        for zh_a in (0, 1):
            total = s1[zh_a, xh, y].astype(F32)
            for d in range(3):
                total = total + ry[d, xh, zh_a].astype(F32)
            s2[xh, zh_a] = total.astype(BF)
        for zh_a in (0, 1):
            for zh_b in (0, 1):
                to = zh_b * 4 + zh_a * 2 + xh

                @pl.when(to != z)
                def _():
                    r_copy(to, xh).start()

        @pl.when(mirrored)
        def _():
            for zh_a in (0, 1):
                for zh_b in (0, 1):
                    turned = s2[xh, zh_a, zh_b].astype(F32).T.astype(BF)
                    for s in range(4):
                        ft[xh, zh_a, zh_b, s] = turned[s * 64 : s * 64 + 64]
                        f_copy(xh, zh_a, zh_b, s).start()

    def beside(b):
        product(x_prev, b, x1)
        product(x_next, b, x2, GY // 2)

    def far_unit(b):
        with jax.named_scope(f'w_far{b}'):
            for j in ORDER:
                pass_on(b, j).wait_recv()
        product(x_far, b, x3)

    with jax.named_scope('prod_e'):
        beside(0)
        product(x, 0, xg)
        product(x, 1, xg)
    with jax.named_scope('settle_e'):
        for x_a, b in ((x_prev, 0), (x_next, 0), (x, 0), (x, 1)):
            settle(x_a, b)
    for j in ORDER:
        x_to_far(1, j)
    with jax.named_scope('put'):
        lax.fori_loop(0, EL, put, 0, unroll=4)
    store_f = pltpu.make_async_copy(outv, out_f, lsem.at[7])
    store_f.start()

    with jax.named_scope('prod_l'):
        beside(1)
    with jax.named_scope('settle_l'):
        settle(x_prev, 1)
        settle(x_next, 1)
    far_unit(0)
    with jax.named_scope('settle_f0'):
        settle(x_far, 0)
    far_unit(1)
    with jax.named_scope('settle_f1'):
        settle(x_far, 1)

    with jax.named_scope('gather_y'):
        @pl.when(same)
        def _():
            gather_y(x // 2)
            gather_y(1 - x // 2)

        @pl.when(mirrored)
        def _():
            gather_y(0)
            gather_y(1)

    total = s2[zl % 2, zl // 2, zh].astype(F32)
    with jax.named_scope('wr'):
        bytes_of(rz, rrecv).wait()
    for d in range(7):
        total = total + rz[d].astype(F32)
    mv[...] = total * (1.0 / 65536.0)

    @pl.when(mirrored)
    def _():
        with jax.named_scope('w_mirror'):
            bytes_of(fr, frecv).wait()
        parts = []
        for s in range(4):
            part = fr[s, 0].astype(F32)
            for other in range(1, 8):
                part = part + fr[s, other].astype(F32)
            parts.append(part)
        mv[...] = mv[...] + jnp.concatenate(parts, axis=1) * (1.0 / 65536.0)
        bytes_of(fr, fsend).wait()

    store_m = pltpu.make_async_copy(mv, out_m, lsem.at[8])
    store_m.start()

    with jax.named_scope('tail'):
        for degree in (0, 1):
            for row in (0, 1):
                for b in (0, 1):
                    halo_copy(degree, row, b).wait_send()
        for b in (0, 1):
            for k in (0, 1):
                bytes_of(fil.at[b, pl.ds(k * GY, GY)], zsend.at[k, b]).wait()
            bytes_of(xg.at[b], xsend.at[b]).wait()
            bytes_of(x3.at[b], gsend.at[b]).wait()
        bytes_of(rc, csend).wait()
        bytes_of(ry, ysend).wait()
        bytes_of(rz, rsend).wait()
        store_f.wait()
        store_m.wait()


def on_device(y_current, y_previous, h_blocks, basis_sizes, neighbours):
    any_space = pl.BlockSpec(memory_space=pl.ANY)
    dma = pltpu.SemaphoreType.DMA
    halves = pltpu.VMEM((2, EL, BMAX, HB), BF)
    met = pltpu.VMEM((2, 2, GY, BMAX, HB), BF)
    return pl.pallas_call(
        main_kernel,
        out_shape=(
            jax.ShapeDtypeStruct((EL, BMAX, BD), BF),
            jax.ShapeDtypeStruct((64, BD), F32),
        ),
        in_specs=[any_space] * 5,
        out_specs=(any_space, any_space),
        scratch_shapes=[
            pltpu.SMEM((4, EL), jnp.int32),
            pltpu.SMEM((EL,), jnp.int32),
            pltpu.SMEM((EL, 8), jnp.int32),
            pltpu.SMEM((EL,), jnp.int32),
            pltpu.SMEM((EL,), jnp.int32),
            pltpu.SMEM((EL,), jnp.int32),
            halves,
            halves,
            pltpu.VMEM((EL, BMAX, 5 * BMAX), BF),
            halves,
            halves,
            *[pltpu.VMEM((GY, BMAX, HB), BF)] * 8,
            pltpu.VMEM((2, EL, BMAX, HB), F32),
            halves,
            pltpu.VMEM((EL, BMAX, BD), BF),
            met,
            pltpu.VMEM((2, 2, GY // 2, BMAX, HB), BF),
            pltpu.VMEM((2, 2, GY // 2, BMAX, HB), BF),
            met,
            pltpu.VMEM((2, 2, 2, 4, 2, 64, BD), BF),
            pltpu.VMEM((2, 2, 4, 2, 64, BD), BF),
            pltpu.VMEM((2, 2, 4, 2, 64, BD), BF),
            pltpu.VMEM((3, 2, 2, 2, 64, BD), BF),
            pltpu.VMEM((2, 2, 2, 64, BD), BF),
            pltpu.VMEM((7, 64, BD), BF),
            pltpu.VMEM((64, BD), F32),
            pltpu.VMEM((2, 2, 2, 4, 64, 64), BF),
            pltpu.VMEM((4, 8, 64, 64), BF),
            dma((9,)),
            dma((2, 2, 2)), dma((2, 2, 2)),
            dma((2, 2)), dma((2, NCH)),
            dma((2,)), dma((2, NCH)),
            dma((2,)), dma((2, NCH)),
            dma, dma((4, 2)),
            dma, dma((3, 2)),
            dma, dma,
            dma, dma,
        ],
        compiler_params=pltpu.CompilerParams(collective_id=0, has_side_effects=True),
        name="chain",
    )(neighbours.T, basis_sizes, y_current, y_previous, h_blocks)


def solution(mesh):
    split = Mesh(mesh.devices.reshape(4, 4, 2, 2, 4), ELEM + BAND)
    return jax.shard_map(
        on_device,
        mesh=split,
        in_specs=(
            P(ELEM, None, BAND),
            P(ELEM, None, BAND),
            P(ELEM, None, None),
            P(ELEM),
            P(ELEM, None),
        ),
        out_specs=(P(ELEM, None, BAND), P(ELEM, BAND)),
        check_vma=False,
    )
```

```python
import jax
import jax.numpy as jnp
from jax import lax
from jax.experimental import pallas as pl
from jax.experimental.pallas import tpu as pltpu
from jax.sharding import Mesh
from jax.sharding import PartitionSpec as P

BMAX = 64
EL = 32
GY = 16
BD = 256
NB = 2048
ROWS = GY * BMAX
HB = 128
CH = 4
NCH = GY // CH
ORDER = (0, 2, 1, 3)

CENTER = 0.3
SCALE = 2.0 / 1.7

ELEM = ("zl", "y", "c")
BAND = ("zh", "x")
BF = jnp.bfloat16
F32 = jnp.float32
MESH_ID = pl.DeviceIdType.MESH


def ones_of(word):
    word = word - (lax.shift_right_logical(word, 1) & 0x55555555)
    word = (word & 0x33333333) + (lax.shift_right_logical(word, 2) & 0x33333333)
    word = (word + lax.shift_right_logical(word, 4)) & 0x0F0F0F0F
    return lax.shift_right_logical(word * 0x01010101, 24)


def make_tables(me, nb, sizes, tbl, slot, link, power):
    for i in range(EL):
        power[i] = jnp.int32(1 << i if i < 31 else -(1 << 31))
    ones, rows = jnp.int32(0), []
    wanted = [jnp.int32(0), jnp.int32(0)]
    for i in range(EL):
        row = jnp.where(nb[0, i] >> 5 == me, 1, 0)
        rows.append(row)
        slot[i] = jnp.where(row == 1, GY + ones, i - ones) & (EL - 1)
        ones = ones + row
        for k in (0, 1):
            wanted[k] = wanted[k] + jnp.where(row == k, power[nb[k, i] & (EL - 1)], 0)
    first = [jnp.int32(0), jnp.int32(0)]
    for i in reversed(range(EL)):
        link[i] = jnp.where(rows[i] == 1, first[1], first[0])
        first = [jnp.where(rows[i] == k, i, first[k]) for k in (0, 1)]
    for row in (0, 1):
        i = first[row]
        for p in range(row * GY, row * GY + GY):
            tbl[p, 0] = i
            tbl[p, 1] = sizes[i]
            tbl[p, 2] = slot[nb[1 - row, i] & (EL - 1)]
            tbl[p, 3] = slot[nb[2, i] & (EL - 1)]
            tbl[p, 4] = slot[nb[3, i] & (EL - 1)]
            tbl[p, 5] = ones_of(wanted[row] & (power[nb[row, i] & (EL - 1)] - 1)) & (GY - 1)
            i = link[i]


def main_kernel(
    nb_h, size_h, yc_h, yp_h, h_h, out_f, out_m, nb, sizes, tbl, slot, link, power,
    yc, yp, hv, cur0, cur1, f000, f001, f010, f011, f100, f101, f110, f111,
    acc, fil, outv, xg, x1, x2, x3, pb, rc, s1, ry, s2, rz, mv,
    lsem, hsend, hrecv, zsend, zrecv, xsend, xrecv, gsend, grecv, csend, crecv, ysend, yrecv, rsend, rrecv,
):
    zl, y, c = (lax.axis_index(a) for a in ELEM)
    zh, x = (lax.axis_index(a) for a in BAND)
    z = zh * 4 + zl
    e = (zl * 4 + y) * 2 + c
    outer = jnp.logical_or(y == 0, y == 3)

    def elem_id(other):
        return {"zl": other // 8, "y": (other // 2) % 4, "c": other % 2}

    def z_id(other):
        return {"zh": other // 4, "zl": other % 4}

    nxt, prv = elem_id((e + 1) % 32), elem_id((e + 31) % 32)
    x_prev, x_next, x_far = (x + 3) % 4, (x + 1) % 4, (x + 2) % 4
    xp, xm = {"x": x_next}, {"x": x_prev}

    def remote(src, dst, ss, rs, to):
        return pltpu.make_async_remote_copy(
            src_ref=src, dst_ref=dst, send_sem=ss, recv_sem=rs, device_id=to, device_id_type=MESH_ID
        )

    loads = [
        pltpu.make_async_copy(src, dst, lsem.at[k])
        for k, (src, dst) in enumerate(
            [(nb_h, nb), (size_h, sizes)]
            + [(yc_h.at[:, :, pl.ds(b * HB, HB)], yc.at[b]) for b in (0, 1)]
            + [(h_h, hv)]
            + [(yp_h.at[:, :, pl.ds(b * HB, HB)], yp.at[b]) for b in (0, 1)]
        )
    ]
    for load in loads:
        load.start()

    barrier = pltpu.get_barrier_semaphore()
    partners = [nxt, prv, xp, xm]
    partners += [{"y": (y + d) % 4} for d in (1, 2, 3)]
    partners += [z_id((z + d) % 8) for d in range(1, 8)]
    for to in partners:
        pl.semaphore_signal(barrier, inc=1, device_id=to, device_id_type=MESH_ID)

    rows = lax.broadcasted_iota(jnp.int32, (BMAX, HB), 0)
    zero = jnp.zeros((BMAX, HB), BF)

    with jax.named_scope('w_load'):
        for load in loads[:2]:
            load.wait()
    with jax.named_scope('tables'):
        make_tables(e, nb, sizes, tbl, slot, link, power)
    for load in loads[2:4]:
        load.wait()

    def pack(row, b):
        def one(p, _):
            value = yc[b, tbl[p, 0]].astype(F32)
            cur0[b, p] = jnp.where(rows < tbl[p, 1], value, 0.0).astype(BF)
            return 0

        lax.fori_loop(row * GY, row * GY + GY, one, 0, unroll=4)

    halo = (((f000, f001), (f010, f011)), ((f100, f101), (f110, f111)))

    def halo_copy(degree, row, b):
        return remote(
            (cur0, cur1)[degree].at[b, pl.ds((1 - row) * GY, GY)], halo[degree][row][b],
            hsend.at[degree, row, b], hrecv.at[degree, row, b], (nxt, prv)[row],
        )

    with jax.named_scope('pack'):
        pack(1, 0)
    with jax.named_scope('barrier'):
        pl.semaphore_wait(barrier, len(partners))
    halo_copy(0, 0, 0).start()
    pack(0, 0)
    halo_copy(0, 1, 0).start()
    pack(1, 1)
    halo_copy(0, 0, 1).start()
    pack(0, 1)
    halo_copy(0, 1, 1).start()
    for load in loads[4:]:
        load.wait()

    def local_part(degree, row, b):
        cur = (cur0, cur1)[degree]

        def one(p, _):
            i = tbl[p, 0]
            own, n2, n3, n4 = cur[b, p], cur[b, tbl[p, 2]], cur[b, tbl[p, 3]], cur[b, tbl[p, 4]]
            pair = [zero, n2] if row == 0 else [n2, zero]
            stack = jnp.concatenate([own] + pair + [n3, n4], axis=0)
            applied = jnp.dot(hv[i], stack, preferred_element_type=F32)
            before = yp[b, i] if degree == 0 else cur0[b, p]
            acc[b, p] = SCALE * (applied - CENTER * own.astype(F32)) - before.astype(F32)
            return 0

        lax.fori_loop(row * GY, row * GY + GY, one, 0, unroll=8)

    def full_value(degree, row, b, p):
        i = tbl[p, 0]
        far = halo[degree][row][b][tbl[p, 5]]
        if row == 0:
            applied = jnp.dot(hv[i, :, 0:128], jnp.concatenate([zero, far], axis=0), preferred_element_type=F32)
        else:
            applied = jnp.dot(hv[i, :, 128:256], jnp.concatenate([far, zero], axis=0), preferred_element_type=F32)
        return jnp.where(rows < tbl[p, 1], acc[b, p] + SCALE * applied, 0.0).astype(BF)

    def first(row, b):
        def one(p, _):
            cur1[b, p] = full_value(0, row, b, p)
            return 0

        lax.fori_loop(row * GY, row * GY + GY, one, 0, unroll=8)

    def z_copy(b, j):
        return remote(
            fil.at[b, pl.ds((1 - zh) * GY + j * CH, CH)], xg.at[b, zh, pl.ds(j * CH, CH)],
            zsend.at[b], zrecv.at[b, j], {"zh": 1 - zh},
        )

    def x_copy(way, b, j, kind):
        part = pl.ds(j * CH, CH)
        h = (zh, 1 - zh)[kind]
        src = fil.at[b, pl.ds(zh * GY + j * CH, CH)] if kind == 0 else xg.at[b, h, part]
        return remote(
            src, (x1, x2)[way].at[b, h, part], xsend.at[way, b], xrecv.at[way, b, j, kind], (xp, xm)[way]
        )

    def pass_on(b, j, kind):
        part, way, h = pl.ds(j * CH, CH), j // 2, (zh, 1 - zh)[kind]
        return remote(
            (x1, x2)[way].at[b, h, part], x3.at[b, h, part], gsend.at[b], grecv.at[b, j, kind], (xp, xm)[way]
        )

    def bytes_of(ref, sem):
        return pltpu.make_async_copy(ref, ref, sem)

    def z_to_x(b):
        for j in ORDER:
            with jax.named_scope(f'wz{b}{j}'):
                z_copy(b, j).wait_recv()
            x_copy(0, b, j, 1).start()
            x_copy(1, b, j, 1).start()

    def second(b):
        for j in ORDER:
            for row in (1, 0):
                for m in range(CH):
                    p = row * GY + j * CH + m
                    fil[b, p] = full_value(1, row, b, p)
            z_copy(b, j).start()
            x_copy(0, b, j, 0).start()
            x_copy(1, b, j, 0).start()
        xg[b, zh] = fil[b, pl.ds(zh * GY, GY)]

    def pass_half(b, kind):
        for j in ORDER:
            with jax.named_scope(f'wx{b}{kind}{j}'):
                x_copy(j // 2, b, j, kind).wait_recv()
            pass_on(b, j, kind).start()

    for b in (0, 1):
        with jax.named_scope(f'local0{b}'):
            local_part(0, 1, b)
            local_part(0, 0, b)
    for b in (0, 1):
        with jax.named_scope(f'w_h0{b}1'):
            halo_copy(0, 1, b).wait_recv()
        first(1, b)
        halo_copy(1, 0, b).start()
        with jax.named_scope(f'w_h0{b}0'):
            halo_copy(0, 0, b).wait_recv()
        first(0, b)
        halo_copy(1, 1, b).start()
        with jax.named_scope(f'local1{b}'):
            local_part(1, 1, b)
            local_part(1, 0, b)
    def finish(b):
        with jax.named_scope(f'w_h1{b}'):
            halo_copy(1, 1, b).wait_recv()
            halo_copy(1, 0, b).wait_recv()
        with jax.named_scope(f'second{b}'):
            second(b)

    finish(0)

    @pl.when(outer)
    def _():
        z_to_x(0)
        pass_half(0, 0)

    finish(1)

    @pl.when(jnp.logical_not(outer))
    def _():
        z_to_x(0)
        pass_half(0, 0)

    pass_half(1, 0)
    z_to_x(1)

    def put(i, _):
        s = slot[i]
        outv[i] = jnp.concatenate([fil[0, s], fil[1, s]], axis=1)
        return 0

    with jax.named_scope('put'):
        lax.fori_loop(0, EL, put, 0, unroll=4)
    store_f = pltpu.make_async_copy(outv, out_f, lsem.at[7])
    store_f.start()

    def bound_for(x_a, b):
        return (x_a % 2) * 2 + b

    def c_copy(x_a, b):
        at = (pl.ds(0, 2), x_a // 2, bound_for(x_a, b))
        return remote(pb.at[(1 - c, *at)], rc.at[at], csend, crecv.at[x_a, b], {"c": 1 - c})

    def product(x_a, b, ref):
        left = jnp.concatenate([ref[b, h].reshape(GY * BMAX, HB) for h in (0, 1)], axis=1)
        for zh_b in (0, 1):
            right = jnp.concatenate([xg[k, zh_b].reshape(GY * BMAX, HB) for k in (0, 1)], axis=1)
            tile = lax.dot_general(left, right, (((0,), (0,)), ((), ())), preferred_element_type=F32).astype(BF)
            for zh_a in (0, 1):
                for core in (0, 1):
                    at = zh_a * HB + core * 64
                    pb[core, zh_a, x_a // 2, bound_for(x_a, b), zh_b] = tile[at : at + 64]
        c_copy(x_a, b).start()

    def y_copy(to, d, xh):
        return remote(
            s1.at[:, xh, to], ry.at[d - 1, xh], ysend, yrecv.at[d - 1, xh], {"y": to}
        )

    def settle(x_a, b):
        xh, to = x_a // 2, bound_for(x_a, b)
        with jax.named_scope(f'wc{b}'):
            c_copy(x_a, b).wait_recv()
        for zh_a in (0, 1):
            s1[zh_a, xh, to] = (pb[c, zh_a, xh, to].astype(F32) + rc[zh_a, xh, to].astype(F32)).astype(BF)

        @pl.when(to != y)
        def _():
            y_copy(to, (to + 4 - y) % 4, xh).start()

    def r_copy(to, src_xh):
        d = (to + 8 - z) % 8
        return remote(
            s2.at[src_xh, (to % 4) // 2, to // 4], rz.at[d - 1], rsend, rrecv, z_id(to)
        )

    def gather_y(xh):
        for d in (1, 3, 2):
            y_copy((y + d) % 4, d, xh).wait_recv()
        for zh_a in (0, 1):
            total = s1[zh_a, xh, y].astype(F32)
            for d in range(3):
                total = total + ry[d, xh, zh_a].astype(F32)
            s2[xh, zh_a] = total.astype(BF)
        for zh_a in (0, 1):
            for zh_b in (0, 1):
                to = zh_b * 4 + zh_a * 2 + xh

                @pl.when(to != z)
                def _():
                    r_copy(to, xh).start()

    def beside(b):
        for way in (0, 1):
            with jax.named_scope(f'w_x{way}'):
                for j in ((2, 3), (0, 1))[way]:
                    for kind in (0, 1):
                        x_copy(way, b, j, kind).wait_recv()
            product((x_prev, x_next)[way], b, (x1, x2)[way])

    def far_unit(b):
        with jax.named_scope(f'w_far{b}'):
            for j in ORDER:
                for kind in (0, 1):
                    pass_on(b, j, kind).wait_recv()
        product(x_far, b, x3)
        settle(x_far, b)

    same = y // 2 == x % 2
    pass_half(0, 1)
    with jax.named_scope('prod_e'):
        product(x, 0, xg)
        product(x, 1, xg)
        beside(0)
    with jax.named_scope('settle_e'):
        settle(x, 0)
        settle(x, 1)
        settle(x_prev, 0)
        settle(x_next, 0)
    pass_half(1, 1)
    with jax.named_scope('prod_l'):
        beside(1)
    with jax.named_scope('settle_l'):
        settle(x_prev, 1)
        settle(x_next, 1)
    far_unit(0)
    far_unit(1)

    with jax.named_scope('gather_y1'):
        @pl.when(same)
        def _():
            gather_y(x // 2)

        @pl.when(jnp.logical_not(same))
        def _():
            gather_y(0)
            gather_y(1)

    with jax.named_scope('gather_y2'):
        @pl.when(same)
        def _():
            gather_y(1 - x // 2)

    total = s2[zl % 2, zl // 2, zh].astype(F32)
    with jax.named_scope('wr'):
        bytes_of(rz, rrecv).wait()
    for d in range(7):
        total = total + rz[d].astype(F32)
    mv[...] = total * (1.0 / 65536.0)
    store_m = pltpu.make_async_copy(mv, out_m, lsem.at[8])
    store_m.start()

    with jax.named_scope('tail'):
        for degree in (0, 1):
            for row in (0, 1):
                for b in (0, 1):
                    halo_copy(degree, row, b).wait_send()
        for b in (0, 1):
            for k in (0, 1):
                bytes_of(xg.at[b], xsend.at[k, b]).wait()
            bytes_of(x3.at[b], gsend.at[b]).wait()
            bytes_of(fil.at[b, pl.ds(0, GY)], zsend.at[b]).wait()
        bytes_of(rc, csend).wait()
        bytes_of(ry, ysend).wait()
        bytes_of(rz, rsend).wait()
        store_f.wait()
        store_m.wait()


def on_device(y_current, y_previous, h_blocks, basis_sizes, neighbours):
    any_space = pl.BlockSpec(memory_space=pl.ANY)
    dma = pltpu.SemaphoreType.DMA
    halves = pltpu.VMEM((2, EL, BMAX, HB), BF)
    met = pltpu.VMEM((2, 2, GY, BMAX, HB), BF)
    return pl.pallas_call(
        main_kernel,
        out_shape=(
            jax.ShapeDtypeStruct((EL, BMAX, BD), BF),
            jax.ShapeDtypeStruct((64, BD), F32),
        ),
        in_specs=[any_space] * 5,
        out_specs=(any_space, any_space),
        scratch_shapes=[
            pltpu.SMEM((4, EL), jnp.int32),
            pltpu.SMEM((EL,), jnp.int32),
            pltpu.SMEM((EL, 8), jnp.int32),
            pltpu.SMEM((EL,), jnp.int32),
            pltpu.SMEM((EL,), jnp.int32),
            pltpu.SMEM((EL,), jnp.int32),
            halves,
            halves,
            pltpu.VMEM((EL, BMAX, 5 * BMAX), BF),
            halves,
            halves,
            *[pltpu.VMEM((GY, BMAX, HB), BF)] * 8,
            pltpu.VMEM((2, EL, BMAX, HB), F32),
            halves,
            pltpu.VMEM((EL, BMAX, BD), BF),
            met,
            met,
            met,
            met,
            pltpu.VMEM((2, 2, 2, 4, 2, 64, BD), BF),
            pltpu.VMEM((2, 2, 4, 2, 64, BD), BF),
            pltpu.VMEM((2, 2, 4, 2, 64, BD), BF),
            pltpu.VMEM((3, 2, 2, 2, 64, BD), BF),
            pltpu.VMEM((2, 2, 2, 64, BD), BF),
            pltpu.VMEM((7, 64, BD), BF),
            pltpu.VMEM((64, BD), F32),
            dma((9,)),
            dma((2, 2, 2)), dma((2, 2, 2)),
            dma((2,)), dma((2, NCH)),
            dma((2, 2)), dma((2, 2, NCH, 2)),
            dma((2,)), dma((2, NCH, 2)),
            dma, dma((4, 2)),
            dma, dma((3, 2)),
            dma, dma,
        ],
        compiler_params=pltpu.CompilerParams(collective_id=0, has_side_effects=True),
        name="chain",
    )(neighbours.T, basis_sizes, y_current, y_previous, h_blocks)


def solution(mesh):
    split = Mesh(mesh.devices.reshape(4, 4, 2, 2, 4), ELEM + BAND)
    return jax.shard_map(
        on_device,
        mesh=split,
        in_specs=(
            P(ELEM, None, BAND),
            P(ELEM, None, BAND),
            P(ELEM, None, None),
            P(ELEM),
            P(ELEM, None),
        ),
        out_specs=(P(ELEM, None, BAND), P(ELEM, BAND)),
        check_vma=False,
    )
```

```python
import jax
import jax.numpy as jnp
from jax import lax
from jax.experimental import pallas as pl
from jax.experimental.pallas import tpu as pltpu
from jax.sharding import Mesh
from jax.sharding import PartitionSpec as P

BMAX = 64
EL = 32
GY = 16
BD = 256
NB = 2048
ROWS = GY * BMAX
HB = 128
CH = 4
NCH = GY // CH
ORDER = (0, 2, 1, 3)

CENTER = 0.3
SCALE = 2.0 / 1.7

ELEM = ("zl", "y", "c")
BAND = ("zh", "x")
BF = jnp.bfloat16
F32 = jnp.float32
MESH_ID = pl.DeviceIdType.MESH


def ones_of(word):
    word = word - (lax.shift_right_logical(word, 1) & 0x55555555)
    word = (word & 0x33333333) + (lax.shift_right_logical(word, 2) & 0x33333333)
    word = (word + lax.shift_right_logical(word, 4)) & 0x0F0F0F0F
    return lax.shift_right_logical(word * 0x01010101, 24)


def make_tables(me, nb, sizes, tbl, slot, link, power):
    for i in range(EL):
        power[i] = jnp.int32(1 << i if i < 31 else -(1 << 31))
    ones, rows = jnp.int32(0), []
    wanted = [jnp.int32(0), jnp.int32(0)]
    for i in range(EL):
        row = jnp.where(nb[0, i] >> 5 == me, 1, 0)
        rows.append(row)
        slot[i] = jnp.where(row == 1, GY + ones, i - ones) & (EL - 1)
        ones = ones + row
        for k in (0, 1):
            wanted[k] = wanted[k] + jnp.where(row == k, power[nb[k, i] & (EL - 1)], 0)
    first = [jnp.int32(0), jnp.int32(0)]
    for i in reversed(range(EL)):
        link[i] = jnp.where(rows[i] == 1, first[1], first[0])
        first = [jnp.where(rows[i] == k, i, first[k]) for k in (0, 1)]
    for row in (0, 1):
        i = first[row]
        for p in range(row * GY, row * GY + GY):
            tbl[p, 0] = i
            tbl[p, 1] = sizes[i]
            tbl[p, 2] = slot[nb[1 - row, i] & (EL - 1)]
            tbl[p, 3] = slot[nb[2, i] & (EL - 1)]
            tbl[p, 4] = slot[nb[3, i] & (EL - 1)]
            tbl[p, 5] = ones_of(wanted[row] & (power[nb[row, i] & (EL - 1)] - 1)) & (GY - 1)
            i = link[i]


def main_kernel(
    nb_h, size_h, yc_h, yp_h, h_h, out_f, out_m, nb, sizes, tbl, slot, link, power,
    yc, yp, hv, cur0, cur1, f000, f001, f010, f011, f100, f101, f110, f111,
    acc, fil, outv, xg, x1, x2, x3, pb, rc, s1, ry, s2, rz, mv,
    lsem, hsend, hrecv, zsend, zrecv, xsend, xrecv, gsend, grecv, csend, crecv, ysend, yrecv, rsend, rrecv, gate,
):
    zl, y, c = (lax.axis_index(a) for a in ELEM)
    zh, x = (lax.axis_index(a) for a in BAND)
    z = zh * 4 + zl
    e = (zl * 4 + y) * 2 + c
    outer = jnp.logical_or(y == 0, y == 3)
    crossing = jnp.logical_or(jnp.logical_and(y == 0, c == 0), jnp.logical_and(y == 3, c == 1))
    last = jnp.logical_or(jnp.logical_and(y == 0, zl == 0), jnp.logical_and(y == 3, zl == 3))
    held = jnp.logical_and(outer, jnp.logical_not(last))

    def elem_id(other):
        return {"zl": other // 8, "y": (other // 2) % 4, "c": other % 2}

    def z_id(other):
        return {"zh": other // 4, "zl": other % 4}

    nxt, prv = elem_id((e + 1) % 32), elem_id((e + 31) % 32)
    x_prev, x_next, x_far = (x + 3) % 4, (x + 1) % 4, (x + 2) % 4
    xp, xm = {"x": x_next}, {"x": x_prev}

    def remote(src, dst, ss, rs, to):
        return pltpu.make_async_remote_copy(
            src_ref=src, dst_ref=dst, send_sem=ss, recv_sem=rs, device_id=to, device_id_type=MESH_ID
        )

    loads = [
        pltpu.make_async_copy(src, dst, lsem.at[k])
        for k, (src, dst) in enumerate(
            [(nb_h, nb), (size_h, sizes)]
            + [(yc_h.at[:, :, pl.ds(b * HB, HB)], yc.at[b]) for b in (0, 1)]
            + [(h_h, hv)]
            + [(yp_h.at[:, :, pl.ds(b * HB, HB)], yp.at[b]) for b in (0, 1)]
        )
    ]
    for load in loads:
        load.start()

    barrier = pltpu.get_barrier_semaphore()
    partners = [nxt, prv, xp, xm]
    partners += [{"y": (y + d) % 4} for d in (1, 2, 3)]
    partners += [z_id((z + d) % 8) for d in range(1, 8)]
    for to in partners:
        pl.semaphore_signal(barrier, inc=1, device_id=to, device_id_type=MESH_ID)

    rows = lax.broadcasted_iota(jnp.int32, (BMAX, HB), 0)
    zero = jnp.zeros((BMAX, HB), BF)

    with jax.named_scope('w_load'):
        for load in loads[:2]:
            load.wait()
    with jax.named_scope('tables'):
        make_tables(e, nb, sizes, tbl, slot, link, power)
    for load in loads[2:4]:
        load.wait()

    def pack(row, b):
        def one(p, _):
            value = yc[b, tbl[p, 0]].astype(F32)
            cur0[b, p] = jnp.where(rows < tbl[p, 1], value, 0.0).astype(BF)
            return 0

        lax.fori_loop(row * GY, row * GY + GY, one, 0, unroll=4)

    halo = (((f000, f001), (f010, f011)), ((f100, f101), (f110, f111)))

    def halo_copy(degree, row, b):
        return remote(
            (cur0, cur1)[degree].at[b, pl.ds((1 - row) * GY, GY)], halo[degree][row][b],
            hsend.at[degree, row, b], hrecv.at[degree, row, b], (nxt, prv)[row],
        )

    with jax.named_scope('pack'):
        pack(1, 0)
    with jax.named_scope('barrier'):
        pl.semaphore_wait(barrier, len(partners))
    halo_copy(0, 0, 0).start()
    pack(0, 0)
    halo_copy(0, 1, 0).start()
    pack(1, 1)
    halo_copy(0, 0, 1).start()
    pack(0, 1)
    halo_copy(0, 1, 1).start()
    for load in loads[4:]:
        load.wait()

    def local_part(degree, row, b):
        cur = (cur0, cur1)[degree]

        def one(p, _):
            i = tbl[p, 0]
            own, n2, n3, n4 = cur[b, p], cur[b, tbl[p, 2]], cur[b, tbl[p, 3]], cur[b, tbl[p, 4]]
            pair = [zero, n2] if row == 0 else [n2, zero]
            stack = jnp.concatenate([own] + pair + [n3, n4], axis=0)
            applied = jnp.dot(hv[i], stack, preferred_element_type=F32)
            before = yp[b, i] if degree == 0 else cur0[b, p]
            acc[b, p] = SCALE * (applied - CENTER * own.astype(F32)) - before.astype(F32)
            return 0

        lax.fori_loop(row * GY, row * GY + GY, one, 0, unroll=8)

    def full_value(degree, row, b, p):
        i = tbl[p, 0]
        far = halo[degree][row][b][tbl[p, 5]]
        if row == 0:
            applied = jnp.dot(hv[i, :, 0:128], jnp.concatenate([zero, far], axis=0), preferred_element_type=F32)
        else:
            applied = jnp.dot(hv[i, :, 128:256], jnp.concatenate([far, zero], axis=0), preferred_element_type=F32)
        return jnp.where(rows < tbl[p, 1], acc[b, p] + SCALE * applied, 0.0).astype(BF)

    def first(row, b):
        def one(p, _):
            cur1[b, p] = full_value(0, row, b, p)
            return 0

        lax.fori_loop(row * GY, row * GY + GY, one, 0, unroll=8)

    def z_copy(b, j):
        return remote(
            fil.at[b, pl.ds((1 - zh) * GY + j * CH, CH)], xg.at[b, zh, pl.ds(j * CH, CH)],
            zsend.at[b], zrecv.at[b, j], {"zh": 1 - zh},
        )

    def x_copy(way, b, j, kind):
        part = pl.ds(j * CH, CH)
        h = (zh, 1 - zh)[kind]
        src = fil.at[b, pl.ds(zh * GY + j * CH, CH)] if kind == 0 else xg.at[b, h, part]
        return remote(
            src, (x1, x2)[way].at[b, h, part], xsend.at[way, b], xrecv.at[way, b, j, kind], (xp, xm)[way]
        )

    def pass_on(b, j, kind):
        part, way, h = pl.ds(j * CH, CH), j // 2, (zh, 1 - zh)[kind]
        return remote(
            (x1, x2)[way].at[b, h, part], x3.at[b, h, part], gsend.at[b], grecv.at[b, j, kind], (xp, xm)[way]
        )

    def bytes_of(ref, sem):
        return pltpu.make_async_copy(ref, ref, sem)

    def z_to_x(b):
        for j in ORDER:
            with jax.named_scope(f'wz{b}{j}'):
                z_copy(b, j).wait_recv()
            x_copy(0, b, j, 1).start()
            x_copy(1, b, j, 1).start()

    def second(b):
        for j in ORDER:
            for row in (1, 0):
                for m in range(CH):
                    p = row * GY + j * CH + m
                    fil[b, p] = full_value(1, row, b, p)
            if b == 0:

                @pl.when(jnp.logical_not(held))
                def _():
                    z_copy(b, j).start()

            else:
                z_copy(b, j).start()
            x_copy(0, b, j, 0).start()
            x_copy(1, b, j, 0).start()
        xg[b, zh] = fil[b, pl.ds(zh * GY, GY)]

    def pass_half(b, kind):
        for j in ORDER:
            with jax.named_scope(f'wx{b}{kind}{j}'):
                x_copy(j // 2, b, j, kind).wait_recv()
            pass_on(b, j, kind).start()

    for b in (0, 1):
        with jax.named_scope(f'local0{b}'):
            local_part(0, 1, b)
            local_part(0, 0, b)
    for b in (0, 1):
        with jax.named_scope(f'w_h0{b}1'):
            halo_copy(0, 1, b).wait_recv()
        first(1, b)
        halo_copy(1, 0, b).start()
        with jax.named_scope(f'w_h0{b}0'):
            halo_copy(0, 0, b).wait_recv()
        first(0, b)
        halo_copy(1, 1, b).start()
        with jax.named_scope(f'local1{b}'):
            local_part(1, 1, b)
            local_part(1, 0, b)
    def finish(b):
        with jax.named_scope(f'w_h1{b}'):
            halo_copy(1, 1, b).wait_recv()
            halo_copy(1, 0, b).wait_recv()
        if b == 1:

            @pl.when(jnp.logical_and(crossing, held))
            def _():
                pl.semaphore_signal(gate, inc=1, device_id={"c": 1 - c}, device_id_type=MESH_ID)

            @pl.when(jnp.logical_and(held, jnp.logical_not(crossing)))
            def _():
                with jax.named_scope('w_gate'):
                    pl.semaphore_wait(gate, 1)

            @pl.when(held)
            def _():
                for j in ORDER:
                    z_copy(0, j).start()

        with jax.named_scope(f'second{b}'):
            second(b)

    finish(0)

    finish(1)
    z_to_x(0)
    pass_half(0, 0)
    pass_half(1, 0)
    z_to_x(1)

    def put(i, _):
        s = slot[i]
        outv[i] = jnp.concatenate([fil[0, s], fil[1, s]], axis=1)
        return 0

    with jax.named_scope('put'):
        lax.fori_loop(0, EL, put, 0, unroll=4)
    store_f = pltpu.make_async_copy(outv, out_f, lsem.at[7])
    store_f.start()

    def bound_for(x_a, b):
        return (x_a % 2) * 2 + b

    def c_copy(x_a, b):
        at = (pl.ds(0, 2), x_a // 2, bound_for(x_a, b))
        return remote(pb.at[(1 - c, *at)], rc.at[at], csend, crecv.at[x_a, b], {"c": 1 - c})

    def product(x_a, b, ref):
        left = jnp.concatenate([ref[b, h].reshape(GY * BMAX, HB) for h in (0, 1)], axis=1)
        for zh_b in (0, 1):
            right = jnp.concatenate([xg[k, zh_b].reshape(GY * BMAX, HB) for k in (0, 1)], axis=1)
            tile = lax.dot_general(left, right, (((0,), (0,)), ((), ())), preferred_element_type=F32).astype(BF)
            for zh_a in (0, 1):
                for core in (0, 1):
                    at = zh_a * HB + core * 64
                    pb[core, zh_a, x_a // 2, bound_for(x_a, b), zh_b] = tile[at : at + 64]
        c_copy(x_a, b).start()

    def y_copy(to, d, xh):
        return remote(
            s1.at[:, xh, to], ry.at[d - 1, xh], ysend, yrecv.at[d - 1, xh], {"y": to}
        )

    def settle(x_a, b):
        xh, to = x_a // 2, bound_for(x_a, b)
        with jax.named_scope(f'wc{b}'):
            c_copy(x_a, b).wait_recv()
        for zh_a in (0, 1):
            s1[zh_a, xh, to] = (pb[c, zh_a, xh, to].astype(F32) + rc[zh_a, xh, to].astype(F32)).astype(BF)

        @pl.when(to != y)
        def _():
            y_copy(to, (to + 4 - y) % 4, xh).start()

    def r_copy(to, src_xh):
        d = (to + 8 - z) % 8
        return remote(
            s2.at[src_xh, (to % 4) // 2, to // 4], rz.at[d - 1], rsend, rrecv, z_id(to)
        )

    def gather_y(xh):
        for d in (1, 3, 2):
            y_copy((y + d) % 4, d, xh).wait_recv()
        for zh_a in (0, 1):
            total = s1[zh_a, xh, y].astype(F32)
            for d in range(3):
                total = total + ry[d, xh, zh_a].astype(F32)
            s2[xh, zh_a] = total.astype(BF)
        for zh_a in (0, 1):
            for zh_b in (0, 1):
                to = zh_b * 4 + zh_a * 2 + xh

                @pl.when(to != z)
                def _():
                    r_copy(to, xh).start()

    def beside(b):
        for way in (0, 1):
            with jax.named_scope(f'w_x{way}'):
                for j in ((2, 3), (0, 1))[way]:
                    for kind in (0, 1):
                        x_copy(way, b, j, kind).wait_recv()
            product((x_prev, x_next)[way], b, (x1, x2)[way])

    def far_unit(b):
        with jax.named_scope(f'w_far{b}'):
            for j in ORDER:
                for kind in (0, 1):
                    pass_on(b, j, kind).wait_recv()
        product(x_far, b, x3)
        settle(x_far, b)

    same = y // 2 == x % 2
    pass_half(0, 1)
    with jax.named_scope('prod_e'):
        product(x, 0, xg)
        product(x, 1, xg)
        beside(0)
    with jax.named_scope('settle_e'):
        settle(x, 0)
        settle(x, 1)
        settle(x_prev, 0)
        settle(x_next, 0)
    pass_half(1, 1)
    with jax.named_scope('prod_l'):
        beside(1)
    with jax.named_scope('settle_l'):
        settle(x_prev, 1)
        settle(x_next, 1)
    far_unit(0)
    far_unit(1)

    with jax.named_scope('gather_y1'):
        @pl.when(same)
        def _():
            gather_y(x // 2)

        @pl.when(jnp.logical_not(same))
        def _():
            gather_y(0)
            gather_y(1)

    with jax.named_scope('gather_y2'):
        @pl.when(same)
        def _():
            gather_y(1 - x // 2)

    total = s2[zl % 2, zl // 2, zh].astype(F32)
    with jax.named_scope('wr'):
        bytes_of(rz, rrecv).wait()
    for d in range(7):
        total = total + rz[d].astype(F32)
    mv[...] = total * (1.0 / 65536.0)
    store_m = pltpu.make_async_copy(mv, out_m, lsem.at[8])
    store_m.start()

    with jax.named_scope('tail'):
        for degree in (0, 1):
            for row in (0, 1):
                for b in (0, 1):
                    halo_copy(degree, row, b).wait_send()
        for b in (0, 1):
            for k in (0, 1):
                bytes_of(xg.at[b], xsend.at[k, b]).wait()
            bytes_of(x3.at[b], gsend.at[b]).wait()
            bytes_of(fil.at[b, pl.ds(0, GY)], zsend.at[b]).wait()
        bytes_of(rc, csend).wait()
        bytes_of(ry, ysend).wait()
        bytes_of(rz, rsend).wait()
        store_f.wait()
        store_m.wait()


def on_device(y_current, y_previous, h_blocks, basis_sizes, neighbours):
    any_space = pl.BlockSpec(memory_space=pl.ANY)
    dma = pltpu.SemaphoreType.DMA
    halves = pltpu.VMEM((2, EL, BMAX, HB), BF)
    met = pltpu.VMEM((2, 2, GY, BMAX, HB), BF)
    return pl.pallas_call(
        main_kernel,
        out_shape=(
            jax.ShapeDtypeStruct((EL, BMAX, BD), BF),
            jax.ShapeDtypeStruct((64, BD), F32),
        ),
        in_specs=[any_space] * 5,
        out_specs=(any_space, any_space),
        scratch_shapes=[
            pltpu.SMEM((4, EL), jnp.int32),
            pltpu.SMEM((EL,), jnp.int32),
            pltpu.SMEM((EL, 8), jnp.int32),
            pltpu.SMEM((EL,), jnp.int32),
            pltpu.SMEM((EL,), jnp.int32),
            pltpu.SMEM((EL,), jnp.int32),
            halves,
            halves,
            pltpu.VMEM((EL, BMAX, 5 * BMAX), BF),
            halves,
            halves,
            *[pltpu.VMEM((GY, BMAX, HB), BF)] * 8,
            pltpu.VMEM((2, EL, BMAX, HB), F32),
            halves,
            pltpu.VMEM((EL, BMAX, BD), BF),
            met,
            met,
            met,
            met,
            pltpu.VMEM((2, 2, 2, 4, 2, 64, BD), BF),
            pltpu.VMEM((2, 2, 4, 2, 64, BD), BF),
            pltpu.VMEM((2, 2, 4, 2, 64, BD), BF),
            pltpu.VMEM((3, 2, 2, 2, 64, BD), BF),
            pltpu.VMEM((2, 2, 2, 64, BD), BF),
            pltpu.VMEM((7, 64, BD), BF),
            pltpu.VMEM((64, BD), F32),
            dma((9,)),
            dma((2, 2, 2)), dma((2, 2, 2)),
            dma((2,)), dma((2, NCH)),
            dma((2, 2)), dma((2, 2, NCH, 2)),
            dma((2,)), dma((2, NCH, 2)),
            dma, dma((4, 2)),
            dma, dma((3, 2)),
            dma, dma,
            pltpu.SemaphoreType.REGULAR,
        ],
        compiler_params=pltpu.CompilerParams(collective_id=0, has_side_effects=True),
        name="chain",
    )(neighbours.T, basis_sizes, y_current, y_previous, h_blocks)


def solution(mesh):
    split = Mesh(mesh.devices.reshape(4, 4, 2, 2, 4), ELEM + BAND)
    return jax.shard_map(
        on_device,
        mesh=split,
        in_specs=(
            P(ELEM, None, BAND),
            P(ELEM, None, BAND),
            P(ELEM, None, None),
            P(ELEM),
            P(ELEM, None),
        ),
        out_specs=(P(ELEM, None, BAND), P(ELEM, BAND)),
        check_vma=False,
    )
```

```python
import jax
import jax.numpy as jnp
from jax import lax
from jax.experimental import pallas as pl
from jax.experimental.pallas import tpu as pltpu
from jax.sharding import Mesh
from jax.sharding import PartitionSpec as P

BMAX = 64
EL = 32
GY = 16
BD = 256
NB = 2048
ROWS = GY * BMAX
HB = 128
CH = 4
NCH = GY // CH
ORDER = (0, 2, 1, 3)

CENTER = 0.3
SCALE = 2.0 / 1.7

ELEM = ("zl", "y", "c")
BAND = ("zh", "x")
BF = jnp.bfloat16
F32 = jnp.float32
MESH_ID = pl.DeviceIdType.MESH


def ones_of(word):
    word = word - (lax.shift_right_logical(word, 1) & 0x55555555)
    word = (word & 0x33333333) + (lax.shift_right_logical(word, 2) & 0x33333333)
    word = (word + lax.shift_right_logical(word, 4)) & 0x0F0F0F0F
    return lax.shift_right_logical(word * 0x01010101, 24)


def make_tables(me, nb, sizes, tbl, slot, link, power):
    for i in range(EL):
        power[i] = jnp.int32(1 << i if i < 31 else -(1 << 31))
    ones, rows = jnp.int32(0), []
    wanted = [jnp.int32(0), jnp.int32(0)]
    for i in range(EL):
        row = jnp.where(nb[0, i] >> 5 == me, 1, 0)
        rows.append(row)
        slot[i] = jnp.where(row == 1, GY + ones, i - ones) & (EL - 1)
        ones = ones + row
        for k in (0, 1):
            wanted[k] = wanted[k] + jnp.where(row == k, power[nb[k, i] & (EL - 1)], 0)
    first = [jnp.int32(0), jnp.int32(0)]
    for i in reversed(range(EL)):
        link[i] = jnp.where(rows[i] == 1, first[1], first[0])
        first = [jnp.where(rows[i] == k, i, first[k]) for k in (0, 1)]
    for row in (0, 1):
        i = first[row]
        for p in range(row * GY, row * GY + GY):
            tbl[p, 0] = i
            tbl[p, 1] = sizes[i]
            tbl[p, 2] = slot[nb[1 - row, i] & (EL - 1)]
            tbl[p, 3] = slot[nb[2, i] & (EL - 1)]
            tbl[p, 4] = slot[nb[3, i] & (EL - 1)]
            tbl[p, 5] = ones_of(wanted[row] & (power[nb[row, i] & (EL - 1)] - 1)) & (GY - 1)
            i = link[i]


def main_kernel(
    nb_h, size_h, yc_h, yp_h, h_h, out_f, out_m, nb, sizes, tbl, slot, link, power,
    yc, yp, hv, cur0, cur1, f000, f001, f010, f011, f100, f101, f110, f111,
    acc, fil, outv, xg, x1, x2, x3, pb, rc, s1, ry, s2, rz, mv,
    lsem, hsend, hrecv, zsend, zrecv, xsend, xrecv, gsend, grecv, csend, crecv, ysend, yrecv, rsend, rrecv,
):
    zl, y, c = (lax.axis_index(a) for a in ELEM)
    zh, x = (lax.axis_index(a) for a in BAND)
    z = zh * 4 + zl
    e = (zl * 4 + y) * 2 + c
    outer = jnp.logical_or(y == 0, y == 3)
    crossing = jnp.logical_or(jnp.logical_and(y == 0, c == 0), jnp.logical_and(y == 3, c == 1))
    last = jnp.logical_or(jnp.logical_and(y == 0, zl == 0), jnp.logical_and(y == 3, zl == 3))
    held = jnp.logical_and(outer, jnp.logical_not(last))

    def elem_id(other):
        return {"zl": other // 8, "y": (other // 2) % 4, "c": other % 2}

    def z_id(other):
        return {"zh": other // 4, "zl": other % 4}

    nxt, prv = elem_id((e + 1) % 32), elem_id((e + 31) % 32)
    x_prev, x_next, x_far = (x + 3) % 4, (x + 1) % 4, (x + 2) % 4
    xp, xm = {"x": x_next}, {"x": x_prev}

    def remote(src, dst, ss, rs, to):
        return pltpu.make_async_remote_copy(
            src_ref=src, dst_ref=dst, send_sem=ss, recv_sem=rs, device_id=to, device_id_type=MESH_ID
        )

    loads = [
        pltpu.make_async_copy(src, dst, lsem.at[k])
        for k, (src, dst) in enumerate(
            [(nb_h, nb), (size_h, sizes)]
            + [(yc_h.at[:, :, pl.ds(b * HB, HB)], yc.at[b]) for b in (0, 1)]
            + [(h_h, hv)]
            + [(yp_h.at[:, :, pl.ds(b * HB, HB)], yp.at[b]) for b in (0, 1)]
        )
    ]
    for load in loads:
        load.start()

    barrier = pltpu.get_barrier_semaphore()
    partners = [nxt, prv, xp, xm]
    partners += [{"y": (y + d) % 4} for d in (1, 2, 3)]
    partners += [z_id((z + d) % 8) for d in range(1, 8)]
    for to in partners:
        pl.semaphore_signal(barrier, inc=1, device_id=to, device_id_type=MESH_ID)

    rows = lax.broadcasted_iota(jnp.int32, (BMAX, HB), 0)
    zero = jnp.zeros((BMAX, HB), BF)

    with jax.named_scope('w_load'):
        for load in loads[:2]:
            load.wait()
    with jax.named_scope('tables'):
        make_tables(e, nb, sizes, tbl, slot, link, power)
    for load in loads[2:4]:
        load.wait()

    def pack(row, b):
        def one(p, _):
            value = yc[b, tbl[p, 0]].astype(F32)
            cur0[b, p] = jnp.where(rows < tbl[p, 1], value, 0.0).astype(BF)
            return 0

        lax.fori_loop(row * GY, row * GY + GY, one, 0, unroll=4)

    halo = (((f000, f001), (f010, f011)), ((f100, f101), (f110, f111)))

    def halo_copy(degree, row, b):
        return remote(
            (cur0, cur1)[degree].at[b, pl.ds((1 - row) * GY, GY)], halo[degree][row][b],
            hsend.at[degree, row, b], hrecv.at[degree, row, b], (nxt, prv)[row],
        )

    with jax.named_scope('pack'):
        pack(1, 0)
    with jax.named_scope('barrier'):
        pl.semaphore_wait(barrier, len(partners))
    halo_copy(0, 0, 0).start()
    pack(0, 0)
    halo_copy(0, 1, 0).start()
    pack(1, 1)
    halo_copy(0, 0, 1).start()
    pack(0, 1)
    halo_copy(0, 1, 1).start()
    for load in loads[4:]:
        load.wait()

    def local_part(degree, row, b):
        cur = (cur0, cur1)[degree]

        def one(p, _):
            i = tbl[p, 0]
            own, n2, n3, n4 = cur[b, p], cur[b, tbl[p, 2]], cur[b, tbl[p, 3]], cur[b, tbl[p, 4]]
            pair = [zero, n2] if row == 0 else [n2, zero]
            stack = jnp.concatenate([own] + pair + [n3, n4], axis=0)
            applied = jnp.dot(hv[i], stack, preferred_element_type=F32)
            before = yp[b, i] if degree == 0 else cur0[b, p]
            acc[b, p] = SCALE * (applied - CENTER * own.astype(F32)) - before.astype(F32)
            return 0

        lax.fori_loop(row * GY, row * GY + GY, one, 0, unroll=8)

    def full_value(degree, row, b, p):
        i = tbl[p, 0]
        far = halo[degree][row][b][tbl[p, 5]]
        if row == 0:
            applied = jnp.dot(hv[i, :, 0:128], jnp.concatenate([zero, far], axis=0), preferred_element_type=F32)
        else:
            applied = jnp.dot(hv[i, :, 128:256], jnp.concatenate([far, zero], axis=0), preferred_element_type=F32)
        return jnp.where(rows < tbl[p, 1], acc[b, p] + SCALE * applied, 0.0).astype(BF)

    def first(row, b):
        def one(p, _):
            cur1[b, p] = full_value(0, row, b, p)
            return 0

        lax.fori_loop(row * GY, row * GY + GY, one, 0, unroll=8)

    def z_copy(b, j):
        return remote(
            fil.at[b, pl.ds((1 - zh) * GY + j * CH, CH)], xg.at[b, zh, pl.ds(j * CH, CH)],
            zsend.at[b], zrecv.at[b, j], {"zh": 1 - zh},
        )

    def x_copy(way, b, j, kind):
        part = pl.ds(j * CH, CH)
        h = (zh, 1 - zh)[kind]
        src = fil.at[b, pl.ds(zh * GY + j * CH, CH)] if kind == 0 else xg.at[b, h, part]
        return remote(
            src, (x1, x2)[way].at[b, h, part], xsend.at[way, b], xrecv.at[way, b, j, kind], (xp, xm)[way]
        )

    def pass_on(b, j, kind):
        part, way, h = pl.ds(j * CH, CH), j // 2, (zh, 1 - zh)[kind]
        return remote(
            (x1, x2)[way].at[b, h, part], x3.at[b, h, part], gsend.at[b], grecv.at[b, j, kind], (xp, xm)[way]
        )

    def bytes_of(ref, sem):
        return pltpu.make_async_copy(ref, ref, sem)

    def z_to_x(b):
        for j in ORDER:
            with jax.named_scope(f'wz{b}{j}'):
                z_copy(b, j).wait_recv()
            x_copy(0, b, j, 1).start()
            x_copy(1, b, j, 1).start()

    def second(b):
        for j in ORDER:
            for row in (1, 0):
                for m in range(CH):
                    p = row * GY + j * CH + m
                    fil[b, p] = full_value(1, row, b, p)
            if b == 0:

                @pl.when(jnp.logical_not(held))
                def _():
                    z_copy(b, j).start()

            else:
                z_copy(b, j).start()
            x_copy(0, b, j, 0).start()
            x_copy(1, b, j, 0).start()
        xg[b, zh] = fil[b, pl.ds(zh * GY, GY)]

    def pass_half(b, kind):
        for j in ORDER:
            with jax.named_scope(f'wx{b}{kind}{j}'):
                x_copy(j // 2, b, j, kind).wait_recv()
            pass_on(b, j, kind).start()

    for b in (0, 1):
        with jax.named_scope(f'local0{b}'):
            local_part(0, 1, b)
            local_part(0, 0, b)
    for b in (0, 1):
        with jax.named_scope(f'w_h0{b}1'):
            halo_copy(0, 1, b).wait_recv()
        first(1, b)
        halo_copy(1, 0, b).start()
        with jax.named_scope(f'w_h0{b}0'):
            halo_copy(0, 0, b).wait_recv()
        first(0, b)
        halo_copy(1, 1, b).start()
        with jax.named_scope(f'local1{b}'):
            local_part(1, 1, b)
            local_part(1, 0, b)
    def finish(b):
        with jax.named_scope(f'w_h1{b}'):
            halo_copy(1, 1, b).wait_recv()
            halo_copy(1, 0, b).wait_recv()
        if b == 1:

            @pl.when(held)
            def _():
                for j in ORDER:
                    z_copy(0, j).start()

        with jax.named_scope(f'second{b}'):
            second(b)

    finish(0)

    finish(1)
    z_to_x(0)
    pass_half(0, 0)
    pass_half(1, 0)
    z_to_x(1)

    def put(i, _):
        s = slot[i]
        outv[i] = jnp.concatenate([fil[0, s], fil[1, s]], axis=1)
        return 0

    with jax.named_scope('put'):
        lax.fori_loop(0, EL, put, 0, unroll=4)
    store_f = pltpu.make_async_copy(outv, out_f, lsem.at[7])
    store_f.start()

    def bound_for(x_a, b):
        return (x_a % 2) * 2 + b

    def c_copy(x_a, b, kind):
        at = ((zh, 1 - zh)[kind], x_a // 2, bound_for(x_a, b))
        return remote(pb.at[(1 - c, *at)], rc.at[at], csend, crecv.at[x_a, b, kind], {"c": 1 - c})

    def product(x_a, b, kind, ref):
        zh_a = (zh, 1 - zh)[kind]
        left = ref[b, zh_a].reshape(GY * BMAX, HB)
        for zh_b in (0, 1):
            right = jnp.concatenate([xg[k, zh_b].reshape(GY * BMAX, HB) for k in (0, 1)], axis=1)
            tile = lax.dot_general(left, right, (((0,), (0,)), ((), ())), preferred_element_type=F32).astype(BF)
            for core in (0, 1):
                pb[core, zh_a, x_a // 2, bound_for(x_a, b), zh_b] = tile[core * 64 : core * 64 + 64]
        c_copy(x_a, b, kind).start()

    def y_copy(to, d, xh, kind):
        zh_a = (zh, 1 - zh)[kind]
        return remote(
            s1.at[zh_a, xh, to], ry.at[d - 1, xh, zh_a], ysend, yrecv.at[d - 1, xh, kind], {"y": to}
        )

    def settle(x_a, b, kind):
        zh_a, xh, to = (zh, 1 - zh)[kind], x_a // 2, bound_for(x_a, b)
        c_copy(x_a, b, kind).wait_recv()
        s1[zh_a, xh, to] = (pb[c, zh_a, xh, to].astype(F32) + rc[zh_a, xh, to].astype(F32)).astype(BF)

        @pl.when(to != y)
        def _():
            y_copy(to, (to + 4 - y) % 4, xh, kind).start()

    def r_copy(to, src_xh):
        d = (to + 8 - z) % 8
        return remote(
            s2.at[src_xh, (to % 4) // 2, to // 4], rz.at[d - 1], rsend, rrecv, z_id(to)
        )

    def gather_y(xh):
        for d in (1, 3, 2):
            for kind in (0, 1):
                y_copy((y + d) % 4, d, xh, kind).wait_recv()
        for zh_a in (0, 1):
            total = s1[zh_a, xh, y].astype(F32)
            for d in range(3):
                total = total + ry[d, xh, zh_a].astype(F32)
            s2[xh, zh_a] = total.astype(BF)
        for zh_a in (0, 1):
            for zh_b in (0, 1):
                to = zh_b * 4 + zh_a * 2 + xh

                @pl.when(to != z)
                def _():
                    r_copy(to, xh).start()

    def wait_beside(b, kind):
        for way in (0, 1):
            for j in ((2, 3), (0, 1))[way]:
                x_copy(way, b, j, kind).wait_recv()

    def wait_far(b, kind):
        for j in ORDER:
            pass_on(b, j, kind).wait_recv()

    def all_of(units):
        for unit, ref in units:
            product(*unit, ref)
        return [unit for unit, _ in units]

    def settle_all(units):
        for unit in units:
            settle(*unit)

    def beside(b, kind):
        return [((x_prev, b, kind), x1), ((x_next, b, kind), x2)]

    same = y // 2 == x % 2
    pass_half(0, 1)
    with jax.named_scope('prod_e'):
        for b in (0, 1):
            wait_beside(b, 0)
        early = all_of([((x, b, kind), xg) for b in (0, 1) for kind in (0, 1)] + beside(0, 0) + beside(1, 0))
    with jax.named_scope('settle_e'):
        settle_all(early)
    with jax.named_scope('w_x0'):
        wait_beside(0, 1)
    with jax.named_scope('prod_m'):
        middle = all_of(beside(0, 1))
    pass_half(1, 1)
    with jax.named_scope('w_far_0'):
        wait_far(0, 0)
        wait_far(1, 0)
    with jax.named_scope('prod_f0'):
        middle += all_of([((x_far, 0, 0), x3), ((x_far, 1, 0), x3)])
    with jax.named_scope('settle_m'):
        settle_all(middle)
    with jax.named_scope('w_x1'):
        wait_beside(1, 1)
    with jax.named_scope('prod_l'):
        late = all_of(beside(1, 1))
        settle_all(late)
    with jax.named_scope('w_far0'):
        wait_far(0, 1)
    settle_all(all_of([((x_far, 0, 1), x3)]))
    with jax.named_scope('w_far1'):
        wait_far(1, 1)
    settle_all(all_of([((x_far, 1, 1), x3)]))

    with jax.named_scope('gather_y1'):
        @pl.when(same)
        def _():
            gather_y(x // 2)

        @pl.when(jnp.logical_not(same))
        def _():
            gather_y(0)
            gather_y(1)

    with jax.named_scope('gather_y2'):
        @pl.when(same)
        def _():
            gather_y(1 - x // 2)

    total = s2[zl % 2, zl // 2, zh].astype(F32)
    with jax.named_scope('wr'):
        bytes_of(rz, rrecv).wait()
    for d in range(7):
        total = total + rz[d].astype(F32)
    mv[...] = total * (1.0 / 65536.0)
    store_m = pltpu.make_async_copy(mv, out_m, lsem.at[8])
    store_m.start()

    with jax.named_scope('tail'):
        for degree in (0, 1):
            for row in (0, 1):
                for b in (0, 1):
                    halo_copy(degree, row, b).wait_send()
        for b in (0, 1):
            for k in (0, 1):
                bytes_of(xg.at[b], xsend.at[k, b]).wait()
            bytes_of(x3.at[b], gsend.at[b]).wait()
            bytes_of(fil.at[b, pl.ds(0, GY)], zsend.at[b]).wait()
        bytes_of(rc, csend).wait()
        bytes_of(ry, ysend).wait()
        bytes_of(rz, rsend).wait()
        store_f.wait()
        store_m.wait()


PARTS = 4


def put_out_kernel(f_h, m_h, f_out, m_out, f_v, m_v, came, gone):
    pairs = [(m_h, m_v, m_out)]
    for k in range(PARTS):
        part = pl.ds(k * EL // PARTS, EL // PARTS)
        pairs.append((f_h.at[part], f_v.at[part], f_out.at[part]))
    into = [pltpu.make_async_copy(a, b, came.at[k]) for k, (a, b, _) in enumerate(pairs)]
    out = [pltpu.make_async_copy(b, a, gone.at[k]) for k, (_, b, a) in enumerate(pairs)]
    for copy in into:
        copy.start()
    for first, then in zip(into, out):
        first.wait()
        then.start()
    for copy in out:
        copy.wait()


def on_device(y_current, y_previous, h_blocks, basis_sizes, neighbours):
    any_space = pl.BlockSpec(memory_space=pl.ANY)
    dma = pltpu.SemaphoreType.DMA
    halves = pltpu.VMEM((2, EL, BMAX, HB), BF)
    met = pltpu.VMEM((2, 2, GY, BMAX, HB), BF)
    filtered, margin = pl.pallas_call(
        main_kernel,
        out_shape=(
            jax.ShapeDtypeStruct((EL, BMAX, BD), BF),
            jax.ShapeDtypeStruct((64, BD), F32),
        ),
        in_specs=[any_space] * 5,
        out_specs=(any_space, any_space),
        scratch_shapes=[
            pltpu.SMEM((4, EL), jnp.int32),
            pltpu.SMEM((EL,), jnp.int32),
            pltpu.SMEM((EL, 8), jnp.int32),
            pltpu.SMEM((EL,), jnp.int32),
            pltpu.SMEM((EL,), jnp.int32),
            pltpu.SMEM((EL,), jnp.int32),
            halves,
            halves,
            pltpu.VMEM((EL, BMAX, 5 * BMAX), BF),
            halves,
            halves,
            *[pltpu.VMEM((GY, BMAX, HB), BF)] * 8,
            pltpu.VMEM((2, EL, BMAX, HB), F32),
            halves,
            pltpu.VMEM((EL, BMAX, BD), BF),
            met,
            met,
            met,
            met,
            pltpu.VMEM((2, 2, 2, 4, 2, 64, BD), BF),
            pltpu.VMEM((2, 2, 4, 2, 64, BD), BF),
            pltpu.VMEM((2, 2, 4, 2, 64, BD), BF),
            pltpu.VMEM((3, 2, 2, 2, 64, BD), BF),
            pltpu.VMEM((2, 2, 2, 64, BD), BF),
            pltpu.VMEM((7, 64, BD), BF),
            pltpu.VMEM((64, BD), F32),
            dma((9,)),
            dma((2, 2, 2)), dma((2, 2, 2)),
            dma((2,)), dma((2, NCH)),
            dma((2, 2)), dma((2, 2, NCH, 2)),
            dma((2,)), dma((2, NCH, 2)),
            dma, dma((4, 2, 2)),
            dma, dma((3, 2, 2)),
            dma, dma,
        ],
        compiler_params=pltpu.CompilerParams(collective_id=0, has_side_effects=True),
        name="chain",
    )(neighbours.T, basis_sizes, y_current, y_previous, h_blocks)
    return pl.pallas_call(
        put_out_kernel,
        out_shape=(
            jax.ShapeDtypeStruct((EL, BMAX, BD), BF),
            jax.ShapeDtypeStruct((64, BD), F32),
        ),
        in_specs=[any_space] * 2,
        out_specs=(any_space, any_space),
        scratch_shapes=[
            pltpu.VMEM((EL, BMAX, BD), BF),
            pltpu.VMEM((64, BD), F32),
            dma((PARTS + 1,)), dma((PARTS + 1,)),
        ],
        name="put_out",
    )(filtered, margin)


def solution(mesh):
    split = Mesh(mesh.devices.reshape(4, 4, 2, 2, 4), ELEM + BAND)
    return jax.shard_map(
        on_device,
        mesh=split,
        in_specs=(
            P(ELEM, None, BAND),
            P(ELEM, None, BAND),
            P(ELEM, None, None),
            P(ELEM),
            P(ELEM, None),
        ),
        out_specs=(P(ELEM, None, BAND), P(ELEM, BAND)),
        check_vma=False,
    )
```

```python
import jax
import jax.numpy as jnp
from jax import lax
from jax.experimental import pallas as pl
from jax.experimental.pallas import tpu as pltpu
from jax.sharding import Mesh
from jax.sharding import PartitionSpec as P

BMAX = 64
EL = 32
GY = 16
BD = 256
NB = 2048
ROWS = GY * BMAX
HB = 128
CH = 4
NCH = GY // CH
ORDER = (0, 2, 1, 3)

CENTER = 0.3
SCALE = 2.0 / 1.7

ELEM = ("zl", "y", "c")
BAND = ("zh", "x")
BF = jnp.bfloat16
F32 = jnp.float32
MESH_ID = pl.DeviceIdType.MESH


def ones_of(word):
    word = word - (lax.shift_right_logical(word, 1) & 0x55555555)
    word = (word & 0x33333333) + (lax.shift_right_logical(word, 2) & 0x33333333)
    word = (word + lax.shift_right_logical(word, 4)) & 0x0F0F0F0F
    return lax.shift_right_logical(word * 0x01010101, 24)


def make_tables(me, nb, sizes, tbl, slot, link, power):
    for i in range(EL):
        power[i] = jnp.int32(1 << i if i < 31 else -(1 << 31))
    ones, rows = jnp.int32(0), []
    wanted = [jnp.int32(0), jnp.int32(0)]
    for i in range(EL):
        row = jnp.where(nb[0, i] >> 5 == me, 1, 0)
        rows.append(row)
        slot[i] = jnp.where(row == 1, GY + ones, i - ones) & (EL - 1)
        ones = ones + row
        for k in (0, 1):
            wanted[k] = wanted[k] + jnp.where(row == k, power[nb[k, i] & (EL - 1)], 0)
    first = [jnp.int32(0), jnp.int32(0)]
    for i in reversed(range(EL)):
        link[i] = jnp.where(rows[i] == 1, first[1], first[0])
        first = [jnp.where(rows[i] == k, i, first[k]) for k in (0, 1)]
    for row in (0, 1):
        i = first[row]
        for p in range(row * GY, row * GY + GY):
            tbl[p, 0] = i
            tbl[p, 1] = sizes[i]
            tbl[p, 2] = slot[nb[1 - row, i] & (EL - 1)]
            tbl[p, 3] = slot[nb[2, i] & (EL - 1)]
            tbl[p, 4] = slot[nb[3, i] & (EL - 1)]
            tbl[p, 5] = ones_of(wanted[row] & (power[nb[row, i] & (EL - 1)] - 1)) & (GY - 1)
            i = link[i]


def main_kernel(
    nb_h, size_h, yc_h, yp_h, h_h, out_f, out_m, nb, sizes, tbl, slot, link, power,
    yc, yp, hv, cur0, cur1, f000, f001, f010, f011, f100, f101, f110, f111,
    acc, fil, outv, xg, x1, x2, x3, pb, rc, s1, ry, s2, rz, mv,
    lsem, hsend, hrecv, zsend, zrecv, xsend, xrecv, gsend, grecv, csend, crecv, ysend, yrecv, rsend, rrecv,
):
    zl, y, c = (lax.axis_index(a) for a in ELEM)
    zh, x = (lax.axis_index(a) for a in BAND)
    z = zh * 4 + zl
    e = (zl * 4 + y) * 2 + c
    outer = jnp.logical_or(y == 0, y == 3)
    crossing = jnp.logical_or(jnp.logical_and(y == 0, c == 0), jnp.logical_and(y == 3, c == 1))
    last = jnp.logical_or(jnp.logical_and(y == 0, zl == 0), jnp.logical_and(y == 3, zl == 3))
    at_once = jnp.where(last, 4, jnp.where(outer, 1, NCH))

    def elem_id(other):
        return {"zl": other // 8, "y": (other // 2) % 4, "c": other % 2}

    def z_id(other):
        return {"zh": other // 4, "zl": other % 4}

    nxt, prv = elem_id((e + 1) % 32), elem_id((e + 31) % 32)
    x_prev, x_next, x_far = (x + 3) % 4, (x + 1) % 4, (x + 2) % 4
    xp, xm = {"x": x_next}, {"x": x_prev}

    def remote(src, dst, ss, rs, to):
        return pltpu.make_async_remote_copy(
            src_ref=src, dst_ref=dst, send_sem=ss, recv_sem=rs, device_id=to, device_id_type=MESH_ID
        )

    loads = [
        pltpu.make_async_copy(src, dst, lsem.at[k])
        for k, (src, dst) in enumerate(
            [(nb_h, nb), (size_h, sizes)]
            + [(yc_h.at[:, :, pl.ds(b * HB, HB)], yc.at[b]) for b in (0, 1)]
            + [(h_h, hv)]
            + [(yp_h.at[:, :, pl.ds(b * HB, HB)], yp.at[b]) for b in (0, 1)]
        )
    ]
    for load in loads:
        load.start()

    barrier = pltpu.get_barrier_semaphore()
    partners = [nxt, prv, xp, xm]
    partners += [{"y": (y + d) % 4} for d in (1, 2, 3)]
    partners += [z_id((z + d) % 8) for d in range(1, 8)]
    for to in partners:
        pl.semaphore_signal(barrier, inc=1, device_id=to, device_id_type=MESH_ID)

    rows = lax.broadcasted_iota(jnp.int32, (BMAX, HB), 0)
    zero = jnp.zeros((BMAX, HB), BF)

    with jax.named_scope('w_load'):
        for load in loads[:2]:
            load.wait()
    with jax.named_scope('tables'):
        make_tables(e, nb, sizes, tbl, slot, link, power)
    for load in loads[2:4]:
        load.wait()

    def pack(row, b):
        def one(p, _):
            value = yc[b, tbl[p, 0]].astype(F32)
            cur0[b, p] = jnp.where(rows < tbl[p, 1], value, 0.0).astype(BF)
            return 0

        lax.fori_loop(row * GY, row * GY + GY, one, 0, unroll=4)

    halo = (((f000, f001), (f010, f011)), ((f100, f101), (f110, f111)))

    def halo_copy(degree, row, b):
        return remote(
            (cur0, cur1)[degree].at[b, pl.ds((1 - row) * GY, GY)], halo[degree][row][b],
            hsend.at[degree, row, b], hrecv.at[degree, row, b], (nxt, prv)[row],
        )

    with jax.named_scope('pack'):
        pack(1, 0)
    with jax.named_scope('barrier'):
        pl.semaphore_wait(barrier, len(partners))
    halo_copy(0, 0, 0).start()
    pack(0, 0)
    halo_copy(0, 1, 0).start()
    pack(1, 1)
    halo_copy(0, 0, 1).start()
    pack(0, 1)
    halo_copy(0, 1, 1).start()
    for load in loads[4:]:
        load.wait()

    def local_part(degree, row, b):
        cur = (cur0, cur1)[degree]

        def one(p, _):
            i = tbl[p, 0]
            own, n2, n3, n4 = cur[b, p], cur[b, tbl[p, 2]], cur[b, tbl[p, 3]], cur[b, tbl[p, 4]]
            pair = [zero, n2] if row == 0 else [n2, zero]
            stack = jnp.concatenate([own] + pair + [n3, n4], axis=0)
            applied = jnp.dot(hv[i], stack, preferred_element_type=F32)
            before = yp[b, i] if degree == 0 else cur0[b, p]
            acc[b, p] = SCALE * (applied - CENTER * own.astype(F32)) - before.astype(F32)
            return 0

        lax.fori_loop(row * GY, row * GY + GY, one, 0, unroll=8)

    def full_value(degree, row, b, p):
        i = tbl[p, 0]
        far = halo[degree][row][b][tbl[p, 5]]
        if row == 0:
            applied = jnp.dot(hv[i, :, 0:128], jnp.concatenate([zero, far], axis=0), preferred_element_type=F32)
        else:
            applied = jnp.dot(hv[i, :, 128:256], jnp.concatenate([far, zero], axis=0), preferred_element_type=F32)
        return jnp.where(rows < tbl[p, 1], acc[b, p] + SCALE * applied, 0.0).astype(BF)

    def first(row, b):
        def one(p, _):
            cur1[b, p] = full_value(0, row, b, p)
            return 0

        lax.fori_loop(row * GY, row * GY + GY, one, 0, unroll=8)

    def z_copy(b, j):
        return remote(
            fil.at[b, pl.ds((1 - zh) * GY + j * CH, CH)], xg.at[b, zh, pl.ds(j * CH, CH)],
            zsend.at[b], zrecv.at[b, j], {"zh": 1 - zh},
        )

    def x_copy(way, b, j, kind):
        part = pl.ds(j * CH, CH)
        h = (zh, 1 - zh)[kind]
        src = fil.at[b, pl.ds(zh * GY + j * CH, CH)] if kind == 0 else xg.at[b, h, part]
        return remote(
            src, (x1, x2)[way].at[b, h, part], xsend.at[way, b], xrecv.at[way, b, j, kind], (xp, xm)[way]
        )

    def pass_on(b, j, kind):
        part, way, h = pl.ds(j * CH, CH), j // 2, (zh, 1 - zh)[kind]
        return remote(
            (x1, x2)[way].at[b, h, part], x3.at[b, h, part], gsend.at[b], grecv.at[b, j, kind], (xp, xm)[way]
        )

    def bytes_of(ref, sem):
        return pltpu.make_async_copy(ref, ref, sem)

    def z_to_x(b):
        for j in ORDER:
            with jax.named_scope(f'wz{b}{j}'):
                z_copy(b, j).wait_recv()
            x_copy(0, b, j, 1).start()
            x_copy(1, b, j, 1).start()

    def second(b):
        for j in ORDER:
            for row in (1, 0):
                for m in range(CH):
                    p = row * GY + j * CH + m
                    fil[b, p] = full_value(1, row, b, p)
            if b == 0:

                @pl.when(ORDER.index(j) < at_once)
                def _():
                    z_copy(b, j).start()

            else:

                @pl.when(jnp.logical_not(last))
                def _():
                    z_copy(b, j).start()

            x_copy(0, b, j, 0).start()
            x_copy(1, b, j, 0).start()
        xg[b, zh] = fil[b, pl.ds(zh * GY, GY)]

    def pass_half(b, kind):
        for j in ORDER:
            with jax.named_scope(f'wx{b}{kind}{j}'):
                x_copy(j // 2, b, j, kind).wait_recv()
            pass_on(b, j, kind).start()

    for b in (0, 1):
        with jax.named_scope(f'local0{b}'):
            local_part(0, 1, b)
            local_part(0, 0, b)
    for b in (0, 1):
        with jax.named_scope(f'w_h0{b}1'):
            halo_copy(0, 1, b).wait_recv()
        first(1, b)
        halo_copy(1, 0, b).start()
        with jax.named_scope(f'w_h0{b}0'):
            halo_copy(0, 0, b).wait_recv()
        first(0, b)
        halo_copy(1, 1, b).start()
        with jax.named_scope(f'local1{b}'):
            local_part(1, 1, b)
            local_part(1, 0, b)
    def finish(b):
        with jax.named_scope(f'w_h1{b}'):
            halo_copy(1, 1, b).wait_recv()
            halo_copy(1, 0, b).wait_recv()
        if b == 1:

            for k, j in enumerate(ORDER):

                @pl.when(k >= at_once)
                def _():
                    z_copy(0, j).start()

        with jax.named_scope(f'second{b}'):
            second(b)

    finish(0)

    finish(1)
    z_to_x(0)
    pass_half(0, 0)
    pass_half(1, 0)

    @pl.when(last)
    def _():
        for j in ORDER:
            z_copy(1, j).start()

    z_to_x(1)

    def put(i, _):
        s = slot[i]
        outv[i] = jnp.concatenate([fil[0, s], fil[1, s]], axis=1)
        return 0

    with jax.named_scope('put'):
        lax.fori_loop(0, EL, put, 0, unroll=4)
    store_f = pltpu.make_async_copy(outv, out_f, lsem.at[7])
    store_f.start()

    def bound_for(x_a, b):
        return (x_a % 2) * 2 + b

    def c_copy(x_a, b, kind):
        at = ((zh, 1 - zh)[kind], x_a // 2, bound_for(x_a, b))
        return remote(pb.at[(1 - c, *at)], rc.at[at], csend, crecv.at[x_a, b, kind], {"c": 1 - c})

    def product(x_a, b, kind, ref):
        zh_a = (zh, 1 - zh)[kind]
        left = ref[b, zh_a].reshape(GY * BMAX, HB)
        for zh_b in (0, 1):
            right = jnp.concatenate([xg[k, zh_b].reshape(GY * BMAX, HB) for k in (0, 1)], axis=1)
            tile = lax.dot_general(left, right, (((0,), (0,)), ((), ())), preferred_element_type=F32).astype(BF)
            for core in (0, 1):
                pb[core, zh_a, x_a // 2, bound_for(x_a, b), zh_b] = tile[core * 64 : core * 64 + 64]
        c_copy(x_a, b, kind).start()

    def y_copy(to, d, xh, kind):
        zh_a = (zh, 1 - zh)[kind]
        return remote(
            s1.at[zh_a, xh, to], ry.at[d - 1, xh, zh_a], ysend, yrecv.at[d - 1, xh, kind], {"y": to}
        )

    def settle(x_a, b, kind):
        zh_a, xh, to = (zh, 1 - zh)[kind], x_a // 2, bound_for(x_a, b)
        c_copy(x_a, b, kind).wait_recv()
        s1[zh_a, xh, to] = (pb[c, zh_a, xh, to].astype(F32) + rc[zh_a, xh, to].astype(F32)).astype(BF)

        @pl.when(to != y)
        def _():
            y_copy(to, (to + 4 - y) % 4, xh, kind).start()

    def r_copy(to, src_xh):
        d = (to + 8 - z) % 8
        return remote(
            s2.at[src_xh, (to % 4) // 2, to // 4], rz.at[d - 1], rsend, rrecv, z_id(to)
        )

    def gather_y(xh, kind):
        zh_a = (zh, 1 - zh)[kind]
        for d in (1, 3, 2):
            y_copy((y + d) % 4, d, xh, kind).wait_recv()
        total = s1[zh_a, xh, y].astype(F32)
        for d in range(3):
            total = total + ry[d, xh, zh_a].astype(F32)
        s2[xh, zh_a] = total.astype(BF)
        for zh_b in (0, 1):
            to = zh_b * 4 + zh_a * 2 + xh

            @pl.when(to != z)
            def _():
                r_copy(to, xh).start()

    def wait_beside(b, kind):
        for way in (0, 1):
            for j in ((2, 3), (0, 1))[way]:
                x_copy(way, b, j, kind).wait_recv()

    def wait_far(b, kind):
        for j in ORDER:
            pass_on(b, j, kind).wait_recv()

    def all_of(units):
        for unit, ref in units:
            product(*unit, ref)
        return [unit for unit, _ in units]

    def settle_all(units):
        for unit in units:
            settle(*unit)

    def beside(b, kind):
        return [((x_prev, b, kind), x1), ((x_next, b, kind), x2)]

    pass_half(0, 1)
    with jax.named_scope('prod_e'):
        for b in (0, 1):
            wait_beside(b, 0)
        early = all_of([((x, b, kind), xg) for b in (0, 1) for kind in (0, 1)] + beside(0, 0) + beside(1, 0))
    with jax.named_scope('settle_e'):
        settle_all(early)
    with jax.named_scope('w_x0'):
        wait_beside(0, 1)
    with jax.named_scope('prod_m'):
        middle = all_of(beside(0, 1))
    pass_half(1, 1)
    with jax.named_scope('w_far_0'):
        wait_far(0, 0)
        wait_far(1, 0)
    with jax.named_scope('prod_f0'):
        middle += all_of([((x_far, 0, 0), x3), ((x_far, 1, 0), x3)])
    with jax.named_scope('settle_m'):
        settle_all(middle)
    with jax.named_scope('w_x1'):
        wait_beside(1, 1)
    with jax.named_scope('prod_l'):
        late = all_of(beside(1, 1))
        settle_all(late)
    with jax.named_scope('w_far0'):
        wait_far(0, 1)
    settle_all(all_of([((x_far, 0, 1), x3)]))
    with jax.named_scope('w_far1'):
        wait_far(1, 1)
    settle_all(all_of([((x_far, 1, 1), x3)]))

    with jax.named_scope('gather_y0'):
        gather_y(x // 2, 0)
        gather_y(1 - x // 2, 0)
    with jax.named_scope('gather_y1'):
        gather_y(x // 2, 1)
    with jax.named_scope('gather_y2'):
        gather_y(1 - x // 2, 1)

    total = s2[zl % 2, zl // 2, zh].astype(F32)
    with jax.named_scope('wr'):
        bytes_of(rz, rrecv).wait()
    for d in range(7):
        total = total + rz[d].astype(F32)
    mv[...] = total * (1.0 / 65536.0)
    store_m = pltpu.make_async_copy(mv, out_m, lsem.at[8])
    store_m.start()

    with jax.named_scope('tail'):
        for degree in (0, 1):
            for row in (0, 1):
                for b in (0, 1):
                    halo_copy(degree, row, b).wait_send()
        for b in (0, 1):
            for k in (0, 1):
                bytes_of(xg.at[b], xsend.at[k, b]).wait()
            bytes_of(x3.at[b], gsend.at[b]).wait()
            bytes_of(fil.at[b, pl.ds(0, GY)], zsend.at[b]).wait()
        bytes_of(rc, csend).wait()
        bytes_of(ry, ysend).wait()
        bytes_of(rz, rsend).wait()
        store_f.wait()
        store_m.wait()


PARTS = 4


def put_out_kernel(f_h, m_h, f_out, m_out, f_v, m_v, came, gone):
    pairs = [(m_h, m_v, m_out)]
    for k in range(PARTS):
        part = pl.ds(k * EL // PARTS, EL // PARTS)
        pairs.append((f_h.at[part], f_v.at[part], f_out.at[part]))
    into = [pltpu.make_async_copy(a, b, came.at[k]) for k, (a, b, _) in enumerate(pairs)]
    out = [pltpu.make_async_copy(b, a, gone.at[k]) for k, (_, b, a) in enumerate(pairs)]
    for copy in into:
        copy.start()
    for first, then in zip(into, out):
        first.wait()
        then.start()
    for copy in out:
        copy.wait()


def on_device(y_current, y_previous, h_blocks, basis_sizes, neighbours):
    any_space = pl.BlockSpec(memory_space=pl.ANY)
    dma = pltpu.SemaphoreType.DMA
    halves = pltpu.VMEM((2, EL, BMAX, HB), BF)
    met = pltpu.VMEM((2, 2, GY, BMAX, HB), BF)
    filtered, margin = pl.pallas_call(
        main_kernel,
        out_shape=(
            jax.ShapeDtypeStruct((EL, BMAX, BD), BF),
            jax.ShapeDtypeStruct((64, BD), F32),
        ),
        in_specs=[any_space] * 5,
        out_specs=(any_space, any_space),
        scratch_shapes=[
            pltpu.SMEM((4, EL), jnp.int32),
            pltpu.SMEM((EL,), jnp.int32),
            pltpu.SMEM((EL, 8), jnp.int32),
            pltpu.SMEM((EL,), jnp.int32),
            pltpu.SMEM((EL,), jnp.int32),
            pltpu.SMEM((EL,), jnp.int32),
            halves,
            halves,
            pltpu.VMEM((EL, BMAX, 5 * BMAX), BF),
            halves,
            halves,
            *[pltpu.VMEM((GY, BMAX, HB), BF)] * 8,
            pltpu.VMEM((2, EL, BMAX, HB), F32),
            halves,
            pltpu.VMEM((EL, BMAX, BD), BF),
            met,
            met,
            met,
            met,
            pltpu.VMEM((2, 2, 2, 4, 2, 64, BD), BF),
            pltpu.VMEM((2, 2, 4, 2, 64, BD), BF),
            pltpu.VMEM((2, 2, 4, 2, 64, BD), BF),
            pltpu.VMEM((3, 2, 2, 2, 64, BD), BF),
            pltpu.VMEM((2, 2, 2, 64, BD), BF),
            pltpu.VMEM((7, 64, BD), BF),
            pltpu.VMEM((64, BD), F32),
            dma((9,)),
            dma((2, 2, 2)), dma((2, 2, 2)),
            dma((2,)), dma((2, NCH)),
            dma((2, 2)), dma((2, 2, NCH, 2)),
            dma((2,)), dma((2, NCH, 2)),
            dma, dma((4, 2, 2)),
            dma, dma((3, 2, 2)),
            dma, dma,
        ],
        compiler_params=pltpu.CompilerParams(collective_id=0, has_side_effects=True),
        name="chain",
    )(neighbours.T, basis_sizes, y_current, y_previous, h_blocks)
    return pl.pallas_call(
        put_out_kernel,
        out_shape=(
            jax.ShapeDtypeStruct((EL, BMAX, BD), BF),
            jax.ShapeDtypeStruct((64, BD), F32),
        ),
        in_specs=[any_space] * 2,
        out_specs=(any_space, any_space),
        scratch_shapes=[
            pltpu.VMEM((EL, BMAX, BD), BF),
            pltpu.VMEM((64, BD), F32),
            dma((PARTS + 1,)), dma((PARTS + 1,)),
        ],
        name="put_out",
    )(filtered, margin)


def solution(mesh):
    split = Mesh(mesh.devices.reshape(4, 4, 2, 2, 4), ELEM + BAND)
    return jax.shard_map(
        on_device,
        mesh=split,
        in_specs=(
            P(ELEM, None, BAND),
            P(ELEM, None, BAND),
            P(ELEM, None, None),
            P(ELEM),
            P(ELEM, None),
        ),
        out_specs=(P(ELEM, None, BAND), P(ELEM, BAND)),
        check_vma=False,
    )
```

```python
import jax
import jax.numpy as jnp
from jax import lax
from jax.experimental import pallas as pl
from jax.experimental.pallas import tpu as pltpu
from jax.sharding import Mesh
from jax.sharding import PartitionSpec as P

BMAX = 64
EL = 32
GY = 16
BD = 256
NB = 2048
ROWS = GY * BMAX
HB = 128
CH = 4
NCH = GY // CH
ORDER = (0, 2, 1, 3)

CENTER = 0.3
SCALE = 2.0 / 1.7

ELEM = ("zl", "y", "c")
BAND = ("zh", "x")
BF = jnp.bfloat16
F32 = jnp.float32
MESH_ID = pl.DeviceIdType.MESH


def ones_of(word):
    word = word - (lax.shift_right_logical(word, 1) & 0x55555555)
    word = (word & 0x33333333) + (lax.shift_right_logical(word, 2) & 0x33333333)
    word = (word + lax.shift_right_logical(word, 4)) & 0x0F0F0F0F
    return lax.shift_right_logical(word * 0x01010101, 24)


def make_tables(me, nb, sizes, tbl, slot, link, power):
    for i in range(EL):
        power[i] = jnp.int32(1 << i if i < 31 else -(1 << 31))
    ones, rows = jnp.int32(0), []
    wanted = [jnp.int32(0), jnp.int32(0)]
    for i in range(EL):
        row = jnp.where(nb[0, i] >> 5 == me, 1, 0)
        rows.append(row)
        slot[i] = jnp.where(row == 1, GY + ones, i - ones) & (EL - 1)
        ones = ones + row
        for k in (0, 1):
            wanted[k] = wanted[k] + jnp.where(row == k, power[nb[k, i] & (EL - 1)], 0)
    first = [jnp.int32(0), jnp.int32(0)]
    for i in reversed(range(EL)):
        link[i] = jnp.where(rows[i] == 1, first[1], first[0])
        first = [jnp.where(rows[i] == k, i, first[k]) for k in (0, 1)]
    for row in (0, 1):
        i = first[row]
        for p in range(row * GY, row * GY + GY):
            tbl[p, 0] = i
            tbl[p, 1] = sizes[i]
            tbl[p, 2] = slot[nb[1 - row, i] & (EL - 1)]
            tbl[p, 3] = slot[nb[2, i] & (EL - 1)]
            tbl[p, 4] = slot[nb[3, i] & (EL - 1)]
            tbl[p, 5] = ones_of(wanted[row] & (power[nb[row, i] & (EL - 1)] - 1)) & (GY - 1)
            i = link[i]


def main_kernel(
    nb_h, size_h, yc_h, yp_h, h_h, out_f, out_m, nb, sizes, tbl, slot, link, power,
    yc, yp, hv, cur0, cur1, f000, f001, f010, f011, f100, f101, f110, f111,
    acc, fil, outv, xg, x1, x2, x3, pb, rc, s1, ry, s2, rz, mv,
    lsem, hsend, hrecv, zsend, zrecv, xsend, xrecv, gsend, grecv, csend, crecv, ysend, yrecv, rsend, rrecv,
):
    zl, y, c = (lax.axis_index(a) for a in ELEM)
    zh, x = (lax.axis_index(a) for a in BAND)
    z = zh * 4 + zl
    e = (zl * 4 + y) * 2 + c
    outer = jnp.logical_or(y == 0, y == 3)
    crossing = jnp.logical_or(jnp.logical_and(y == 0, c == 0), jnp.logical_and(y == 3, c == 1))
    last = jnp.logical_or(jnp.logical_and(y == 0, zl == 0), jnp.logical_and(y == 3, zl == 3))
    at_once = jnp.where(last, 4, jnp.where(outer, 1, NCH))

    def elem_id(other):
        return {"zl": other // 8, "y": (other // 2) % 4, "c": other % 2}

    def z_id(other):
        return {"zh": other // 4, "zl": other % 4}

    nxt, prv = elem_id((e + 1) % 32), elem_id((e + 31) % 32)
    x_prev, x_next, x_far = (x + 3) % 4, (x + 1) % 4, (x + 2) % 4
    xp, xm = {"x": x_next}, {"x": x_prev}

    def remote(src, dst, ss, rs, to):
        return pltpu.make_async_remote_copy(
            src_ref=src, dst_ref=dst, send_sem=ss, recv_sem=rs, device_id=to, device_id_type=MESH_ID
        )

    loads = [
        pltpu.make_async_copy(src, dst, lsem.at[k])
        for k, (src, dst) in enumerate(
            [(nb_h, nb), (size_h, sizes)]
            + [(yc_h.at[:, :, pl.ds(b * HB, HB)], yc.at[b]) for b in (0, 1)]
            + [(h_h, hv)]
            + [(yp_h.at[:, :, pl.ds(b * HB, HB)], yp.at[b]) for b in (0, 1)]
        )
    ]
    for load in loads:
        load.start()

    barrier = pltpu.get_barrier_semaphore()
    partners = [nxt, prv, xp, xm]
    partners += [{"y": (y + d) % 4} for d in (1, 2, 3)]
    partners += [z_id((z + d) % 8) for d in range(1, 8)]
    for to in partners:
        pl.semaphore_signal(barrier, inc=1, device_id=to, device_id_type=MESH_ID)

    rows = lax.broadcasted_iota(jnp.int32, (BMAX, HB), 0)
    zero = jnp.zeros((BMAX, HB), BF)

    with jax.named_scope('w_load'):
        for load in loads[:2]:
            load.wait()
    with jax.named_scope('tables'):
        make_tables(e, nb, sizes, tbl, slot, link, power)
    for load in loads[2:4]:
        load.wait()

    def pack(row, b):
        def one(p, _):
            value = yc[b, tbl[p, 0]].astype(F32)
            cur0[b, p] = jnp.where(rows < tbl[p, 1], value, 0.0).astype(BF)
            return 0

        lax.fori_loop(row * GY, row * GY + GY, one, 0, unroll=4)

    halo = (((f000, f001), (f010, f011)), ((f100, f101), (f110, f111)))

    def halo_copy(degree, row, b):
        return remote(
            (cur0, cur1)[degree].at[b, pl.ds((1 - row) * GY, GY)], halo[degree][row][b],
            hsend.at[degree, row, b], hrecv.at[degree, row, b], (nxt, prv)[row],
        )

    with jax.named_scope('pack'):
        for b in (0, 1):
            pack(1, b)
            pack(0, b)
    with jax.named_scope('barrier'):
        pl.semaphore_wait(barrier, len(partners))

    for core in (0, 1):

        @pl.when(c == core)
        def _():
            for row in (1 - core, core):
                for b in (0, 1):
                    halo_copy(0, row, b).start()

    for load in loads[4:]:
        load.wait()

    def local_part(degree, row, b):
        cur = (cur0, cur1)[degree]

        def one(p, _):
            i = tbl[p, 0]
            own, n2, n3, n4 = cur[b, p], cur[b, tbl[p, 2]], cur[b, tbl[p, 3]], cur[b, tbl[p, 4]]
            pair = [zero, n2] if row == 0 else [n2, zero]
            stack = jnp.concatenate([own] + pair + [n3, n4], axis=0)
            applied = jnp.dot(hv[i], stack, preferred_element_type=F32)
            before = yp[b, i] if degree == 0 else cur0[b, p]
            acc[b, p] = SCALE * (applied - CENTER * own.astype(F32)) - before.astype(F32)
            return 0

        lax.fori_loop(row * GY, row * GY + GY, one, 0, unroll=8)

    def full_value(degree, row, b, p):
        i = tbl[p, 0]
        far = halo[degree][row][b][tbl[p, 5]]
        if row == 0:
            applied = jnp.dot(hv[i, :, 0:128], jnp.concatenate([zero, far], axis=0), preferred_element_type=F32)
        else:
            applied = jnp.dot(hv[i, :, 128:256], jnp.concatenate([far, zero], axis=0), preferred_element_type=F32)
        return jnp.where(rows < tbl[p, 1], acc[b, p] + SCALE * applied, 0.0).astype(BF)

    def first(row, b):
        def one(p, _):
            cur1[b, p] = full_value(0, row, b, p)
            return 0

        lax.fori_loop(row * GY, row * GY + GY, one, 0, unroll=8)

    def z_copy(b, j):
        return remote(
            fil.at[b, pl.ds((1 - zh) * GY + j * CH, CH)], xg.at[b, zh, pl.ds(j * CH, CH)],
            zsend.at[b], zrecv.at[b, j], {"zh": 1 - zh},
        )

    def x_copy(way, b, j, kind):
        part = pl.ds(j * CH, CH)
        h = (zh, 1 - zh)[kind]
        src = fil.at[b, pl.ds(zh * GY + j * CH, CH)] if kind == 0 else xg.at[b, h, part]
        return remote(
            src, (x1, x2)[way].at[b, h, part], xsend.at[way, b], xrecv.at[way, b, j, kind], (xp, xm)[way]
        )

    def pass_on(b, j, kind):
        part, way, h = pl.ds(j * CH, CH), j // 2, (zh, 1 - zh)[kind]
        return remote(
            (x1, x2)[way].at[b, h, part], x3.at[b, h, part], gsend.at[b], grecv.at[b, j, kind], (xp, xm)[way]
        )

    def bytes_of(ref, sem):
        return pltpu.make_async_copy(ref, ref, sem)

    def z_to_x(b):
        for j in ORDER:
            with jax.named_scope(f'wz{b}{j}'):
                z_copy(b, j).wait_recv()
            x_copy(0, b, j, 1).start()
            x_copy(1, b, j, 1).start()

    def second(b):
        for j in ORDER:
            for row in (1, 0):
                for m in range(CH):
                    p = row * GY + j * CH + m
                    fil[b, p] = full_value(1, row, b, p)
            if b == 0:

                @pl.when(ORDER.index(j) < at_once)
                def _():
                    z_copy(b, j).start()

            else:

                @pl.when(jnp.logical_not(last))
                def _():
                    z_copy(b, j).start()

            x_copy(0, b, j, 0).start()
            x_copy(1, b, j, 0).start()
        xg[b, zh] = fil[b, pl.ds(zh * GY, GY)]

    def pass_half(b, kind):
        for j in ORDER:
            with jax.named_scope(f'wx{b}{kind}{j}'):
                x_copy(j // 2, b, j, kind).wait_recv()
            pass_on(b, j, kind).start()

    for b in (0, 1):
        with jax.named_scope(f'local0{b}'):
            local_part(0, 1, b)
            local_part(0, 0, b)
    for b in (0, 1):
        with jax.named_scope(f'w_h0{b}1'):
            halo_copy(0, 1, b).wait_recv()
        first(1, b)
        halo_copy(1, 0, b).start()
        with jax.named_scope(f'w_h0{b}0'):
            halo_copy(0, 0, b).wait_recv()
        first(0, b)
        halo_copy(1, 1, b).start()
        with jax.named_scope(f'local1{b}'):
            local_part(1, 1, b)
            local_part(1, 0, b)
    def finish(b):
        with jax.named_scope(f'w_h1{b}'):
            halo_copy(1, 1, b).wait_recv()
            halo_copy(1, 0, b).wait_recv()
        if b == 1:

            for k, j in enumerate(ORDER):

                @pl.when(k >= at_once)
                def _():
                    z_copy(0, j).start()

        with jax.named_scope(f'second{b}'):
            second(b)

    finish(0)

    finish(1)
    z_to_x(0)
    pass_half(0, 0)
    pass_half(1, 0)

    @pl.when(last)
    def _():
        for j in ORDER:
            z_copy(1, j).start()

    z_to_x(1)

    def put(i, _):
        s = slot[i]
        outv[i] = jnp.concatenate([fil[0, s], fil[1, s]], axis=1)
        return 0

    with jax.named_scope('put'):
        lax.fori_loop(0, EL, put, 0, unroll=4)
    store_f = pltpu.make_async_copy(outv, out_f, lsem.at[7])
    store_f.start()

    def bound_for(x_a, b):
        return (x_a % 2) * 2 + b

    def c_copy(x_a, b, kind):
        at = ((zh, 1 - zh)[kind], x_a // 2, bound_for(x_a, b))
        return remote(pb.at[(1 - c, *at)], rc.at[at], csend, crecv.at[x_a, b, kind], {"c": 1 - c})

    def product(x_a, b, kind, ref):
        zh_a = (zh, 1 - zh)[kind]
        left = ref[b, zh_a].reshape(GY * BMAX, HB)
        for zh_b in (0, 1):
            right = jnp.concatenate([xg[k, zh_b].reshape(GY * BMAX, HB) for k in (0, 1)], axis=1)
            tile = lax.dot_general(left, right, (((0,), (0,)), ((), ())), preferred_element_type=F32).astype(BF)
            for core in (0, 1):
                pb[core, zh_a, x_a // 2, bound_for(x_a, b), zh_b] = tile[core * 64 : core * 64 + 64]
        c_copy(x_a, b, kind).start()

    def y_copy(to, d, xh, kind):
        zh_a = (zh, 1 - zh)[kind]
        return remote(
            s1.at[zh_a, xh, to], ry.at[d - 1, xh, zh_a], ysend, yrecv.at[d - 1, xh, kind], {"y": to}
        )

    def settle(x_a, b, kind):
        zh_a, xh, to = (zh, 1 - zh)[kind], x_a // 2, bound_for(x_a, b)
        c_copy(x_a, b, kind).wait_recv()
        s1[zh_a, xh, to] = (pb[c, zh_a, xh, to].astype(F32) + rc[zh_a, xh, to].astype(F32)).astype(BF)

        @pl.when(to != y)
        def _():
            y_copy(to, (to + 4 - y) % 4, xh, kind).start()

    def r_copy(to, src_xh):
        d = (to + 8 - z) % 8
        return remote(
            s2.at[src_xh, (to % 4) // 2, to // 4], rz.at[d - 1], rsend, rrecv, z_id(to)
        )

    def gather_y(xh, kind):
        zh_a = (zh, 1 - zh)[kind]
        for d in (1, 3, 2):
            y_copy((y + d) % 4, d, xh, kind).wait_recv()
        total = s1[zh_a, xh, y].astype(F32)
        for d in range(3):
            total = total + ry[d, xh, zh_a].astype(F32)
        s2[xh, zh_a] = total.astype(BF)
        for zh_b in (0, 1):
            to = zh_b * 4 + zh_a * 2 + xh

            @pl.when(to != z)
            def _():
                r_copy(to, xh).start()

    def wait_beside(b, kind):
        for way in (0, 1):
            for j in ((2, 3), (0, 1))[way]:
                x_copy(way, b, j, kind).wait_recv()

    def wait_far(b, kind):
        for j in ORDER:
            pass_on(b, j, kind).wait_recv()

    def all_of(units):
        for unit, ref in units:
            product(*unit, ref)
        return [unit for unit, _ in units]

    def settle_all(units):
        for unit in units:
            settle(*unit)

    def beside(b, kind):
        return [((x_prev, b, kind), x1), ((x_next, b, kind), x2)]

    pass_half(0, 1)
    with jax.named_scope('prod_e'):
        for b in (0, 1):
            wait_beside(b, 0)
        early = all_of([((x, b, kind), xg) for b in (0, 1) for kind in (0, 1)] + beside(0, 0) + beside(1, 0))
    with jax.named_scope('settle_e'):
        settle_all(early)
    with jax.named_scope('w_x0'):
        wait_beside(0, 1)
    with jax.named_scope('prod_m'):
        middle = all_of(beside(0, 1))
    pass_half(1, 1)
    with jax.named_scope('w_far_0'):
        wait_far(0, 0)
        wait_far(1, 0)
    with jax.named_scope('prod_f0'):
        middle += all_of([((x_far, 0, 0), x3), ((x_far, 1, 0), x3)])
    with jax.named_scope('settle_m'):
        settle_all(middle)
    with jax.named_scope('w_x1'):
        wait_beside(1, 1)
    with jax.named_scope('prod_l'):
        late = all_of(beside(1, 1))
        settle_all(late)
    with jax.named_scope('w_far0'):
        wait_far(0, 1)
    settle_all(all_of([((x_far, 0, 1), x3)]))
    with jax.named_scope('w_far1'):
        wait_far(1, 1)
    settle_all(all_of([((x_far, 1, 1), x3)]))

    with jax.named_scope('gather_y0'):
        gather_y(x // 2, 0)
        gather_y(1 - x // 2, 0)
    with jax.named_scope('gather_y1'):
        gather_y(x // 2, 1)
    with jax.named_scope('gather_y2'):
        gather_y(1 - x // 2, 1)

    total = s2[zl % 2, zl // 2, zh].astype(F32)
    with jax.named_scope('wr'):
        bytes_of(rz, rrecv).wait()
    for d in range(7):
        total = total + rz[d].astype(F32)
    mv[...] = total * (1.0 / 65536.0)
    store_m = pltpu.make_async_copy(mv, out_m, lsem.at[8])
    store_m.start()

    with jax.named_scope('tail'):
        for degree in (0, 1):
            for row in (0, 1):
                for b in (0, 1):
                    halo_copy(degree, row, b).wait_send()
        for b in (0, 1):
            for k in (0, 1):
                bytes_of(xg.at[b], xsend.at[k, b]).wait()
            bytes_of(x3.at[b], gsend.at[b]).wait()
            bytes_of(fil.at[b, pl.ds(0, GY)], zsend.at[b]).wait()
        bytes_of(rc, csend).wait()
        bytes_of(ry, ysend).wait()
        bytes_of(rz, rsend).wait()
        store_f.wait()
        store_m.wait()


PARTS = 4


def put_out_kernel(f_h, m_h, f_out, m_out, f_v, m_v, came, gone):
    pairs = [(m_h, m_v, m_out)]
    for k in range(PARTS):
        part = pl.ds(k * EL // PARTS, EL // PARTS)
        pairs.append((f_h.at[part], f_v.at[part], f_out.at[part]))
    into = [pltpu.make_async_copy(a, b, came.at[k]) for k, (a, b, _) in enumerate(pairs)]
    out = [pltpu.make_async_copy(b, a, gone.at[k]) for k, (_, b, a) in enumerate(pairs)]
    for copy in into:
        copy.start()
    for first, then in zip(into, out):
        first.wait()
        then.start()
    for copy in out:
        copy.wait()


def on_device(y_current, y_previous, h_blocks, basis_sizes, neighbours):
    any_space = pl.BlockSpec(memory_space=pl.ANY)
    dma = pltpu.SemaphoreType.DMA
    halves = pltpu.VMEM((2, EL, BMAX, HB), BF)
    met = pltpu.VMEM((2, 2, GY, BMAX, HB), BF)
    filtered, margin = pl.pallas_call(
        main_kernel,
        out_shape=(
            jax.ShapeDtypeStruct((EL, BMAX, BD), BF),
            jax.ShapeDtypeStruct((64, BD), F32),
        ),
        in_specs=[any_space] * 5,
        out_specs=(any_space, any_space),
        scratch_shapes=[
            pltpu.SMEM((4, EL), jnp.int32),
            pltpu.SMEM((EL,), jnp.int32),
            pltpu.SMEM((EL, 8), jnp.int32),
            pltpu.SMEM((EL,), jnp.int32),
            pltpu.SMEM((EL,), jnp.int32),
            pltpu.SMEM((EL,), jnp.int32),
            halves,
            halves,
            pltpu.VMEM((EL, BMAX, 5 * BMAX), BF),
            halves,
            halves,
            *[pltpu.VMEM((GY, BMAX, HB), BF)] * 8,
            pltpu.VMEM((2, EL, BMAX, HB), F32),
            halves,
            pltpu.VMEM((EL, BMAX, BD), BF),
            met,
            met,
            met,
            met,
            pltpu.VMEM((2, 2, 2, 4, 2, 64, BD), BF),
            pltpu.VMEM((2, 2, 4, 2, 64, BD), BF),
            pltpu.VMEM((2, 2, 4, 2, 64, BD), BF),
            pltpu.VMEM((3, 2, 2, 2, 64, BD), BF),
            pltpu.VMEM((2, 2, 2, 64, BD), BF),
            pltpu.VMEM((7, 64, BD), BF),
            pltpu.VMEM((64, BD), F32),
            dma((9,)),
            dma((2, 2, 2)), dma((2, 2, 2)),
            dma((2,)), dma((2, NCH)),
            dma((2, 2)), dma((2, 2, NCH, 2)),
            dma((2,)), dma((2, NCH, 2)),
            dma, dma((4, 2, 2)),
            dma, dma((3, 2, 2)),
            dma, dma,
        ],
        compiler_params=pltpu.CompilerParams(collective_id=0, has_side_effects=True),
        name="chain",
    )(neighbours.T, basis_sizes, y_current, y_previous, h_blocks)
    return pl.pallas_call(
        put_out_kernel,
        out_shape=(
            jax.ShapeDtypeStruct((EL, BMAX, BD), BF),
            jax.ShapeDtypeStruct((64, BD), F32),
        ),
        in_specs=[any_space] * 2,
        out_specs=(any_space, any_space),
        scratch_shapes=[
            pltpu.VMEM((EL, BMAX, BD), BF),
            pltpu.VMEM((64, BD), F32),
            dma((PARTS + 1,)), dma((PARTS + 1,)),
        ],
        name="put_out",
    )(filtered, margin)


def solution(mesh):
    split = Mesh(mesh.devices.reshape(4, 4, 2, 2, 4), ELEM + BAND)
    return jax.shard_map(
        on_device,
        mesh=split,
        in_specs=(
            P(ELEM, None, BAND),
            P(ELEM, None, BAND),
            P(ELEM, None, None),
            P(ELEM),
            P(ELEM, None),
        ),
        out_specs=(P(ELEM, None, BAND), P(ELEM, BAND)),
        check_vma=False,
    )
```

```python
import jax
import jax.numpy as jnp
from jax import lax
from jax.experimental import pallas as pl
from jax.experimental.pallas import tpu as pltpu
from jax.sharding import Mesh
from jax.sharding import PartitionSpec as P

BMAX = 64
EL = 32
GY = 16
BD = 256
NB = 2048
ROWS = GY * BMAX
HB = 128
CH = 4
NCH = GY // CH
ORDER = (0, 2, 1, 3)

CENTER = 0.3
SCALE = 2.0 / 1.7

ELEM = ("zl", "y", "c")
BAND = ("zh", "x")
BF = jnp.bfloat16
F32 = jnp.float32
MESH_ID = pl.DeviceIdType.MESH


def ones_of(word):
    word = word - (lax.shift_right_logical(word, 1) & 0x55555555)
    word = (word & 0x33333333) + (lax.shift_right_logical(word, 2) & 0x33333333)
    word = (word + lax.shift_right_logical(word, 4)) & 0x0F0F0F0F
    return lax.shift_right_logical(word * 0x01010101, 24)


def make_tables(me, nb, sizes, tbl, slot, link, power):
    for i in range(EL):
        power[i] = jnp.int32(1 << i if i < 31 else -(1 << 31))
    ones, rows = jnp.int32(0), []
    wanted = [jnp.int32(0), jnp.int32(0)]
    for i in range(EL):
        row = jnp.where(nb[0, i] >> 5 == me, 1, 0)
        rows.append(row)
        slot[i] = jnp.where(row == 1, GY + ones, i - ones) & (EL - 1)
        ones = ones + row
        for k in (0, 1):
            wanted[k] = wanted[k] + jnp.where(row == k, power[nb[k, i] & (EL - 1)], 0)
    first = [jnp.int32(0), jnp.int32(0)]
    for i in reversed(range(EL)):
        link[i] = jnp.where(rows[i] == 1, first[1], first[0])
        first = [jnp.where(rows[i] == k, i, first[k]) for k in (0, 1)]
    for row in (0, 1):
        i = first[row]
        for p in range(row * GY, row * GY + GY):
            tbl[p, 0] = i
            tbl[p, 1] = sizes[i]
            tbl[p, 2] = slot[nb[1 - row, i] & (EL - 1)]
            tbl[p, 3] = slot[nb[2, i] & (EL - 1)]
            tbl[p, 4] = slot[nb[3, i] & (EL - 1)]
            tbl[p, 5] = ones_of(wanted[row] & (power[nb[row, i] & (EL - 1)] - 1)) & (GY - 1)
            i = link[i]


def main_kernel(
    nb_h, size_h, yc_h, yp_h, h_h, out_f, out_m, nb, sizes, tbl, slot, link, power,
    yc, yp, hv, cur0, cur1, f000, f001, f010, f011, f100, f101, f110, f111,
    acc, fil, outv, xg, x1, x2, x3, pb, rc, s1, ry, s2, rz, mv,
    lsem, hsend, hrecv, zsend, zrecv, xsend, xrecv, gsend, grecv, csend, crecv, ysend, yrecv, rsend, rrecv,
):
    zl, y, c = (lax.axis_index(a) for a in ELEM)
    zh, x = (lax.axis_index(a) for a in BAND)
    z = zh * 4 + zl
    e = (zl * 4 + y) * 2 + c
    outer = jnp.logical_or(y == 0, y == 3)
    crossing = jnp.logical_or(jnp.logical_and(y == 0, c == 0), jnp.logical_and(y == 3, c == 1))
    last = jnp.logical_or(jnp.logical_and(y == 0, zl == 0), jnp.logical_and(y == 3, zl == 3))
    at_once = jnp.where(last, 4, jnp.where(outer, 1, NCH))

    def elem_id(other):
        return {"zl": other // 8, "y": (other // 2) % 4, "c": other % 2}

    def z_id(other):
        return {"zh": other // 4, "zl": other % 4}

    nxt, prv = elem_id((e + 1) % 32), elem_id((e + 31) % 32)
    x_prev, x_next, x_far = (x + 3) % 4, (x + 1) % 4, (x + 2) % 4
    xp, xm = {"x": x_next}, {"x": x_prev}

    def remote(src, dst, ss, rs, to):
        return pltpu.make_async_remote_copy(
            src_ref=src, dst_ref=dst, send_sem=ss, recv_sem=rs, device_id=to, device_id_type=MESH_ID
        )

    loads = [
        pltpu.make_async_copy(src, dst, lsem.at[k])
        for k, (src, dst) in enumerate(
            [(nb_h, nb), (size_h, sizes)]
            + [(yc_h.at[:, :, pl.ds(b * HB, HB)], yc.at[b]) for b in (0, 1)]
            + [(h_h, hv)]
            + [(yp_h.at[:, :, pl.ds(b * HB, HB)], yp.at[b]) for b in (0, 1)]
        )
    ]
    for load in loads:
        load.start()

    barrier = pltpu.get_barrier_semaphore()
    partners = [nxt, prv, xp, xm]
    partners += [{"y": (y + d) % 4} for d in (1, 2, 3)]
    partners += [z_id((z + d) % 8) for d in range(1, 8)]
    for to in partners:
        pl.semaphore_signal(barrier, inc=1, device_id=to, device_id_type=MESH_ID)

    rows = lax.broadcasted_iota(jnp.int32, (BMAX, HB), 0)
    zero = jnp.zeros((BMAX, HB), BF)

    with jax.named_scope('w_load'):
        for load in loads[:2]:
            load.wait()
    with jax.named_scope('tables'):
        make_tables(e, nb, sizes, tbl, slot, link, power)
    for load in loads[2:4]:
        load.wait()

    def pack(row, b):
        def one(p, _):
            value = yc[b, tbl[p, 0]].astype(F32)
            cur0[b, p] = jnp.where(rows < tbl[p, 1], value, 0.0).astype(BF)
            return 0

        lax.fori_loop(row * GY, row * GY + GY, one, 0, unroll=4)

    halo = (((f000, f001), (f010, f011)), ((f100, f101), (f110, f111)))

    def halo_copy(degree, row, b):
        return remote(
            (cur0, cur1)[degree].at[b, pl.ds((1 - row) * GY, GY)], halo[degree][row][b],
            hsend.at[degree, row, b], hrecv.at[degree, row, b], (nxt, prv)[row],
        )

    with jax.named_scope('pack'):
        for b in (0, 1):
            pack(1, b)
            pack(0, b)
    with jax.named_scope('barrier'):
        pl.semaphore_wait(barrier, len(partners))

    for core in (0, 1):

        @pl.when(c == core)
        def _():
            for row in (1 - core, core):
                for b in (0, 1):
                    halo_copy(0, row, b).start()

    for load in loads[4:]:
        load.wait()

    def local_part(degree, row, b):
        cur = (cur0, cur1)[degree]

        def one(p, _):
            i = tbl[p, 0]
            own, n2, n3, n4 = cur[b, p], cur[b, tbl[p, 2]], cur[b, tbl[p, 3]], cur[b, tbl[p, 4]]
            pair = [zero, n2] if row == 0 else [n2, zero]
            stack = jnp.concatenate([own] + pair + [n3, n4], axis=0)
            applied = jnp.dot(hv[i], stack, preferred_element_type=F32)
            before = yp[b, i] if degree == 0 else cur0[b, p]
            acc[b, p] = SCALE * (applied - CENTER * own.astype(F32)) - before.astype(F32)
            return 0

        lax.fori_loop(row * GY, row * GY + GY, one, 0, unroll=8)

    def full_value(degree, row, b, p):
        i = tbl[p, 0]
        far = halo[degree][row][b][tbl[p, 5]]
        if row == 0:
            applied = jnp.dot(hv[i, :, 0:128], jnp.concatenate([zero, far], axis=0), preferred_element_type=F32)
        else:
            applied = jnp.dot(hv[i, :, 128:256], jnp.concatenate([far, zero], axis=0), preferred_element_type=F32)
        return jnp.where(rows < tbl[p, 1], acc[b, p] + SCALE * applied, 0.0).astype(BF)

    def first(row, b):
        def one(p, _):
            cur1[b, p] = full_value(0, row, b, p)
            return 0

        lax.fori_loop(row * GY, row * GY + GY, one, 0, unroll=8)

    def z_copy(b, j):
        return remote(
            fil.at[b, pl.ds((1 - zh) * GY + j * CH, CH)], xg.at[b, zh, pl.ds(j * CH, CH)],
            zsend.at[b], zrecv.at[b, j], {"zh": 1 - zh},
        )

    def x_copy(way, b, j, kind):
        part = pl.ds(j * CH, CH)
        h = (zh, 1 - zh)[kind]
        src = fil.at[b, pl.ds(zh * GY + j * CH, CH)] if kind == 0 else xg.at[b, h, part]
        return remote(
            src, (x1, x2)[way].at[b, h, part], xsend.at[way, b], xrecv.at[way, b, j, kind], (xp, xm)[way]
        )

    def pass_on(b, j, kind):
        part, way, h = pl.ds(j * CH, CH), j // 2, (zh, 1 - zh)[kind]
        return remote(
            (x1, x2)[way].at[b, h, part], x3.at[b, h, part], gsend.at[b], grecv.at[b, j, kind], (xp, xm)[way]
        )

    def bytes_of(ref, sem):
        return pltpu.make_async_copy(ref, ref, sem)

    def z_to_x(b):
        for j in ORDER:
            with jax.named_scope(f'wz{b}{j}'):
                z_copy(b, j).wait_recv()
            x_copy(0, b, j, 1).start()
            x_copy(1, b, j, 1).start()

    def second(b):
        for j in ORDER:
            for row in (1, 0):
                for m in range(CH):
                    p = row * GY + j * CH + m
                    fil[b, p] = full_value(1, row, b, p)
            if b == 0:

                @pl.when(ORDER.index(j) < at_once)
                def _():
                    z_copy(b, j).start()

            else:

                @pl.when(jnp.logical_not(last))
                def _():
                    z_copy(b, j).start()

            x_copy(0, b, j, 0).start()
            x_copy(1, b, j, 0).start()
        xg[b, zh] = fil[b, pl.ds(zh * GY, GY)]

    def pass_half(b, kind):
        for j in ORDER:
            with jax.named_scope(f'wx{b}{kind}{j}'):
                x_copy(j // 2, b, j, kind).wait_recv()
            pass_on(b, j, kind).start()

    for b in (0, 1):
        with jax.named_scope(f'local0{b}'):
            local_part(0, 1, b)
            local_part(0, 0, b)
    for b in (0, 1):
        with jax.named_scope(f'w_h0{b}1'):
            halo_copy(0, 1, b).wait_recv()
        first(1, b)
        halo_copy(1, 0, b).start()
        with jax.named_scope(f'w_h0{b}0'):
            halo_copy(0, 0, b).wait_recv()
        first(0, b)
        halo_copy(1, 1, b).start()
        with jax.named_scope(f'local1{b}'):
            local_part(1, 1, b)
            local_part(1, 0, b)
    def finish(b):
        with jax.named_scope(f'w_h1{b}'):
            halo_copy(1, 1, b).wait_recv()
            halo_copy(1, 0, b).wait_recv()
        if b == 1:

            for k, j in enumerate(ORDER):

                @pl.when(k >= at_once)
                def _():
                    z_copy(0, j).start()

        with jax.named_scope(f'second{b}'):
            second(b)

    finish(0)

    finish(1)
    z_to_x(0)
    pass_half(0, 0)
    pass_half(1, 0)

    @pl.when(last)
    def _():
        for j in ORDER:
            z_copy(1, j).start()

    z_to_x(1)

    def put(i, _):
        s = slot[i]
        outv[i] = jnp.concatenate([fil[0, s], fil[1, s]], axis=1)
        return 0

    with jax.named_scope('put'):
        lax.fori_loop(0, EL, put, 0, unroll=4)
    store_f = pltpu.make_async_copy(outv, out_f, lsem.at[7])
    store_f.start()

    def bound_for(x_a, b):
        return (x_a % 2) * 2 + b

    def c_copy(x_a, b, kind):
        at = ((zh, 1 - zh)[kind], x_a // 2, bound_for(x_a, b))
        return remote(pb.at[(1 - c, *at)], rc.at[at], csend, crecv.at[x_a, b, kind], {"c": 1 - c})

    def product(x_a, b, kind, ref):
        zh_a = (zh, 1 - zh)[kind]
        left = ref[b, zh_a].reshape(GY * BMAX, HB)
        for zh_b in (0, 1):
            right = jnp.concatenate([xg[k, zh_b].reshape(GY * BMAX, HB) for k in (0, 1)], axis=1)
            tile = lax.dot_general(left, right, (((0,), (0,)), ((), ())), preferred_element_type=F32).astype(BF)
            for core in (0, 1):
                pb[core, zh_a, x_a // 2, bound_for(x_a, b), zh_b] = tile[core * 64 : core * 64 + 64]
        c_copy(x_a, b, kind).start()

    def y_copy(to, d, xh, kind):
        zh_a = (zh, 1 - zh)[kind]
        return remote(
            s1.at[zh_a, xh, to], ry.at[d - 1, xh, zh_a], ysend, yrecv.at[d - 1, xh, kind], {"y": to}
        )

    def settle(x_a, b, kind):
        zh_a, xh, to = (zh, 1 - zh)[kind], x_a // 2, bound_for(x_a, b)
        c_copy(x_a, b, kind).wait_recv()
        s1[zh_a, xh, to] = (pb[c, zh_a, xh, to].astype(F32) + rc[zh_a, xh, to].astype(F32)).astype(BF)

        @pl.when(to != y)
        def _():
            y_copy(to, (to + 4 - y) % 4, xh, kind).start()

    def r_copy(to, src_xh):
        d = (to + 8 - z) % 8
        return remote(
            s2.at[src_xh, (to % 4) // 2, to // 4], rz.at[d - 1], rsend, rrecv, z_id(to)
        )

    def gather_y(xh, kind):
        zh_a = (zh, 1 - zh)[kind]
        for d in (1, 3, 2):
            y_copy((y + d) % 4, d, xh, kind).wait_recv()
        total = s1[zh_a, xh, y].astype(F32)
        for d in range(3):
            total = total + ry[d, xh, zh_a].astype(F32)
        s2[xh, zh_a] = total.astype(BF)
        for zh_b in (1 - zh, zh):
            to = zh_b * 4 + zh_a * 2 + xh

            @pl.when(to != z)
            def _():
                r_copy(to, xh).start()

    def wait_beside(b, kind):
        for way in (0, 1):
            for j in ((2, 3), (0, 1))[way]:
                x_copy(way, b, j, kind).wait_recv()

    def wait_far(b, kind):
        for j in ORDER:
            pass_on(b, j, kind).wait_recv()

    def all_of(units):
        for unit, ref in units:
            product(*unit, ref)
        return [unit for unit, _ in units]

    def settle_all(units):
        for unit in units:
            settle(*unit)

    def beside(b, kind):
        return [((x_prev, b, kind), x1), ((x_next, b, kind), x2)]

    pass_half(0, 1)
    with jax.named_scope('prod_e'):
        for b in (0, 1):
            wait_beside(b, 0)
        early = all_of([((x, b, kind), xg) for b in (0, 1) for kind in (0, 1)] + beside(0, 0) + beside(1, 0))
    with jax.named_scope('settle_e'):
        settle_all(early)
    with jax.named_scope('w_x0'):
        wait_beside(0, 1)
    with jax.named_scope('prod_m'):
        middle = all_of(beside(0, 1))
    pass_half(1, 1)
    with jax.named_scope('w_far_0'):
        wait_far(0, 0)
        wait_far(1, 0)
    with jax.named_scope('prod_f0'):
        middle += all_of([((x_far, 0, 0), x3), ((x_far, 1, 0), x3)])
    with jax.named_scope('settle_m'):
        settle_all(middle)
    with jax.named_scope('w_x1'):
        wait_beside(1, 1)
    with jax.named_scope('prod_l'):
        late = all_of(beside(1, 1))
        settle_all(late)
    with jax.named_scope('w_far0'):
        wait_far(0, 1)
    settle_all(all_of([((x_far, 0, 1), x3)]))
    with jax.named_scope('w_far1'):
        wait_far(1, 1)
    settle_all(all_of([((x_far, 1, 1), x3)]))

    with jax.named_scope('gather_y0'):
        gather_y(x // 2, 0)
        gather_y(1 - x // 2, 0)
    with jax.named_scope('gather_y1'):
        gather_y(x // 2, 1)
    with jax.named_scope('gather_y2'):
        gather_y(1 - x // 2, 1)

    total = s2[zl % 2, zl // 2, zh].astype(F32)
    with jax.named_scope('wr'):
        bytes_of(rz, rrecv).wait()
    for d in range(7):
        total = total + rz[d].astype(F32)
    mv[...] = total * (1.0 / 65536.0)
    store_m = pltpu.make_async_copy(mv, out_m, lsem.at[8])
    store_m.start()

    with jax.named_scope('tail'):
        for degree in (0, 1):
            for row in (0, 1):
                for b in (0, 1):
                    halo_copy(degree, row, b).wait_send()
        for b in (0, 1):
            for k in (0, 1):
                bytes_of(xg.at[b], xsend.at[k, b]).wait()
            bytes_of(x3.at[b], gsend.at[b]).wait()
            bytes_of(fil.at[b, pl.ds(0, GY)], zsend.at[b]).wait()
        bytes_of(rc, csend).wait()
        bytes_of(ry, ysend).wait()
        bytes_of(rz, rsend).wait()
        store_f.wait()
        store_m.wait()


PARTS = 4


def put_out_kernel(f_h, m_h, f_out, m_out, f_v, m_v, came, gone):
    pairs = [(m_h, m_v, m_out)]
    for k in range(PARTS):
        part = pl.ds(k * EL // PARTS, EL // PARTS)
        pairs.append((f_h.at[part], f_v.at[part], f_out.at[part]))
    into = [pltpu.make_async_copy(a, b, came.at[k]) for k, (a, b, _) in enumerate(pairs)]
    out = [pltpu.make_async_copy(b, a, gone.at[k]) for k, (_, b, a) in enumerate(pairs)]
    for copy in into:
        copy.start()
    for first, then in zip(into, out):
        first.wait()
        then.start()
    for copy in out:
        copy.wait()


def on_device(y_current, y_previous, h_blocks, basis_sizes, neighbours):
    any_space = pl.BlockSpec(memory_space=pl.ANY)
    dma = pltpu.SemaphoreType.DMA
    halves = pltpu.VMEM((2, EL, BMAX, HB), BF)
    met = pltpu.VMEM((2, 2, GY, BMAX, HB), BF)
    filtered, margin = pl.pallas_call(
        main_kernel,
        out_shape=(
            jax.ShapeDtypeStruct((EL, BMAX, BD), BF),
            jax.ShapeDtypeStruct((64, BD), F32),
        ),
        in_specs=[any_space] * 5,
        out_specs=(any_space, any_space),
        scratch_shapes=[
            pltpu.SMEM((4, EL), jnp.int32),
            pltpu.SMEM((EL,), jnp.int32),
            pltpu.SMEM((EL, 8), jnp.int32),
            pltpu.SMEM((EL,), jnp.int32),
            pltpu.SMEM((EL,), jnp.int32),
            pltpu.SMEM((EL,), jnp.int32),
            halves,
            halves,
            pltpu.VMEM((EL, BMAX, 5 * BMAX), BF),
            halves,
            halves,
            *[pltpu.VMEM((GY, BMAX, HB), BF)] * 8,
            pltpu.VMEM((2, EL, BMAX, HB), F32),
            halves,
            pltpu.VMEM((EL, BMAX, BD), BF),
            met,
            met,
            met,
            met,
            pltpu.VMEM((2, 2, 2, 4, 2, 64, BD), BF),
            pltpu.VMEM((2, 2, 4, 2, 64, BD), BF),
            pltpu.VMEM((2, 2, 4, 2, 64, BD), BF),
            pltpu.VMEM((3, 2, 2, 2, 64, BD), BF),
            pltpu.VMEM((2, 2, 2, 64, BD), BF),
            pltpu.VMEM((7, 64, BD), BF),
            pltpu.VMEM((64, BD), F32),
            dma((9,)),
            dma((2, 2, 2)), dma((2, 2, 2)),
            dma((2,)), dma((2, NCH)),
            dma((2, 2)), dma((2, 2, NCH, 2)),
            dma((2,)), dma((2, NCH, 2)),
            dma, dma((4, 2, 2)),
            dma, dma((3, 2, 2)),
            dma, dma,
        ],
        compiler_params=pltpu.CompilerParams(collective_id=0, has_side_effects=True),
        name="chain",
    )(neighbours.T, basis_sizes, y_current, y_previous, h_blocks)
    return pl.pallas_call(
        put_out_kernel,
        out_shape=(
            jax.ShapeDtypeStruct((EL, BMAX, BD), BF),
            jax.ShapeDtypeStruct((64, BD), F32),
        ),
        in_specs=[any_space] * 2,
        out_specs=(any_space, any_space),
        scratch_shapes=[
            pltpu.VMEM((EL, BMAX, BD), BF),
            pltpu.VMEM((64, BD), F32),
            dma((PARTS + 1,)), dma((PARTS + 1,)),
        ],
        name="put_out",
    )(filtered, margin)


def solution(mesh):
    split = Mesh(mesh.devices.reshape(4, 4, 2, 2, 4), ELEM + BAND)
    return jax.shard_map(
        on_device,
        mesh=split,
        in_specs=(
            P(ELEM, None, BAND),
            P(ELEM, None, BAND),
            P(ELEM, None, None),
            P(ELEM),
            P(ELEM, None),
        ),
        out_specs=(P(ELEM, None, BAND), P(ELEM, BAND)),
        check_vma=False,
    )
```
